512 devices in a mesh: azim: 32 (over z, x_lo), frame: 16 (over x_hi, y, core).
Axes of the slice: x: 4 (x_hi: 2, x_lo: 2; x = x_hi * 2 + x_lo), y: 4, z: 16, core: 2. Of those that a mesh axis runs over, the one named last changes fastest.
Arguments:
- features: bfloat16 [16, 14, 448, 384], P('frame', None, 'azim'), may hold values from -6 to 6
- position_bias: float32 [169, 12], replicated, may hold values from -4 to 4
- attend_weight: bfloat16 [384, 1152], replicated, may hold values from -0.3125 to 0.3125
- output_weight: bfloat16 [384, 384], replicated, may hold values from -0.3125 to 0.3125
- merge_weight: bfloat16 [1536, 768], replicated, may hold values from -0.15625 to 0.15625
- cotangent: bfloat16 [16, 7, 224, 768], P('frame', None, 'azim'), may hold values from -6 to 6
Outputs:
- merged: bfloat16 [16, 7, 224, 768], P('frame', None, 'azim')
- feature_grad: bfloat16 [16, 14, 448, 384], P('frame', None, 'azim')
- attend_grad: float32 [442368], P(('azim', 'frame'))
- output_grad: float32 [147456], P(('azim', 'frame'))
The draws below stay inside these ranges and needn't reach their ends.
All inputs are finite; a program needn't handle non-finite values.
Results may differ from the reference program's by a relative error of at most 0.0094.
Values may be sent and summed in bfloat16 or wider, within the bound.
A program may use at most 64 MiB of HBM per device.

```python
import jax
import jax.numpy as jnp
from jax import lax

C2 = 384
HEADS2 = 12
C3 = 768
ROWS = 14
COLS = 448
FRAMES = 16


def levels(own_key, dims, cuts, low, top_value):
    level = 1.0
    for dim, blocks in cuts:
        heights = jax.random.uniform(jax.random.fold_in(jax.random.fold_in(own_key, 6), dim), (blocks,), jnp.float32, low / len(cuts), top_value / len(cuts))
        level = level * jnp.repeat(jnp.exp(heights), dims[dim] // blocks).reshape((-1,) + (1,) * (len(dims) - 1 - dim))
    return level


def gaussian(rng, shape, spread, reach, shards=(), held_as=jnp.bfloat16):
    level = levels(rng, shape, shards, -0.22, 0.18) if shards else 1.0
    values = jax.random.normal(rng, shape, jnp.float32) * spread * level
    return jnp.minimum(jnp.maximum(values, -reach), reach).astype(held_as)


def setup_inputs(seed: int = 0) -> dict:
    streams_of = jax.random.split(jax.random.key(seed), 7)
    return {
        "features": gaussian(streams_of[0], (FRAMES, ROWS, COLS, C2), 1.0, 6.0, ((0, 16), (2, 32))),
        "position_bias": gaussian(streams_of[1], (169, HEADS2), 1.0, 4.0, (), jnp.float32),
        "attend_weight": gaussian(streams_of[2], (C2, 3 * C2), C2 ** -0.5, 0.3125),
        "output_weight": gaussian(streams_of[3], (C2, C2), C2 ** -0.5, 0.3125),
        "merge_weight": gaussian(streams_of[4], (4 * C2, C3), (4 * C2) ** -0.5, 0.15625),
        "cotangent": gaussian(streams_of[5], (FRAMES, ROWS // 2, COLS // 2, C3), 1.0, 6.0, ((0, 16), (2, 32))),
    }


def to_windows(grid):
    row_count, col_count, channels = grid.shape
    grid = grid.reshape(row_count // 7, 7, col_count // 7, 7, channels).transpose(0, 2, 1, 3, 4)
    return grid.reshape(row_count // 7, col_count // 7, 49, channels)

def from_windows(blocks, row_count, col_count):
    channels = blocks.shape[-1]
    grid = blocks.reshape(row_count // 7, col_count // 7, 7, 7, channels).transpose(0, 2, 1, 3, 4)
    return grid.reshape(row_count, col_count, channels)

def normalize(values):
    centred = values - lax.optimization_barrier(jnp.mean(values, -1, keepdims=True))
    inverse_std = lax.rsqrt(lax.optimization_barrier(jnp.mean(centred * centred, -1, keepdims=True)) + 1e-05)
    return (centred * inverse_std, inverse_std)

def normalize_back(normed, inverse_std, grads):
    first = lax.optimization_barrier(jnp.mean(grads, -1, keepdims=True))
    second = lax.optimization_barrier(jnp.mean(grads * normed, -1, keepdims=True))
    return inverse_std * (grads - first - normed * second)

def window_bias(position_bias, row_count):
    position = jnp.arange(49)
    pos_row = position // 7
    pos_col = position % 7
    bias_index = (pos_row[:, None] - pos_row[None, :] + 6) * 13 + (pos_col[:, None] - pos_col[None, :] + 6)
    one_hot = (bias_index.reshape(-1)[:, None] == jnp.arange(169)[None, :]).astype(position_bias.dtype)
    pos_bias = jnp.dot(one_hot, position_bias, precision=lax.Precision.HIGHEST)
    pos_bias = pos_bias.reshape(49, 49, -1).transpose(2, 0, 1)
    line_index = jnp.arange(row_count // 7)[:, None] * 7 + pos_row[None, :]
    region = (line_index >= row_count - 7).astype(jnp.int32) + (line_index >= row_count - 3).astype(jnp.int32)
    row_mask = jnp.where(region[:, :, None] == region[:, None, :], 0.0, -100.0).astype(position_bias.dtype)
    return (pos_bias, row_mask)

def merge_quads(grid):
    row_count, col_count, channels = grid.shape
    grid = grid.reshape(row_count // 2, 2, col_count // 2, 2, channels).transpose(0, 2, 3, 1, 4)
    return grid.reshape(row_count // 2, col_count // 2, 4 * channels)

def split_quads(grid, channels):
    half_rows, half_cols, _ = grid.shape
    grid = grid.reshape(half_rows, half_cols, 2, 2, channels).transpose(0, 3, 1, 2, 4)
    return grid.reshape(2 * half_rows, 2 * half_cols, channels)

def attention_forward(rolled, attend_weight, pos_bias, row_mask):
    row_count, col_count, channels = rolled.shape
    head_count = pos_bias.shape[0]
    head_size = channels // head_count
    projected = jnp.dot(rolled.reshape(-1, channels), attend_weight, preferred_element_type=jnp.float32)
    projected = projected.astype(jnp.bfloat16).reshape(row_count, col_count, 3 * channels)
    blocks = to_windows(projected)
    head_shape = blocks.shape[:3] + (head_count, head_size)
    queries = blocks[..., :channels].reshape(head_shape).astype(jnp.float32)
    key_block = blocks[..., channels:2 * channels].reshape(head_shape).astype(jnp.float32)
    value_block = blocks[..., 2 * channels:].reshape(head_shape).astype(jnp.float32)
    scores = jnp.einsum('abqhd,abkhd->abhqk', queries, key_block) * head_size ** (-0.5)
    scores = scores + pos_bias[None, None] + row_mask[:, None, None]
    probs = jax.nn.softmax(scores, -1)
    probs16 = probs.astype(jnp.bfloat16)
    attended = jnp.einsum('abhqk,abkhd->abqhd', probs16.astype(jnp.float32), value_block)
    attended = attended.astype(jnp.bfloat16).reshape(head_shape[:3] + (channels,))
    return (from_windows(attended, row_count, col_count), (queries, key_block, value_block, probs, probs16))

def attention_backward(attended_grad, saved, head_size):
    queries, key_block, value_block, probs, probs16 = saved
    row_count, col_count, channels = attended_grad.shape
    outer = to_windows(attended_grad).reshape(queries.shape).astype(jnp.float32)
    value_grad = jnp.einsum('abhqk,abqhd->abkhd', probs16.astype(jnp.float32), outer)
    score_grad = jnp.einsum('abqhd,abkhd->abhqk', outer, value_block)
    soft_grad = probs * (score_grad - lax.optimization_barrier(jnp.sum(probs * score_grad, -1, keepdims=True))) * head_size ** (-0.5)
    soft16 = soft_grad.astype(jnp.bfloat16).astype(jnp.float32)
    query_grad = jnp.einsum('abhqk,abkhd->abqhd', soft16, key_block)
    key_grad = jnp.einsum('abhqk,abqhd->abkhd', soft16, queries)
    flat_shape = queries.shape[:3] + (channels,)
    joined = jnp.concatenate([query_grad.reshape(flat_shape), key_grad.reshape(flat_shape), value_grad.reshape(flat_shape)], -1)
    return from_windows(joined.astype(jnp.bfloat16), row_count, col_count)

def token_product(left, right):
    return lax.dot_general(left.reshape(-1, left.shape[-1]), right.reshape(-1, right.shape[-1]), (((0,), (0,)), ((), ())), preferred_element_type=jnp.float32)

def frame_pass(features, cotangent, attend_weight, output_weight, merge_weight, pos_bias, row_mask):
    row_count, col_count, channels = features.shape
    head_size = channels // pos_bias.shape[0]
    normed, inverse_std = normalize(features.astype(jnp.float32))
    normed = jnp.roll(normed, (-3, -3), (0, 1))
    inverse_std = jnp.roll(inverse_std, (-3, -3), (0, 1))
    rolled = normed.astype(jnp.bfloat16)
    attended, saved = attention_forward(rolled, attend_weight, pos_bias, row_mask)
    branch = jnp.dot(attended.reshape(-1, channels), output_weight, preferred_element_type=jnp.float32)
    branch = jnp.roll(branch.reshape(row_count, col_count, channels), (3, 3), (0, 1))
    hidden = (features.astype(jnp.float32) + branch).astype(jnp.bfloat16)
    quad_normed, quad_std = normalize(merge_quads(hidden).astype(jnp.float32))
    quad16 = quad_normed.astype(jnp.bfloat16)
    out_width = merge_weight.shape[1]
    merged = jnp.dot(quad16.reshape(-1, 4 * channels), merge_weight, preferred_element_type=jnp.float32)
    merged = merged.astype(jnp.bfloat16).reshape(row_count // 2, col_count // 2, out_width)
    quad_grad_in = jnp.dot(cotangent.reshape(-1, out_width), merge_weight.T, preferred_element_type=jnp.float32)
    quad_grad = normalize_back(quad_normed, quad_std, quad_grad_in.reshape(quad_normed.shape))
    hidden_grad = split_quads(quad_grad, channels).astype(jnp.bfloat16)
    branch_grad = jnp.roll(hidden_grad, (-3, -3), (0, 1))
    output_grad = token_product(attended, branch_grad)
    attended_grad = jnp.dot(branch_grad.reshape(-1, channels), output_weight.T, preferred_element_type=jnp.float32)
    attended_grad = attended_grad.astype(jnp.bfloat16).reshape(row_count, col_count, channels)
    projected_grad = attention_backward(attended_grad, saved, head_size)
    attend_grad = token_product(rolled, projected_grad)
    normed_grad = jnp.dot(projected_grad.reshape(-1, 3 * channels), attend_weight.T, preferred_element_type=jnp.float32)
    rolled_grad = normalize_back(normed, inverse_std, normed_grad.reshape(row_count, col_count, channels))
    rolled_grad = jnp.roll(rolled_grad, (3, 3), (0, 1))
    feature_grad = (hidden_grad.astype(jnp.float32) + rolled_grad).astype(jnp.bfloat16)
    return (merged, feature_grad, attend_grad, output_grad)

def reference(features, position_bias, attend_weight, output_weight, merge_weight, cotangent):
    pos_bias, row_mask = window_bias(position_bias, ROWS)

    def one_frame(pair):
        return frame_pass(pair[0], pair[1], attend_weight, output_weight, merge_weight, pos_bias, row_mask)
    merged, feature_grad, attend_grad, output_grad = lax.map(one_frame, (features, cotangent))
    return (merged, feature_grad, lax.optimization_barrier(jnp.sum(attend_grad, 0)).reshape(-1), lax.optimization_barrier(jnp.sum(output_grad, 0)).reshape(-1))
```

```python
import functools

import jax
import jax.numpy as jnp
import ml_dtypes
import numpy as np
from jax import lax
from jax.experimental import pallas as pl
from jax.experimental.pallas import tpu as pltpu
from jax.sharding import Mesh
from jax.sharding import PartitionSpec as P

AZIM = ("azim_0", "azim_1")
AZIM_FRAME = ("azim_0", "azim_1", "frame_0", "frame_1", "frame_2")
FRAME = ("frame_0", "frame_1", "frame_2")

BF = jnp.bfloat16
F32 = jnp.float32
C = 384
OUT = 768
GROUPS = 3
SCALE = 32 ** (-0.5)
WINDOWS = ((0, 1), (1, 1), (0, 0), (1, 0))


def position_row(row, col):
    return 4 * row + col if col < 4 else 32 + 3 * row + col - 4


def east_row(row, col):
    rolled = (row - 3) % 14
    return 32 * (rolled // 7) + 3 * (rolled % 7) + col


@functools.cache
def tables():
    to_window = np.zeros((256, 224), np.float32)
    for a in range(2):
        for b in range(2):
            for row in range(7):
                for col in range(7):
                    frame_row, frame_col = (7 * a + row + 3) % 14, 7 * b + col + 3
                    if frame_col >= 14:
                        continue
                    at = position_row(row, col)
                    line = 64 * a + at if b == 0 else 128 + 32 * a + at
                    to_window[line, 16 * frame_row + frame_col] = 1
    for row in range(14):
        for col in range(3):
            to_window[192 + east_row(row, col), 16 * row + col] = 1
    to_quad = np.zeros((256, 224), np.float32)
    for block in range(4):
        for i in range(7):
            for j in range(7):
                token = 16 * (2 * i + block % 2) + 2 * j + block // 2
                to_quad[64 * block + 8 * i + j, token] = 1
    window_to_quad = to_quad @ to_window.T
    rows = np.zeros((C, C), np.float32)
    for c in range(2):
        for xi in range(4):
            for k in range(3):
                for z in range(16):
                    rows[192 * c + 48 * xi + 16 * k + z, 24 * z + 6 * xi + 3 * c + k] = 1
    index = np.full((64, 64), 255.0, np.float32)
    mask = np.zeros((2, 64, 64), np.float32)
    valid = np.zeros(64, bool)
    for row in range(7):
        for col in range(7):
            p = position_row(row, col)
            valid[p] = True
            for row_q in range(7):
                for col_q in range(7):
                    q = position_row(row_q, col_q)
                    index[p, q] = 13 * (row - row_q + 6) + col - col_q + 6
                    if (row < 4) != (row_q < 4):
                        mask[1, p, q] = -100.0
    mask[:, :, ~valid] = -1e30
    mask = np.concatenate([mask, mask], -1)
    bf = ml_dtypes.bfloat16
    return (
        to_window.astype(bf),
        np.ascontiguousarray(to_window.T).astype(bf),
        to_quad.astype(bf),
        np.ascontiguousarray(to_quad.T).astype(bf),
        window_to_quad.astype(bf),
        np.ascontiguousarray(window_to_quad.T).astype(bf),
        rows.astype(bf),
        index.reshape(32, 128),
        mask,
    )


def mm(left, right):
    return lax.dot_general(left, right, (((1,), (0,)), ((), ())), preferred_element_type=F32)


def mm_t(left, right):
    return lax.dot_general(left, right, (((1,), (1,)), ((), ())), preferred_element_type=F32)


def t_mm(left, right):
    return lax.dot_general(left, right, (((0,), (0,)), ((), ())), preferred_element_type=F32)


def normalize(values):
    centred = values - jnp.mean(values, -1, keepdims=True)
    inverse_std = lax.rsqrt(jnp.mean(centred * centred, -1, keepdims=True) + 1e-05)
    return centred * inverse_std, inverse_std


def normalize_back(normed, inverse_std, grads):
    first = jnp.mean(grads, -1, keepdims=True)
    second = jnp.mean(grads * normed, -1, keepdims=True)
    return inverse_std * (grads - first - normed * second)


def window_of(values, a, b):
    if b == 0:
        return values[64 * a : 64 * a + 64]
    near, far = 128 + 32 * a, 192 + 32 * a
    return jnp.concatenate([values[near : near + 32], values[far : far + 32]], 0)


def put_window(ref, a, b, lanes, values):
    if b == 0:
        ref[64 * a : 64 * a + 64, lanes] = values
    else:
        near, far = 128 + 32 * a, 192 + 32 * a
        ref[near : near + 32, lanes] = values[:32]
        ref[far : far + 32, lanes] = values[32:]


def get_window(ref, a, b, lanes):
    if b == 0:
        return ref[64 * a : 64 * a + 64, lanes]
    near, far = 128 + 32 * a, 192 + 32 * a
    return jnp.concatenate([ref[near : near + 32, lanes], ref[far : far + 32, lanes]], 0)


def halves(op, empty, low, values):
    first = op(jnp.where(low, values, empty), -1, keepdims=True)
    second = op(jnp.where(low, empty, values), -1, keepdims=True)
    return jnp.where(low, first, second)


NAMES = (
    "feat", "cot", "pos", "w_attend", "w_out", "w_merge", "to_window", "to_window_t", "to_quad",
    "to_quad_t", "win_quad", "win_quad_t", "row_pick", "index", "mask",
)
ORDER = (
    "feat", "to_window", "w_attend", "pos", "index", "mask", "cot", "w_merge", "row_pick",
    "to_quad", "win_quad", "w_out", "win_quad_t", "to_quad_t", "to_window_t",
)
N_IN = len(NAMES)


def kernel(scatter, *refs):
    given, refs = refs[:N_IN], refs[N_IN:]
    merged_ref, grad_ref, share_ref = refs[:3]
    if scatter:
        refs = refs[3:]
    else:
        local_ref, refs = refs[3], refs[4:]
    held, refs = refs[:N_IN], refs[N_IN:]
    (
        x_scr, cot_scr, table_scr, bias_a, bias_b, normed_scr, std_scr,
        normed_east, std_east, qkv, probs, attended, branch_grad, outer, proj_grad,
        hidden_grad, left_o, left_r, feature_scr,
        ex_send, ex_recv,
        g_own, g_send, g_recv, x_own, x_send, x_recv, y_send, y_recv, z_line, z_send, z_recv,
        in_sem, ex_ssem, ex_rsem, c_ssem, c_rsem, x_ssem, x_rsem, y_ssem, y_rsem,
        z_ssem, z_rsem, near_sem,
    ) = refs
    (
        feat, cot, pos, w_attend, w_out, w_merge, to_window, to_window_t, to_quad, to_quad_t,
        win_quad, win_quad_t, row_pick, index, mask,
    ) = held
    copies = {
        name: pltpu.make_async_copy(given[i], held[i], in_sem.at[i])
        for i, name in enumerate(NAMES)
    }
    for name in ORDER:
        copies[name].start()

    z, x_lo = lax.axis_index("azim_0"), lax.axis_index("azim_1")
    x_hi, y, core = (lax.axis_index(name) for name in FRAME)
    n_z = lax.axis_size("azim_0")
    n_azim = n_z * 2
    azim = 2 * z + x_lo
    east, west = (azim + 1) % n_azim, (azim + n_azim - 1) % n_azim
    east_id = {"azim_0": east // 2, "azim_1": east % 2}
    west_id = {"azim_0": west // 2, "azim_1": west % 2}
    xi = 2 * x_lo + x_hi

    def x_id(step):
        other = (xi + step) % 4
        return {"azim_1": other // 2, "frame_0": other % 2}

    def z_id(step):
        return {"azim_0": (z + n_z + step) % n_z}

    barrier = pltpu.get_barrier_semaphore()
    near = [east_id, west_id]
    if scatter:
        near += [{"frame_2": 1 - core}]
        near += [x_id(step) for step in (1, 2, 3)]
        near += [{"frame_1": (y + step) % 4} for step in (1, 2, 3)]
        near += [{"frame_1": (y + step) % 4, "frame_2": 1 - core} for step in (1, 2, 3)]
        near += [z_id(1), z_id(-1)]
    for device in near:
        pl.semaphore_signal(barrier, inc=1, device_id=device)

    def exchange(i, device):
        return pltpu.make_async_remote_copy(
            src_ref=ex_send.at[i], dst_ref=ex_recv.at[i], send_sem=ex_ssem.at[i],
            recv_sem=ex_rsem.at[i], device_id=device,
        )

    copies["feat"].wait()
    x_scr[...] = jnp.zeros_like(x_scr)
    for row in range(14):
        x_scr[row, 0:14, :] = feat[row].astype(F32)
    tokens = x_scr[...].reshape(224, C)
    tokens16 = tokens.astype(BF)
    copies["to_window"].wait()
    ex_send[0] = mm(to_window[192:256], tokens16).astype(BF)
    pl.semaphore_wait(barrier, len(near))
    exchange(0, west_id).start()
    if scatter:
        for step in (1, -1):
            pl.semaphore_signal(near_sem.at[0], inc=1, device_id=z_id(step))

    def widen_reach(i):
        if not scatter:
            return
        pl.semaphore_wait(near_sem.at[i], 2)
        if i < 2:
            for step in (2 ** (i + 1), -(2 ** (i + 1))):
                pl.semaphore_signal(near_sem.at[i + 1], inc=1, device_id=z_id(step))

    normed, inverse_std = normalize(tokens)
    normed_scr[...] = normed
    std_scr[...] = inverse_std
    rolled_own = mm(to_window[0:192], normed.astype(BF)).astype(BF)
    copies["w_attend"].wait()
    qkv[0:192] = mm(rolled_own, w_attend[...]).astype(BF)

    copies["pos"].wait()
    copies["index"].wait()
    copies["mask"].wait()
    table_scr[...] = jnp.zeros_like(table_scr)
    table_scr[0:12, 0:169] = pos[...]
    table = table_scr[...]
    high = table.astype(BF).astype(F32)
    both = jnp.concatenate([high, table - high], 0).astype(BF)
    lane = lax.broadcasted_iota(jnp.int32, (1, 128), 1)
    entry = lax.broadcasted_iota(jnp.int32, (256, 128), 0).astype(F32)
    for t in range(0, 32, 4):
        picks = [
            jnp.where(entry == index[u : u + 1, :], 1.0, 0.0).astype(BF) for u in range(t, t + 4)
        ]
        wide = mm(both, jnp.concatenate(picks, 1))
        for u in range(4):
            part = wide[:, 128 * u : 128 * u + 128]
            part = part[0:16] + part[16:32]
            turned = pltpu.roll(part, 64, 1)
            p = 2 * (t + u)
            bias_a[pl.ds(p, 16, stride=64), :] = part
            bias_a[pl.ds(p + 1, 16, stride=64), :] = turned
            bias_b[pl.ds(p, 16, stride=64), :] = turned
            bias_b[pl.ds(p + 1, 16, stride=64), :] = part
    low = lane < 64

    def pair_bias(pair):
        first = bias_a[128 * pair : 128 * pair + 64, :]
        second = bias_b[128 * pair + 64 : 128 * pair + 128, :]
        return jnp.where(low, first, second)

    copies["cot"].wait()
    cot_scr[...] = jnp.zeros_like(cot_scr)
    for row in range(7):
        cot_scr[row, 0:7, :] = cot[row].astype(F32)
    copies["w_merge"].wait()
    quad_grad_in = mm_t(cot_scr[...].reshape(64, OUT).astype(BF), w_merge[...])

    exchange(0, west_id).wait()
    widen_reach(0)
    normed, inverse_std = normalize(ex_recv[0].astype(F32))
    normed_east[...] = normed
    std_east[...] = inverse_std
    rolled_east = normed.astype(BF)
    qkv[192:256] = mm(rolled_east, w_attend[...]).astype(BF)

    head_lanes = [(lane // 32 == h).astype(F32).astype(BF) for h in range(4)]

    def spread(block):
        return jnp.concatenate([block * head_lanes[h] for h in range(4)], 0)

    def heads_of(wide):
        total = wide[0:64] * head_lanes[0].astype(F32)
        for h in range(1, 4):
            total = total + wide[64 * h : 64 * h + 64] * head_lanes[h].astype(F32)
        return total

    def group_lanes(kind, group):
        start = C * kind + 128 * group
        return slice(start, start + 128)

    def units_of(windows):
        return [(w, group) for w in windows for group in range(GROUPS)]

    def of_window(ref, w, kind, group):
        return get_window(ref, *WINDOWS[w], group_lanes(kind, group))

    ones = (lax.broadcasted_iota(jnp.int32, (128, 128), 0) < 64) == low
    ones = ones.astype(F32).astype(BF)

    def half_sums(values):
        joined = jnp.concatenate(values, 0)
        high = joined.astype(BF)
        rest = (joined - high.astype(F32)).astype(BF)
        total = mm(high, ones) + mm(rest, ones)
        return [total[64 * i : 64 * i + 64] for i in range(len(values))]

    def split_halves(wide):
        return [part[:, 128 * i : 128 * i + 128] for part in wide for i in range(2)]

    def join_halves(parts):
        return [
            jnp.concatenate([parts[i].astype(BF), parts[i + 1].astype(BF)], 1)
            for i in range(0, len(parts), 2)
        ]

    def attend(*windows):
        units = units_of(windows)
        scores = [
            mm_t(of_window(qkv, w, 0, g), spread(of_window(qkv, w, 1, g))) for w, g in units
        ]
        parts = split_halves(scores)
        for i, (w, g) in enumerate(units):
            for j in range(2):
                bias = pair_bias(2 * g + j) + mask[WINDOWS[w][0]]
                parts[2 * i + j] = parts[2 * i + j] * SCALE + bias
        tops = [halves(jnp.max, -3e38, low, part) for part in parts]
        parts = [jnp.exp(part - top) for part, top in zip(parts, tops)]
        sums = half_sums(parts)
        parts = [part * (1.0 / total) for part, total in zip(parts, sums)]
        for i, (w, g) in enumerate(units):
            for j in range(2):
                probs[GROUPS * w + g, :, 128 * j : 128 * j + 128] = parts[2 * i + j]
        for (w, g), prob in zip(units, join_halves(parts)):
            result = mm(prob, spread(of_window(qkv, w, 2, g))).astype(BF)
            put_window(attended, *WINDOWS[w], group_lanes(0, g), result)

    attend(0, 1)
    ex_send[1] = attended[192:256]
    exchange(1, east_id).start()
    attend(2, 3)
    copies["row_pick"].wait()
    left_r[:, 0:192] = mm_t(row_pick[...], rolled_own).astype(BF)
    left_r[:, 192:256] = mm_t(row_pick[...], rolled_east).astype(BF)
    left_o[...] = mm_t(row_pick[...], attended[...]).astype(BF)
    copies["to_quad"].wait()
    copies["win_quad"].wait()
    copies["w_out"].wait()
    features_quad = mm(to_quad[...], tokens16)
    exchange(1, east_id).wait()
    widen_reach(1)

    extended = jnp.concatenate([attended[0:192], ex_recv[1]], 0)
    attended_quad = mm(win_quad[...], extended).astype(BF)
    hidden = (features_quad + mm(attended_quad, w_out[...])).astype(BF).astype(F32)
    quads = [hidden[64 * e : 64 * e + 64] for e in range(4)]

    def mean(blocks):
        total = (blocks[0] + blocks[1]) + (blocks[2] + blocks[3])
        return jnp.sum(total, -1, keepdims=True) * (1.0 / (4 * C))

    centre = mean(quads)
    quads = [quad - centre for quad in quads]
    quad_std = lax.rsqrt(mean([quad * quad for quad in quads]) + 1e-05)
    quads = [quad * quad_std for quad in quads]
    grads = [quad_grad_in[:, C * e : C * e + C] for e in range(4)]
    first = mean(grads)
    second = mean([grad * quad for grad, quad in zip(grads, quads)])
    for e in range(4):
        value = quad_std * (grads[e] - first - quads[e] * second)
        hidden_grad[64 * e : 64 * e + 64] = value.astype(BF)
    copies["win_quad_t"].wait()
    ex_send[2] = mm(win_quad_t[192:256], hidden_grad[...]).astype(BF)
    exchange(2, west_id).start()
    own_grad = mm(win_quad_t[0:192], hidden_grad[...]).astype(BF)
    branch_grad[0:192] = own_grad
    outer[0:192] = mm_t(own_grad, w_out[...]).astype(BF)
    merged = mm(jnp.concatenate([quad.astype(BF) for quad in quads], 1), w_merge[...])
    for i in range(7):
        merged_ref[i] = merged[8 * i : 8 * i + 7].astype(BF)
    copies["to_quad_t"].wait()
    hidden_own = mm(to_quad_t[...], hidden_grad[...])

    def values_back(*windows):
        units = units_of(windows)
        wide = [
            t_mm(probs[GROUPS * w + g].astype(BF), of_window(outer, w, 0, g)) for w, g in units
        ]
        for (w, g), value in zip(units, wide):
            back = heads_of(value).astype(BF)
            put_window(proj_grad, *WINDOWS[w], group_lanes(2, g), back)

    def scores_back(*windows):
        units = units_of(windows)
        wide = [
            mm_t(of_window(outer, w, 0, g), spread(of_window(qkv, w, 2, g))) for w, g in units
        ]
        grads = split_halves(wide)
        prob = split_halves([probs[GROUPS * w + g] for w, g in units])
        sums = half_sums([p * grad for p, grad in zip(prob, grads)])
        parts = [p * (grad - total) * SCALE for p, grad, total in zip(prob, grads, sums)]
        soft = join_halves(parts)
        wide = [t_mm(part, of_window(qkv, w, 0, g)) for (w, g), part in zip(units, soft)]
        for (w, g), part in zip(units, soft):
            back = mm(part, spread(of_window(qkv, w, 1, g))).astype(BF)
            put_window(proj_grad, *WINDOWS[w], group_lanes(0, g), back)
        for (w, g), value in zip(units, wide):
            back = heads_of(value).astype(BF)
            put_window(proj_grad, *WINDOWS[w], group_lanes(1, g), back)

    def core_copy(i):
        return pltpu.make_async_remote_copy(
            src_ref=g_send.at[i, 1 - core], dst_ref=g_recv.at[i], send_sem=c_ssem.at[i],
            recv_sem=c_rsem.at[i], device_id={"frame_2": 1 - core},
        )

    def start_core(i, product):
        product = product.reshape(2, 192, C)
        g_own[i] = product
        if scatter:
            g_send[i] = product.astype(BF)
            core_copy(i).start()

    def x_copy(i, step):
        return pltpu.make_async_remote_copy(
            src_ref=x_send.at[i, (xi + step) % 4], dst_ref=x_recv.at[i, step - 1],
            send_sem=x_ssem.at[i, step - 1], recv_sem=x_rsem.at[i, step - 1],
            device_id=x_id(step),
        )

    def start_x(i):
        if not scatter:
            return
        core_copy(i).wait()
        total = (g_own[i, core] + g_recv[i].astype(F32)).reshape(4, 48, C)
        x_own[i] = total
        x_send[i] = total.astype(BF)
        for step in (2, 1, 3):
            x_copy(i, step).start()

    def end_x(i):
        for step in (1, 2, 3):
            x_copy(i, step).wait()
        total = x_own[i, xi]
        for step in (1, 2, 3):
            total = total + x_recv[i, step - 1].astype(F32)
        return total

    scores_back(2, 3)
    exchange(2, west_id).wait()
    widen_reach(2)
    branch_grad[192:256] = ex_recv[2]
    outer[192:256] = mm_t(ex_recv[2], w_out[...]).astype(BF)
    start_core(0, mm(left_o[...], branch_grad[...]))
    values_back(0, 1, 2, 3)
    start_core(1, mm(left_r[...], proj_grad[:, 2 * C : 3 * C]))
    start_x(0)
    scores_back(0, 1)
    start_x(1)
    start_core(2, mm(left_r[...], proj_grad[:, 0:C]))
    start_core(3, mm(left_r[...], proj_grad[:, C : 2 * C]))
    east_grad = mm_t(proj_grad[192:256], w_attend[...])
    east_grad = normalize_back(normed_east[...], std_east[...], east_grad)
    ex_send[3] = east_grad.astype(BF)
    exchange(3, east_id).start()
    start_x(2)
    start_x(3)
    copies["to_window_t"].wait()
    own_proj = mm(to_window_t[:, 0:192], proj_grad[0:192]).astype(BF)
    own_grad = mm_t(own_proj, w_attend[...])
    own_grad = normalize_back(normed_scr[...], std_scr[...], own_grad)
    feature_scr[...] = hidden_own + own_grad

    def end_features():
        exchange(3, east_id).wait()
        grad = feature_scr[...] + mm(to_window_t[:, 192:256], ex_recv[3])
        grad = grad.reshape(14, 16, C)
        for row in range(14):
            grad_ref[row] = grad[row, 0:14].astype(BF)

    if not scatter:
        end_features()
        share_ref[...] = jnp.zeros_like(share_ref)
        local_ref[...] = g_own[...]
        return

    output_sum, values_sum = end_x(0), end_x(1)
    queries_sum, keys_sum = end_x(2), end_x(3)
    joined = jnp.concatenate([queries_sum, keys_sum, values_sum], 1)
    quarters = [
        joined[:, 0:384],
        pltpu.roll(joined[:, 256:768], 512 - 32, 1)[:, 0:384],
        pltpu.roll(joined[:, 512:1024], 512 - 64, 1)[:, 0:384],
        pltpu.roll(joined[:, 768:1152], 384 - 96, 1),
    ]
    pieces = [
        output_sum[:, 0:128],
        pltpu.roll(output_sum[:, 0:256], 256 - 96, 1)[:, 0:128],
        pltpu.roll(output_sum[:, 128:384], 256 - 64, 1)[:, 0:128],
        pltpu.roll(output_sum[:, 256:384], 128 - 32, 1),
    ]
    for m in range(4):
        for i in range(3):
            k, t = divmod(3 * m + i, 4)
            rows = slice(16 * k, 16 * k + 16)
            y_send[m, :, 384 * i : 384 * i + 384] = quarters[t][rows].astype(BF)
            lanes = slice(1152 + 128 * i, 1280 + 128 * i)
            y_send[m, :, lanes] = pieces[t][rows].astype(BF)

    def y_copy(m):
        return pltpu.make_async_remote_copy(
            src_ref=y_send.at[m], dst_ref=y_recv.at[y], send_sem=y_ssem.at[m],
            recv_sem=y_rsem.at[y],
            device_id={"frame_1": 2 * core + m // 2, "frame_2": m % 2},
        )

    def y_landed(source):
        return pltpu.make_async_remote_copy(
            src_ref=y_send.at[0], dst_ref=y_recv.at[source], send_sem=y_ssem.at[0],
            recv_sem=y_rsem.at[source], device_id={"frame_2": 1 - core},
        )

    for m in range(4):
        mine = jnp.logical_and(2 * core + m // 2 == y, core == m % 2)

        @pl.when(mine)
        def _():
            y_recv[y] = y_send[m]

        @pl.when(jnp.logical_not(mine))
        def _():
            y_copy(m).start()

    for source in range(4):
        mine = jnp.logical_and(y == source, y // 2 == core)

        @pl.when(jnp.logical_not(mine))
        def _():
            y_landed(source).wait_recv()

    total = y_recv[0].astype(F32)
    for source in range(1, 4):
        total = total + y_recv[source].astype(F32)
    for t in range(12):
        z_line[pl.ds(t, 16, stride=16), :] = total[:, 128 * t : 128 * t + 128]
    for t in range(12, 16):
        z_line[pl.ds(t, 16, stride=16), :] = jnp.zeros((16, 128), F32)
    z_send[...] = z_line[...].reshape(16, 16, 128).astype(BF)

    def z_copy(step):
        return pltpu.make_async_remote_copy(
            src_ref=z_send.at[(z + step) % 16], dst_ref=z_recv.at[step - 1],
            send_sem=z_ssem.at[step - 1], recv_sem=z_rsem.at[step - 1], device_id=z_id(step),
        )

    steps = sorted(range(1, 16), key=lambda step: -min(step, 16 - step))
    for step in steps:
        z_copy(step).start()
    end_features()
    for m in range(4):
        mine = jnp.logical_and(2 * core + m // 2 == y, core == m % 2)

        @pl.when(jnp.logical_not(mine))
        def _():
            y_copy(m).wait_send()

    total = z_send[z].astype(F32)
    for step in steps[::-1]:
        z_copy(step).wait()
        total = total + z_recv[step - 1].astype(F32)
    share_ref[...] = total


def finish(merged_in, grad_in, share, merged_ref, grad_ref, attend_ref, output_ref):
    merged_ref[0] = merged_in[...]
    grad_ref[0] = grad_in[...]
    lane = lax.broadcasted_iota(jnp.int32, (1, 128), 1)

    def row(i, turn=0):
        value = share[i : i + 1, :]
        return pltpu.roll(value, turn, 1) if turn else value

    one = [row(i, 32) for i in (3, 4, 5)]
    two = [row(i, 64) for i in (6, 7, 8)]
    low, half = lane < 32, lane < 64
    attend = [
        row(0),
        row(1),
        jnp.where(low, row(2), one[0]),
        jnp.where(low, one[0], one[1]),
        jnp.where(low, one[1], jnp.where(half, one[2], two[0])),
        jnp.where(half, two[0], two[1]),
        jnp.where(half, two[1], two[2]),
    ]
    middle, last = row(10, 96), row(11, 64)
    output = [jnp.where(lane < 96, row(9), middle), jnp.where(half, middle, last), last]
    for ref, rows in ((attend_ref, attend), (output_ref, output)):
        for i, value in enumerate(rows):
            count = min(128, ref.shape[0] - 128 * i)
            ref[128 * i : 128 * i + count] = value.reshape(128)[:count]


def local_call(scatter, features, position_bias, attend_weight, output_weight, merge_weight, cotangent):
    given = (features[0], cotangent[0], position_bias.T, attend_weight, output_weight, merge_weight)
    given = given + tuple(jnp.asarray(table) for table in tables())
    dma = pltpu.SemaphoreType.DMA
    scratch = [pltpu.VMEM(a.shape, a.dtype) for a in given]
    scratch += [
        pltpu.VMEM((14, 16, C), F32),
        pltpu.VMEM((8, 8, OUT), F32),
        pltpu.VMEM((16, 256), F32),
        pltpu.VMEM((1024, 128), F32),
        pltpu.VMEM((1024, 128), F32),
        pltpu.VMEM((224, C), F32),
        pltpu.VMEM((224, 1), F32),
        pltpu.VMEM((64, C), F32),
        pltpu.VMEM((64, 1), F32),
        pltpu.VMEM((256, 3 * C), BF),
        pltpu.VMEM((12, 64, 256), F32),
        pltpu.VMEM((256, C), BF),
        pltpu.VMEM((256, C), BF),
        pltpu.VMEM((256, C), BF),
        pltpu.VMEM((256, 3 * C), BF),
        pltpu.VMEM((256, C), BF),
        pltpu.VMEM((C, 256), BF),
        pltpu.VMEM((C, 256), BF),
        pltpu.VMEM((224, C), F32),
        pltpu.VMEM((4, 64, C), BF),
        pltpu.VMEM((4, 64, C), BF),
        pltpu.VMEM((4, 2, 192, C), F32),
        pltpu.VMEM((4, 2, 192, C), BF),
        pltpu.VMEM((4, 192, C), BF),
        pltpu.VMEM((4, 4, 48, C), F32),
        pltpu.VMEM((4, 4, 48, C), BF),
        pltpu.VMEM((4, 3, 48, C), BF),
        pltpu.VMEM((4, 16, 1536), BF),
        pltpu.VMEM((4, 16, 1536), BF),
        pltpu.VMEM((256, 128), F32),
        pltpu.VMEM((16, 16, 128), BF),
        pltpu.VMEM((15, 16, 128), BF),
        dma((N_IN,)), dma((4,)), dma((4,)), dma((4,)), dma((4,)), dma((4, 3)), dma((4, 3)),
        dma((4,)), dma((4,)), dma((15,)), dma((15,)), pltpu.SemaphoreType.REGULAR((3,)),
    ]
    vmem = pl.BlockSpec(memory_space=pltpu.VMEM)
    return pl.pallas_call(
        functools.partial(kernel, scatter),
        out_shape=(
            jax.ShapeDtypeStruct((7, 7, OUT), BF),
            jax.ShapeDtypeStruct((14, 14, C), BF),
            jax.ShapeDtypeStruct((16, 128), F32),
        )
        + (() if scatter else (jax.ShapeDtypeStruct((4, 2, 192, C), F32),)),
        in_specs=[pl.BlockSpec(memory_space=pl.ANY)] * N_IN,
        out_specs=(vmem,) * (3 if scatter else 4),
        scratch_shapes=scratch,
        compiler_params=pltpu.CompilerParams(collective_id=0, has_side_effects=True),
    )(*given)


def per_device(*arrays):
    merged, feature_grad, share = local_call(True, *arrays)
    vmem = pl.BlockSpec(memory_space=pltpu.VMEM)
    return pl.pallas_call(
        finish,
        out_shape=(
            jax.ShapeDtypeStruct((1, *merged.shape), BF),
            jax.ShapeDtypeStruct((1, *feature_grad.shape), BF),
            jax.ShapeDtypeStruct((864,), F32),
            jax.ShapeDtypeStruct((288,), F32),
        ),
        in_specs=(vmem,) * 3,
        out_specs=(vmem,) * 4,
    )(merged, feature_grad, share)


def solution(mesh):
    split = Mesh(mesh.devices.reshape(16, 2, 2, 4, 2), AZIM_FRAME)
    placed = (P(FRAME, None, AZIM, None), P(), P(), P(), P(), P(FRAME, None, AZIM, None))
    return jax.shard_map(
        per_device,
        mesh=split,
        in_specs=placed,
        out_specs=(
            P(FRAME, None, AZIM, None),
            P(FRAME, None, AZIM, None),
            P(AZIM_FRAME),
            P(AZIM_FRAME),
        ),
        check_vma=False,
    )
```

```python
import functools

import jax
import jax.numpy as jnp
import ml_dtypes
import numpy as np
from jax import lax
from jax.experimental import pallas as pl
from jax.experimental.pallas import tpu as pltpu
from jax.sharding import Mesh
from jax.sharding import PartitionSpec as P

AZIM = ("azim_0", "azim_1")
AZIM_FRAME = ("azim_0", "azim_1", "frame_0", "frame_1", "frame_2")
FRAME = ("frame_0", "frame_1", "frame_2")

BF = jnp.bfloat16
F32 = jnp.float32
C = 384
OUT = 768
GROUPS = 3
SCALE = 32 ** (-0.5)
WINDOWS = ((0, 1), (1, 1), (0, 0), (1, 0))


def position_row(row, col):
    return 4 * row + col if col < 4 else 32 + 3 * row + col - 4


def east_row(row, col):
    rolled = (row - 3) % 14
    return 32 * (rolled // 7) + 3 * (rolled % 7) + col


@functools.cache
def tables():
    to_window = np.zeros((256, 224), np.float32)
    for a in range(2):
        for b in range(2):
            for row in range(7):
                for col in range(7):
                    frame_row, frame_col = (7 * a + row + 3) % 14, 7 * b + col + 3
                    if frame_col >= 14:
                        continue
                    at = position_row(row, col)
                    line = 64 * a + at if b == 0 else 128 + 32 * a + at
                    to_window[line, 16 * frame_row + frame_col] = 1
    for row in range(14):
        for col in range(3):
            to_window[192 + east_row(row, col), 16 * row + col] = 1
    to_quad = np.zeros((256, 224), np.float32)
    for block in range(4):
        for i in range(7):
            for j in range(7):
                token = 16 * (2 * i + block % 2) + 2 * j + block // 2
                to_quad[64 * block + 8 * i + j, token] = 1
    window_to_quad = to_quad @ to_window.T
    rows = np.zeros((C, C), np.float32)
    for c in range(2):
        for xi in range(4):
            for k in range(3):
                for z in range(16):
                    rows[192 * c + 48 * xi + 16 * k + z, 24 * z + 6 * xi + 3 * c + k] = 1
    index = np.full((64, 64), 255.0, np.float32)
    mask = np.zeros((2, 64, 64), np.float32)
    valid = np.zeros(64, bool)
    for row in range(7):
        for col in range(7):
            p = position_row(row, col)
            valid[p] = True
            for row_q in range(7):
                for col_q in range(7):
                    q = position_row(row_q, col_q)
                    index[p, q] = 13 * (row - row_q + 6) + col - col_q + 6
                    if (row < 4) != (row_q < 4):
                        mask[1, p, q] = -100.0
    mask[:, :, ~valid] = -1e30
    mask = np.concatenate([mask, mask], -1)
    bf = ml_dtypes.bfloat16
    return (
        to_window.astype(bf),
        np.ascontiguousarray(to_window.T).astype(bf),
        to_quad.astype(bf),
        np.ascontiguousarray(to_quad.T).astype(bf),
        window_to_quad.astype(bf),
        np.ascontiguousarray(window_to_quad.T).astype(bf),
        rows.astype(bf),
        index.reshape(32, 128),
        mask,
    )


def mm(left, right):
    return lax.dot_general(left, right, (((1,), (0,)), ((), ())), preferred_element_type=F32)


def mm_t(left, right):
    return lax.dot_general(left, right, (((1,), (1,)), ((), ())), preferred_element_type=F32)


def t_mm(left, right):
    return lax.dot_general(left, right, (((0,), (0,)), ((), ())), preferred_element_type=F32)


def normalize(values):
    centred = values - jnp.mean(values, -1, keepdims=True)
    inverse_std = lax.rsqrt(jnp.mean(centred * centred, -1, keepdims=True) + 1e-05)
    return centred * inverse_std, inverse_std


def normalize_back(normed, inverse_std, grads):
    first = jnp.mean(grads, -1, keepdims=True)
    second = jnp.mean(grads * normed, -1, keepdims=True)
    return inverse_std * (grads - first - normed * second)


def window_of(values, a, b):
    if b == 0:
        return values[64 * a : 64 * a + 64]
    near, far = 128 + 32 * a, 192 + 32 * a
    return jnp.concatenate([values[near : near + 32], values[far : far + 32]], 0)


def put_window(ref, a, b, lanes, values):
    if b == 0:
        ref[64 * a : 64 * a + 64, lanes] = values
    else:
        near, far = 128 + 32 * a, 192 + 32 * a
        ref[near : near + 32, lanes] = values[:32]
        ref[far : far + 32, lanes] = values[32:]


def get_window(ref, a, b, lanes):
    if b == 0:
        return ref[64 * a : 64 * a + 64, lanes]
    near, far = 128 + 32 * a, 192 + 32 * a
    return jnp.concatenate([ref[near : near + 32, lanes], ref[far : far + 32, lanes]], 0)


def halves(op, empty, low, values):
    first = op(jnp.where(low, values, empty), -1, keepdims=True)
    second = op(jnp.where(low, empty, values), -1, keepdims=True)
    return jnp.where(low, first, second)


NAMES = (
    "feat", "cot", "pos", "w_attend", "w_out", "w_merge", "to_window", "to_window_t", "to_quad",
    "to_quad_t", "win_quad", "win_quad_t", "row_pick", "index", "mask",
)
ORDER = (
    "feat", "to_window", "w_attend", "pos", "index", "mask", "cot", "w_merge", "row_pick",
    "to_quad", "win_quad", "w_out", "win_quad_t", "to_quad_t", "to_window_t",
)
N_IN = len(NAMES)


def kernel(scatter, *refs):
    given, refs = refs[:N_IN], refs[N_IN:]
    merged_ref, grad_ref, share_ref = refs[:3]
    if scatter:
        refs = refs[3:]
    else:
        local_ref, refs = refs[3], refs[4:]
    held, refs = refs[:N_IN], refs[N_IN:]
    (
        x_scr, cot_scr, table_scr, bias_a, bias_b, normed_scr, std_scr,
        normed_east, std_east, qkv, probs, attended, branch_grad, outer, proj_grad,
        hidden_grad, left_o, left_r, feature_scr,
        ex_send, ex_recv,
        g_own, g_send, g_recv, x_own, x_send, x_recv, y_send, y_recv,
        x_own2, x_send2, x_recv2, y_send2, y_recv2, z_line, z_send, z_recv,
        in_sem, ex_ssem, ex_rsem, c_ssem, c_rsem, x_ssem, x_rsem, y_ssem, y_rsem,
        z_ssem, z_rsem, near_sem,
    ) = refs
    (
        feat, cot, pos, w_attend, w_out, w_merge, to_window, to_window_t, to_quad, to_quad_t,
        win_quad, win_quad_t, row_pick, index, mask,
    ) = held
    copies = {
        name: pltpu.make_async_copy(given[i], held[i], in_sem.at[i])
        for i, name in enumerate(NAMES)
    }
    for name in ORDER:
        copies[name].start()

    z, x_lo = lax.axis_index("azim_0"), lax.axis_index("azim_1")
    x_hi, y, core = (lax.axis_index(name) for name in FRAME)
    n_z = lax.axis_size("azim_0")
    n_azim = n_z * 2
    azim = 2 * z + x_lo
    east, west = (azim + 1) % n_azim, (azim + n_azim - 1) % n_azim
    east_id = {"azim_0": east // 2, "azim_1": east % 2}
    west_id = {"azim_0": west // 2, "azim_1": west % 2}
    xi = 2 * x_lo + x_hi

    def x_id(step):
        other = (xi + step) % 4
        return {"azim_1": other // 2, "frame_0": other % 2}

    def z_id(step):
        return {"azim_0": (z + n_z + step) % n_z}

    barrier = pltpu.get_barrier_semaphore()
    near = [east_id, west_id]
    if scatter:
        near += [{"frame_2": 1 - core}]
        near += [x_id(step) for step in (1, 2, 3)]
        near += [{"frame_1": (y + step) % 4} for step in (1, 2, 3)]
        near += [{"frame_1": (y + step) % 4, "frame_2": 1 - core} for step in (1, 2, 3)]
        near += [z_id(1), z_id(-1)]
    for device in near:
        pl.semaphore_signal(barrier, inc=1, device_id=device)

    def exchange(i, device):
        return pltpu.make_async_remote_copy(
            src_ref=ex_send.at[i], dst_ref=ex_recv.at[i], send_sem=ex_ssem.at[i],
            recv_sem=ex_rsem.at[i], device_id=device,
        )

    copies["feat"].wait()
    x_scr[...] = jnp.zeros_like(x_scr)
    for row in range(14):
        x_scr[row, 0:14, :] = feat[row].astype(F32)
    tokens = x_scr[...].reshape(224, C)
    tokens16 = tokens.astype(BF)
    copies["to_window"].wait()
    ex_send[0] = mm(to_window[192:256], tokens16).astype(BF)
    pl.semaphore_wait(barrier, len(near))
    exchange(0, west_id).start()
    if scatter:
        for step in (1, -1):
            pl.semaphore_signal(near_sem.at[0], inc=1, device_id=z_id(step))

    def widen_reach(i):
        if not scatter:
            return
        pl.semaphore_wait(near_sem.at[i], 2)
        if i < 2:
            for step in (2 ** (i + 1), -(2 ** (i + 1))):
                pl.semaphore_signal(near_sem.at[i + 1], inc=1, device_id=z_id(step))

    normed, inverse_std = normalize(tokens)
    normed_scr[...] = normed
    std_scr[...] = inverse_std
    rolled_own = mm(to_window[0:192], normed.astype(BF)).astype(BF)
    copies["w_attend"].wait()
    qkv[0:192] = mm(rolled_own, w_attend[...]).astype(BF)

    copies["pos"].wait()
    copies["index"].wait()
    copies["mask"].wait()
    table_scr[...] = jnp.zeros_like(table_scr)
    table_scr[0:12, 0:169] = pos[...]
    table = table_scr[...]
    high = table.astype(BF).astype(F32)
    both = jnp.concatenate([high, table - high], 0).astype(BF)
    lane = lax.broadcasted_iota(jnp.int32, (1, 128), 1)
    entry = lax.broadcasted_iota(jnp.int32, (256, 128), 0).astype(F32)
    for t in range(0, 32, 4):
        picks = [
            jnp.where(entry == index[u : u + 1, :], 1.0, 0.0).astype(BF) for u in range(t, t + 4)
        ]
        wide = mm(both, jnp.concatenate(picks, 1))
        for u in range(4):
            part = wide[:, 128 * u : 128 * u + 128]
            part = part[0:16] + part[16:32]
            turned = pltpu.roll(part, 64, 1)
            p = 2 * (t + u)
            bias_a[pl.ds(p, 16, stride=64), :] = part
            bias_a[pl.ds(p + 1, 16, stride=64), :] = turned
            bias_b[pl.ds(p, 16, stride=64), :] = turned
            bias_b[pl.ds(p + 1, 16, stride=64), :] = part
    low = lane < 64

    def pair_bias(pair):
        first = bias_a[128 * pair : 128 * pair + 64, :]
        second = bias_b[128 * pair + 64 : 128 * pair + 128, :]
        return jnp.where(low, first, second)

    copies["cot"].wait()
    cot_scr[...] = jnp.zeros_like(cot_scr)
    for row in range(7):
        cot_scr[row, 0:7, :] = cot[row].astype(F32)
    copies["w_merge"].wait()
    quad_grad_in = mm_t(cot_scr[...].reshape(64, OUT).astype(BF), w_merge[...])

    exchange(0, west_id).wait()
    widen_reach(0)
    normed, inverse_std = normalize(ex_recv[0].astype(F32))
    normed_east[...] = normed
    std_east[...] = inverse_std
    rolled_east = normed.astype(BF)
    qkv[192:256] = mm(rolled_east, w_attend[...]).astype(BF)

    head_lanes = [(lane // 32 == h).astype(F32).astype(BF) for h in range(4)]

    def spread(block):
        return jnp.concatenate([block * head_lanes[h] for h in range(4)], 0)

    def heads_of(wide):
        total = wide[0:64] * head_lanes[0].astype(F32)
        for h in range(1, 4):
            total = total + wide[64 * h : 64 * h + 64] * head_lanes[h].astype(F32)
        return total

    def group_lanes(kind, group):
        start = C * kind + 128 * group
        return slice(start, start + 128)

    def units_of(windows):
        return [(w, group) for w in windows for group in range(GROUPS)]

    def of_window(ref, w, kind, group):
        return get_window(ref, *WINDOWS[w], group_lanes(kind, group))

    ones = (lax.broadcasted_iota(jnp.int32, (128, 128), 0) < 64) == low
    ones = ones.astype(F32).astype(BF)

    def half_sums(values):
        joined = jnp.concatenate(values, 0)
        high = joined.astype(BF)
        rest = (joined - high.astype(F32)).astype(BF)
        total = mm(high, ones) + mm(rest, ones)
        return [total[64 * i : 64 * i + 64] for i in range(len(values))]

    def split_halves(wide):
        return [part[:, 128 * i : 128 * i + 128] for part in wide for i in range(2)]

    def join_halves(parts):
        return [
            jnp.concatenate([parts[i].astype(BF), parts[i + 1].astype(BF)], 1)
            for i in range(0, len(parts), 2)
        ]

    def attend(*windows):
        units = units_of(windows)
        scores = [
            mm_t(of_window(qkv, w, 0, g), spread(of_window(qkv, w, 1, g))) for w, g in units
        ]
        parts = split_halves(scores)
        for i, (w, g) in enumerate(units):
            for j in range(2):
                bias = pair_bias(2 * g + j) + mask[WINDOWS[w][0]]
                parts[2 * i + j] = parts[2 * i + j] * SCALE + bias
        tops = [halves(jnp.max, -3e38, low, part) for part in parts]
        parts = [jnp.exp(part - top) for part, top in zip(parts, tops)]
        sums = half_sums(parts)
        parts = [part * (1.0 / total) for part, total in zip(parts, sums)]
        for i, (w, g) in enumerate(units):
            for j in range(2):
                probs[GROUPS * w + g, :, 128 * j : 128 * j + 128] = parts[2 * i + j]
        for (w, g), prob in zip(units, join_halves(parts)):
            result = mm(prob, spread(of_window(qkv, w, 2, g))).astype(BF)
            put_window(attended, *WINDOWS[w], group_lanes(0, g), result)

    attend(0, 1)
    ex_send[1] = attended[192:256]
    exchange(1, east_id).start()
    attend(2, 3)
    copies["row_pick"].wait()
    left_r[:, 0:192] = mm_t(row_pick[...], rolled_own).astype(BF)
    left_r[:, 192:256] = mm_t(row_pick[...], rolled_east).astype(BF)
    left_o[...] = mm_t(row_pick[...], attended[...]).astype(BF)
    copies["to_quad"].wait()
    copies["win_quad"].wait()
    copies["w_out"].wait()
    features_quad = mm(to_quad[...], tokens16)
    exchange(1, east_id).wait()
    widen_reach(1)

    extended = jnp.concatenate([attended[0:192], ex_recv[1]], 0)
    attended_quad = mm(win_quad[...], extended).astype(BF)
    hidden = (features_quad + mm(attended_quad, w_out[...])).astype(BF).astype(F32)
    quads = [hidden[64 * e : 64 * e + 64] for e in range(4)]

    def mean(blocks):
        total = (blocks[0] + blocks[1]) + (blocks[2] + blocks[3])
        return jnp.sum(total, -1, keepdims=True) * (1.0 / (4 * C))

    centre = mean(quads)
    quads = [quad - centre for quad in quads]
    quad_std = lax.rsqrt(mean([quad * quad for quad in quads]) + 1e-05)
    quads = [quad * quad_std for quad in quads]
    grads = [quad_grad_in[:, C * e : C * e + C] for e in range(4)]
    first = mean(grads)
    second = mean([grad * quad for grad, quad in zip(grads, quads)])
    for e in range(4):
        value = quad_std * (grads[e] - first - quads[e] * second)
        hidden_grad[64 * e : 64 * e + 64] = value.astype(BF)
    copies["win_quad_t"].wait()
    ex_send[2] = mm(win_quad_t[192:256], hidden_grad[...]).astype(BF)
    exchange(2, west_id).start()
    own_grad = mm(win_quad_t[0:192], hidden_grad[...]).astype(BF)
    branch_grad[0:192] = own_grad
    outer[0:192] = mm_t(own_grad, w_out[...]).astype(BF)
    merged = mm(jnp.concatenate([quad.astype(BF) for quad in quads], 1), w_merge[...])
    for i in range(7):
        merged_ref[i] = merged[8 * i : 8 * i + 7].astype(BF)
    copies["to_quad_t"].wait()
    hidden_own = mm(to_quad_t[...], hidden_grad[...])

    def values_back(*windows):
        units = units_of(windows)
        wide = [
            t_mm(probs[GROUPS * w + g].astype(BF), of_window(outer, w, 0, g)) for w, g in units
        ]
        for (w, g), value in zip(units, wide):
            back = heads_of(value).astype(BF)
            put_window(proj_grad, *WINDOWS[w], group_lanes(2, g), back)

    def scores_back(*windows):
        units = units_of(windows)
        wide = [
            mm_t(of_window(outer, w, 0, g), spread(of_window(qkv, w, 2, g))) for w, g in units
        ]
        grads = split_halves(wide)
        prob = split_halves([probs[GROUPS * w + g] for w, g in units])
        sums = half_sums([p * grad for p, grad in zip(prob, grads)])
        parts = [p * (grad - total) * SCALE for p, grad, total in zip(prob, grads, sums)]
        soft = join_halves(parts)
        wide = [t_mm(part, of_window(qkv, w, 0, g)) for (w, g), part in zip(units, soft)]
        for (w, g), part in zip(units, soft):
            back = mm(part, spread(of_window(qkv, w, 1, g))).astype(BF)
            put_window(proj_grad, *WINDOWS[w], group_lanes(0, g), back)
        for (w, g), value in zip(units, wide):
            back = heads_of(value).astype(BF)
            put_window(proj_grad, *WINDOWS[w], group_lanes(1, g), back)

    def core_copy(i):
        return pltpu.make_async_remote_copy(
            src_ref=g_send.at[i, 1 - core], dst_ref=g_recv.at[i], send_sem=c_ssem.at[i],
            recv_sem=c_rsem.at[i], device_id={"frame_2": 1 - core},
        )

    def start_core(i, product):
        product = product.reshape(2, 192, C)
        g_own[i] = product
        if scatter:
            g_send[i] = product.astype(BF)
            core_copy(i).start()

    def x_copies(i, sent, landing):
        return [
            pltpu.make_async_remote_copy(
                src_ref=sent.at[(xi + step) % 4], dst_ref=landing.at[step - 1],
                send_sem=x_ssem.at[i, step - 1], recv_sem=x_rsem.at[i, step - 1],
                device_id=x_id(step),
            )
            for step in (2, 1, 3)
        ]

    def y_copy(i, m, sent, landing):
        return pltpu.make_async_remote_copy(
            src_ref=sent.at[m], dst_ref=landing.at[y], send_sem=y_ssem.at[i, m],
            recv_sem=y_rsem.at[i, y],
            device_id={"frame_1": 2 * core + m // 2, "frame_2": m % 2},
        )

    def y_landed(i, source, sent, landing):
        return pltpu.make_async_remote_copy(
            src_ref=sent.at[0], dst_ref=landing.at[source], send_sem=y_ssem.at[i, 0],
            recv_sem=y_rsem.at[i, source], device_id={"frame_2": 1 - core},
        )

    def stays(m):
        return jnp.logical_and(2 * core + m // 2 == y, core == m % 2)

    def start_y(i, sent, landing):
        for m in range(4):

            @pl.when(stays(m))
            def _():
                landing[y] = sent[m]

            @pl.when(jnp.logical_not(stays(m)))
            def _():
                y_copy(i, m, sent, landing).start()

    def end_y(i, sent, landing):
        for source in range(4):
            mine = jnp.logical_and(y == source, y // 2 == core)

            @pl.when(jnp.logical_not(mine))
            def _():
                y_landed(i, source, sent, landing).wait_recv()

        for m in range(4):

            @pl.when(jnp.logical_not(stays(m)))
            def _():
                y_copy(i, m, sent, landing).wait_send()

        total = landing[0].astype(F32)
        for source in range(1, 4):
            total = total + landing[source].astype(F32)
        return total

    wide_lane = lax.broadcasted_iota(jnp.int32, (1, C), 1)

    def segments(i, block):
        one, two, three = (block[16 * k : 16 * k + 16] for k in range(3))

        def left(value, count):
            return pltpu.roll(value, C - count, 1)

        if i == 0:
            second = jnp.where(wide_lane < 96, left(one, 288), pltpu.roll(two, 96, 1))
            third = jnp.where(wide_lane < 192, left(two, 192), pltpu.roll(three, 192, 1))
            return one, second, third, left(three, 96)
        if i == 1:
            return one, left(one, 96), two, three
        if i == 2:
            return one, two, three, left(three, 288)
        return one, two, left(two, 192), three

    def start_first(i):
        if not scatter:
            return
        core_copy(i).wait()
        total = (g_own[i, core] + g_recv[i].astype(F32)).reshape(4, 48, C)
        j = i // 2
        if i % 2 == 0:
            x_own[j] = total
            x_send[j] = total.astype(BF)
            for copy in x_copies(i, x_send.at[j], x_recv.at[j]):
                copy.start()
        else:
            for block in range(4):
                for m, value in enumerate(segments(i, total[block])):
                    y_send[j, m, block] = value.astype(BF)
            start_y(i, y_send.at[j], y_recv.at[j])

    def start_second(i):
        j = i // 2
        if i % 2 == 0:
            for copy in x_copies(i, x_send.at[j], x_recv.at[j]):
                copy.wait()
            total = x_own[j, xi]
            for step in (1, 2, 3):
                total = total + x_recv[j, step - 1].astype(F32)
            for m, value in enumerate(segments(i, total)):
                y_send2[j, m] = value.astype(BF)
            start_y(4 + j, y_send2.at[j], y_recv2.at[j])
        else:
            total = end_y(i, y_send.at[j], y_recv.at[j])
            x_own2[j] = total
            x_send2[j] = total.astype(BF)
            for copy in x_copies(4 + j, x_send2.at[j], x_recv2.at[j]):
                copy.start()

    def z_copy(j, step):
        return pltpu.make_async_remote_copy(
            src_ref=z_send.at[j, (z + step) % 16], dst_ref=z_recv.at[j, step - 1],
            send_sem=z_ssem.at[j, step - 1], recv_sem=z_rsem.at[j, step - 1],
            device_id=z_id(step),
        )

    z_steps = sorted(range(1, 16), key=lambda step: -min(step, 16 - step))

    def start_z(j):
        first = end_y(4 + j, y_send2.at[j], y_recv2.at[j])
        for copy in x_copies(4 + j, x_send2.at[j], x_recv2.at[j]):
            copy.wait()
        second = x_own2[j, xi]
        for step in (1, 2, 3):
            second = second + x_recv2[j, step - 1].astype(F32)
        for t in range(3):
            lanes = slice(128 * t, 128 * t + 128)
            z_line[j, pl.ds(t, 16, stride=8), :] = first[:, lanes]
            z_line[j, pl.ds(t + 3, 16, stride=8), :] = second[:, lanes]
        for t in (6, 7):
            z_line[j, pl.ds(t, 16, stride=8), :] = jnp.zeros((16, 128), F32)
        z_send[j] = z_line[j].reshape(16, 8, 128).astype(BF)
        for step in z_steps:
            z_copy(j, step).start()

    def end_z(j):
        total = z_send[j, z].astype(F32)
        for step in z_steps[::-1]:
            z_copy(j, step).wait()
            total = total + z_recv[j, step - 1].astype(F32)
        share_ref[8 * j : 8 * j + 8] = total

    scores_back(2, 3)
    exchange(2, west_id).wait()
    widen_reach(2)
    branch_grad[192:256] = ex_recv[2]
    outer[192:256] = mm_t(ex_recv[2], w_out[...]).astype(BF)
    start_core(0, mm(left_o[...], branch_grad[...]))
    values_back(0, 1, 2, 3)
    start_core(1, mm(left_r[...], proj_grad[:, 2 * C : 3 * C]))
    start_first(0)
    scores_back(0, 1)
    start_first(1)
    start_core(2, mm(left_r[...], proj_grad[:, 0:C]))
    start_core(3, mm(left_r[...], proj_grad[:, C : 2 * C]))
    east_grad = mm_t(proj_grad[192:256], w_attend[...])
    east_grad = normalize_back(normed_east[...], std_east[...], east_grad)
    ex_send[3] = east_grad.astype(BF)
    exchange(3, east_id).start()
    start_first(2)
    start_first(3)
    if scatter:
        start_second(0)
        start_second(1)
    copies["to_window_t"].wait()
    own_proj = mm(to_window_t[:, 0:192], proj_grad[0:192]).astype(BF)
    own_grad = mm_t(own_proj, w_attend[...])
    own_grad = normalize_back(normed_scr[...], std_scr[...], own_grad)
    feature_scr[...] = hidden_own + own_grad

    def end_features():
        exchange(3, east_id).wait()
        grad = feature_scr[...] + mm(to_window_t[:, 192:256], ex_recv[3])
        grad = grad.reshape(14, 16, C)
        for row in range(14):
            grad_ref[row] = grad[row, 0:14].astype(BF)

    if scatter:
        start_z(0)
        start_second(2)
        start_second(3)
        end_features()
        start_z(1)
        end_z(0)
        end_z(1)
    else:
        end_features()
        share_ref[...] = jnp.zeros_like(share_ref)
        local_ref[...] = g_own[...]


def finish(merged_in, grad_in, share, merged_ref, grad_ref, attend_ref, output_ref):
    merged_ref[0] = merged_in[...]
    grad_ref[0] = grad_in[...]
    lane = lax.broadcasted_iota(jnp.int32, (1, 128), 1)

    def put(ref, pieces):
        lines = [jnp.zeros((1, 128), F32) for _ in range(-(-ref.shape[0] // 128))]
        start = 0
        for first, width in pieces:
            skip, turn = divmod(start, 128)
            values = [share[first + i : first + i + 1, :] for i in range(3)]
            if turn:
                values = [pltpu.roll(value, turn, 1) for value in values]
            for j in range(skip, (start + width - 1) // 128 + 1):
                value = values[min(j - skip, 2)]
                if turn and j > skip:
                    value = jnp.where(lane < turn, values[j - skip - 1], value)
                at = lane + 128 * j
                inside = jnp.logical_and(at >= start, at < start + width)
                lines[j] = jnp.where(inside, value, lines[j])
            start += width
        for j, value in enumerate(lines):
            count = min(128, ref.shape[0] - 128 * j)
            ref[128 * j : 128 * j + count] = value.reshape(128)[:count]

    put(output_ref, ((0, 288),))
    v, q, k = 3, 8, 11
    segment = 2 * (lax.axis_index("frame_1") % 2) + lax.axis_index("frame_2")
    for m, pieces in enumerate((
        ((q, 384), (k, 384), (v, 96)),
        ((v, 288), (q, 384), (k, 192)),
        ((k, 192), (v, 384), (q, 288)),
        ((q, 96), (k, 384), (v, 384)),
    )):
        pl.when(segment == m)(functools.partial(put, attend_ref, pieces))


def local_call(scatter, features, position_bias, attend_weight, output_weight, merge_weight, cotangent):
    given = (features[0], cotangent[0], position_bias.T, attend_weight, output_weight, merge_weight)
    given = given + tuple(jnp.asarray(table) for table in tables())
    dma = pltpu.SemaphoreType.DMA
    scratch = [pltpu.VMEM(a.shape, a.dtype) for a in given]
    scratch += [
        pltpu.VMEM((14, 16, C), F32),
        pltpu.VMEM((8, 8, OUT), F32),
        pltpu.VMEM((16, 256), F32),
        pltpu.VMEM((1024, 128), F32),
        pltpu.VMEM((1024, 128), F32),
        pltpu.VMEM((224, C), F32),
        pltpu.VMEM((224, 1), F32),
        pltpu.VMEM((64, C), F32),
        pltpu.VMEM((64, 1), F32),
        pltpu.VMEM((256, 3 * C), BF),
        pltpu.VMEM((12, 64, 256), F32),
        pltpu.VMEM((256, C), BF),
        pltpu.VMEM((256, C), BF),
        pltpu.VMEM((256, C), BF),
        pltpu.VMEM((256, 3 * C), BF),
        pltpu.VMEM((256, C), BF),
        pltpu.VMEM((C, 256), BF),
        pltpu.VMEM((C, 256), BF),
        pltpu.VMEM((224, C), F32),
        pltpu.VMEM((4, 64, C), BF),
        pltpu.VMEM((4, 64, C), BF),
        pltpu.VMEM((4, 2, 192, C), F32),
        pltpu.VMEM((4, 2, 192, C), BF),
        pltpu.VMEM((4, 192, C), BF),
        pltpu.VMEM((2, 4, 48, C), F32),
        pltpu.VMEM((2, 4, 48, C), BF),
        pltpu.VMEM((2, 3, 48, C), BF),
        pltpu.VMEM((2, 4, 4, 16, C), BF),
        pltpu.VMEM((2, 4, 4, 16, C), BF),
        pltpu.VMEM((2, 4, 16, C), F32),
        pltpu.VMEM((2, 4, 16, C), BF),
        pltpu.VMEM((2, 3, 16, C), BF),
        pltpu.VMEM((2, 4, 16, C), BF),
        pltpu.VMEM((2, 4, 16, C), BF),
        pltpu.VMEM((2, 128, 128), F32),
        pltpu.VMEM((2, 16, 8, 128), BF),
        pltpu.VMEM((2, 15, 8, 128), BF),
        dma((N_IN,)), dma((4,)), dma((4,)), dma((4,)), dma((4,)), dma((6, 3)), dma((6, 3)),
        dma((6, 4)), dma((6, 4)), dma((2, 15)), dma((2, 15)), pltpu.SemaphoreType.REGULAR((3,)),
    ]
    vmem = pl.BlockSpec(memory_space=pltpu.VMEM)
    return pl.pallas_call(
        functools.partial(kernel, scatter),
        out_shape=(
            jax.ShapeDtypeStruct((7, 7, OUT), BF),
            jax.ShapeDtypeStruct((14, 14, C), BF),
            jax.ShapeDtypeStruct((16, 128), F32),
        )
        + (() if scatter else (jax.ShapeDtypeStruct((4, 2, 192, C), F32),)),
        in_specs=[pl.BlockSpec(memory_space=pl.ANY)] * N_IN,
        out_specs=(vmem,) * (3 if scatter else 4),
        scratch_shapes=scratch,
        compiler_params=pltpu.CompilerParams(collective_id=0, has_side_effects=True),
    )(*given)


def per_device(*arrays):
    merged, feature_grad, share = local_call(True, *arrays)
    vmem = pl.BlockSpec(memory_space=pltpu.VMEM)
    return pl.pallas_call(
        finish,
        out_shape=(
            jax.ShapeDtypeStruct((1, *merged.shape), BF),
            jax.ShapeDtypeStruct((1, *feature_grad.shape), BF),
            jax.ShapeDtypeStruct((864,), F32),
            jax.ShapeDtypeStruct((288,), F32),
        ),
        in_specs=(vmem,) * 3,
        out_specs=(vmem,) * 4,
    )(merged, feature_grad, share)


def solution(mesh):
    split = Mesh(mesh.devices.reshape(16, 2, 2, 4, 2), AZIM_FRAME)
    placed = (P(FRAME, None, AZIM, None), P(), P(), P(), P(), P(FRAME, None, AZIM, None))
    return jax.shard_map(
        per_device,
        mesh=split,
        in_specs=placed,
        out_specs=(
            P(FRAME, None, AZIM, None),
            P(FRAME, None, AZIM, None),
            P(AZIM_FRAME),
            P(AZIM_FRAME),
        ),
        check_vma=False,
    )
```

```python
import functools

import jax
import jax.numpy as jnp
import ml_dtypes
import numpy as np
from jax import lax
from jax.experimental import pallas as pl
from jax.experimental.pallas import tpu as pltpu
from jax.sharding import Mesh
from jax.sharding import PartitionSpec as P

AZIM = ("azim_0", "azim_1")
AZIM_FRAME = ("azim_0", "azim_1", "frame_0", "frame_1", "frame_2")
FRAME = ("frame_0", "frame_1", "frame_2")

BF = jnp.bfloat16
F32 = jnp.float32
C = 384
OUT = 768
GROUPS = 3
SCALE = 32 ** (-0.5)
WINDOWS = ((0, 1), (1, 1), (0, 0), (1, 0))


def position_row(row, col):
    return 4 * row + col if col < 4 else 32 + 3 * row + col - 4


def east_row(row, col):
    rolled = (row - 3) % 14
    return 32 * (rolled // 7) + 3 * (rolled % 7) + col


@functools.cache
def tables():
    to_window = np.zeros((256, 224), np.float32)
    for a in range(2):
        for b in range(2):
            for row in range(7):
                for col in range(7):
                    frame_row, frame_col = (7 * a + row + 3) % 14, 7 * b + col + 3
                    if frame_col >= 14:
                        continue
                    at = position_row(row, col)
                    line = 64 * a + at if b == 0 else 128 + 32 * a + at
                    to_window[line, 16 * frame_row + frame_col] = 1
    for row in range(14):
        for col in range(3):
            to_window[192 + east_row(row, col), 16 * row + col] = 1
    to_quad = np.zeros((256, 224), np.float32)
    for block in range(4):
        for i in range(7):
            for j in range(7):
                token = 16 * (2 * i + block % 2) + 2 * j + block // 2
                to_quad[64 * block + 8 * i + j, token] = 1
    window_to_quad = to_quad @ to_window.T
    rows = np.zeros((C, C), np.float32)
    for c in range(2):
        for xi in range(4):
            for k in range(3):
                for z in range(16):
                    rows[192 * c + 48 * xi + 16 * k + z, 24 * z + 6 * xi + 3 * c + k] = 1
    index = np.full((64, 64), 255.0, np.float32)
    mask = np.zeros((2, 64, 64), np.float32)
    valid = np.zeros(64, bool)
    for row in range(7):
        for col in range(7):
            p = position_row(row, col)
            valid[p] = True
            for row_q in range(7):
                for col_q in range(7):
                    q = position_row(row_q, col_q)
                    index[p, q] = 13 * (row - row_q + 6) + col - col_q + 6
                    if (row < 4) != (row_q < 4):
                        mask[1, p, q] = -100.0
    mask[:, :, ~valid] = -1e30
    mask = np.concatenate([mask, mask], -1)
    bf = ml_dtypes.bfloat16
    return (
        to_window.astype(bf),
        np.ascontiguousarray(to_window.T).astype(bf),
        to_quad.astype(bf),
        np.ascontiguousarray(to_quad.T).astype(bf),
        window_to_quad.astype(bf),
        np.ascontiguousarray(window_to_quad.T).astype(bf),
        rows.astype(bf),
        index.reshape(32, 128),
        mask,
    )


def mm(left, right):
    return lax.dot_general(left, right, (((1,), (0,)), ((), ())), preferred_element_type=F32)


def mm_t(left, right):
    return lax.dot_general(left, right, (((1,), (1,)), ((), ())), preferred_element_type=F32)


def t_mm(left, right):
    return lax.dot_general(left, right, (((0,), (0,)), ((), ())), preferred_element_type=F32)


def normalize(values):
    centred = values - jnp.mean(values, -1, keepdims=True)
    inverse_std = lax.rsqrt(jnp.mean(centred * centred, -1, keepdims=True) + 1e-05)
    return centred * inverse_std, inverse_std


def normalize_back(normed, inverse_std, grads):
    first = jnp.mean(grads, -1, keepdims=True)
    second = jnp.mean(grads * normed, -1, keepdims=True)
    return inverse_std * (grads - first - normed * second)


def window_of(values, a, b):
    if b == 0:
        return values[64 * a : 64 * a + 64]
    near, far = 128 + 32 * a, 192 + 32 * a
    return jnp.concatenate([values[near : near + 32], values[far : far + 32]], 0)


def put_window(ref, a, b, lanes, values):
    if b == 0:
        ref[64 * a : 64 * a + 64, lanes] = values
    else:
        near, far = 128 + 32 * a, 192 + 32 * a
        ref[near : near + 32, lanes] = values[:32]
        ref[far : far + 32, lanes] = values[32:]


def get_window(ref, a, b, lanes):
    if b == 0:
        return ref[64 * a : 64 * a + 64, lanes]
    near, far = 128 + 32 * a, 192 + 32 * a
    return jnp.concatenate([ref[near : near + 32, lanes], ref[far : far + 32, lanes]], 0)


def halves(op, empty, low, values):
    first = op(jnp.where(low, values, empty), -1, keepdims=True)
    second = op(jnp.where(low, empty, values), -1, keepdims=True)
    return jnp.where(low, first, second)


NAMES = (
    "feat", "cot", "pos", "w_attend", "w_out", "w_merge", "to_window", "to_window_t", "to_quad",
    "to_quad_t", "win_quad", "win_quad_t", "row_pick", "index", "mask",
)
ORDER = (
    "feat", "to_window", "w_attend", "pos", "index", "mask", "cot", "w_merge", "row_pick",
    "to_quad", "win_quad", "w_out", "win_quad_t", "to_quad_t", "to_window_t",
)
N_IN = len(NAMES)


def kernel(scatter, *refs):
    given, refs = refs[:N_IN], refs[N_IN:]
    merged_ref, grad_ref, share_ref = refs[:3]
    if scatter:
        refs = refs[3:]
    else:
        local_ref, refs = refs[3], refs[4:]
    held, refs = refs[:N_IN], refs[N_IN:]
    (
        x_scr, cot_scr, table_scr, bias_a, bias_b, normed_scr, std_scr,
        normed_east, std_east, qkv, probs, attended, branch_grad, outer, proj_grad,
        hidden_grad, left_o, left_r, feature_scr,
        ex_send, ex_recv,
        g_own, g_send, g_recv, x_own, x_send, x_recv, y_send, y_recv,
        x_own2, x_send2, x_recv2, y_send2, y_recv2, z_line, z_send, z_recv,
        in_sem, ex_ssem, ex_rsem, c_ssem, c_rsem, x_ssem, x_rsem, y_ssem, y_rsem,
        z_ssem, z_rsem, near_sem,
    ) = refs
    (
        feat, cot, pos, w_attend, w_out, w_merge, to_window, to_window_t, to_quad, to_quad_t,
        win_quad, win_quad_t, row_pick, index, mask,
    ) = held
    copies = {
        name: pltpu.make_async_copy(given[i], held[i], in_sem.at[i])
        for i, name in enumerate(NAMES)
    }
    for name in ORDER:
        copies[name].start()

    z, x_lo = lax.axis_index("azim_0"), lax.axis_index("azim_1")
    x_hi, y, core = (lax.axis_index(name) for name in FRAME)
    n_z = lax.axis_size("azim_0")
    n_azim = n_z * 2
    azim = 2 * z + x_lo
    east, west = (azim + 1) % n_azim, (azim + n_azim - 1) % n_azim
    east_id = {"azim_0": east // 2, "azim_1": east % 2}
    west_id = {"azim_0": west // 2, "azim_1": west % 2}
    xi = 2 * x_lo + x_hi

    def x_id(step):
        other = (xi + step) % 4
        return {"azim_1": other // 2, "frame_0": other % 2}

    def z_id(step):
        return {"azim_0": (z + n_z + step) % n_z}

    barrier = pltpu.get_barrier_semaphore()
    near = [east_id, west_id]
    if scatter:
        near += [{"frame_2": 1 - core}]
        near += [x_id(step) for step in (1, 2, 3)]
        near += [{"frame_1": (y + step) % 4} for step in (1, 2, 3)]
        near += [{"frame_1": (y + step) % 4, "frame_2": 1 - core} for step in (1, 2, 3)]
        near += [z_id(1), z_id(-1)]
    for device in near:
        pl.semaphore_signal(barrier, inc=1, device_id=device)

    def exchange(i, device):
        return pltpu.make_async_remote_copy(
            src_ref=ex_send.at[i], dst_ref=ex_recv.at[i], send_sem=ex_ssem.at[i],
            recv_sem=ex_rsem.at[i], device_id=device,
        )

    copies["feat"].wait()
    x_scr[...] = jnp.zeros_like(x_scr)
    for row in range(14):
        x_scr[row, 0:14, :] = feat[row].astype(F32)
    tokens = x_scr[...].reshape(224, C)
    tokens16 = tokens.astype(BF)
    copies["to_window"].wait()
    ex_send[0] = mm(to_window[192:256], tokens16).astype(BF)
    pl.semaphore_wait(barrier, len(near))
    exchange(0, west_id).start()
    if scatter:
        for step in (1, -1):
            pl.semaphore_signal(near_sem.at[0], inc=1, device_id=z_id(step))

    def widen_reach(i):
        if not scatter:
            return
        pl.semaphore_wait(near_sem.at[i], 2)
        if i < 2:
            for step in (2 ** (i + 1), -(2 ** (i + 1))):
                pl.semaphore_signal(near_sem.at[i + 1], inc=1, device_id=z_id(step))

    normed, inverse_std = normalize(tokens)
    normed_scr[...] = normed
    std_scr[...] = inverse_std
    rolled_own = mm(to_window[0:192], normed.astype(BF)).astype(BF)
    copies["w_attend"].wait()
    qkv[0:192] = mm(rolled_own, w_attend[...]).astype(BF)

    copies["pos"].wait()
    copies["index"].wait()
    copies["mask"].wait()
    table_scr[...] = jnp.zeros_like(table_scr)
    table_scr[0:12, 0:169] = pos[...]
    table = table_scr[...]
    high = table.astype(BF).astype(F32)
    both = jnp.concatenate([high, table - high], 0).astype(BF)
    lane = lax.broadcasted_iota(jnp.int32, (1, 128), 1)
    entry = lax.broadcasted_iota(jnp.int32, (256, 128), 0).astype(F32)
    for t in range(0, 32, 4):
        picks = [
            jnp.where(entry == index[u : u + 1, :], 1.0, 0.0).astype(BF) for u in range(t, t + 4)
        ]
        wide = mm(both, jnp.concatenate(picks, 1))
        for u in range(4):
            part = wide[:, 128 * u : 128 * u + 128]
            part = part[0:16] + part[16:32]
            turned = pltpu.roll(part, 64, 1)
            p = 2 * (t + u)
            bias_a[pl.ds(p, 16, stride=64), :] = part
            bias_a[pl.ds(p + 1, 16, stride=64), :] = turned
            bias_b[pl.ds(p, 16, stride=64), :] = turned
            bias_b[pl.ds(p + 1, 16, stride=64), :] = part
    low = lane < 64

    def pair_bias(pair):
        first = bias_a[128 * pair : 128 * pair + 64, :]
        second = bias_b[128 * pair + 64 : 128 * pair + 128, :]
        return jnp.where(low, first, second)

    copies["cot"].wait()
    cot_scr[...] = jnp.zeros_like(cot_scr)
    for row in range(7):
        cot_scr[row, 0:7, :] = cot[row].astype(F32)
    copies["w_merge"].wait()
    quad_grad_in = mm_t(cot_scr[...].reshape(64, OUT).astype(BF), w_merge[...])

    exchange(0, west_id).wait()
    widen_reach(0)
    normed, inverse_std = normalize(ex_recv[0].astype(F32))
    normed_east[...] = normed
    std_east[...] = inverse_std
    rolled_east = normed.astype(BF)
    qkv[192:256] = mm(rolled_east, w_attend[...]).astype(BF)

    head_lanes = [(lane // 32 == h).astype(F32).astype(BF) for h in range(4)]

    def spread(block):
        return jnp.concatenate([block * head_lanes[h] for h in range(4)], 0)

    def heads_of(wide):
        total = wide[0:64] * head_lanes[0].astype(F32)
        for h in range(1, 4):
            total = total + wide[64 * h : 64 * h + 64] * head_lanes[h].astype(F32)
        return total

    def group_lanes(kind, group):
        start = C * kind + 128 * group
        return slice(start, start + 128)

    def units_of(windows):
        return [(w, group) for w in windows for group in range(GROUPS)]

    def of_window(ref, w, kind, group):
        return get_window(ref, *WINDOWS[w], group_lanes(kind, group))

    ones = (lax.broadcasted_iota(jnp.int32, (128, 128), 0) < 64) == low
    ones = ones.astype(F32).astype(BF)

    def half_sums(values):
        joined = jnp.concatenate(values, 0)
        high = joined.astype(BF)
        rest = (joined - high.astype(F32)).astype(BF)
        total = mm(high, ones) + mm(rest, ones)
        return [total[64 * i : 64 * i + 64] for i in range(len(values))]

    def split_halves(wide):
        return [part[:, 128 * i : 128 * i + 128] for part in wide for i in range(2)]

    def join_halves(parts):
        return [
            jnp.concatenate([parts[i].astype(BF), parts[i + 1].astype(BF)], 1)
            for i in range(0, len(parts), 2)
        ]

    def attend(*windows):
        units = units_of(windows)
        scores = [
            mm_t(of_window(qkv, w, 0, g), spread(of_window(qkv, w, 1, g))) for w, g in units
        ]
        parts = split_halves(scores)
        for i, (w, g) in enumerate(units):
            for j in range(2):
                bias = pair_bias(2 * g + j) + mask[WINDOWS[w][0]]
                parts[2 * i + j] = parts[2 * i + j] * SCALE + bias
        tops = [halves(jnp.max, -3e38, low, part) for part in parts]
        parts = [jnp.exp(part - top) for part, top in zip(parts, tops)]
        sums = half_sums(parts)
        parts = [part * (1.0 / total) for part, total in zip(parts, sums)]
        for i, (w, g) in enumerate(units):
            for j in range(2):
                probs[GROUPS * w + g, :, 128 * j : 128 * j + 128] = parts[2 * i + j]
        for (w, g), prob in zip(units, join_halves(parts)):
            result = mm(prob, spread(of_window(qkv, w, 2, g))).astype(BF)
            put_window(attended, *WINDOWS[w], group_lanes(0, g), result)

    attend(0, 1)
    ex_send[1] = attended[192:256]
    exchange(1, east_id).start()
    attend(2, 3)
    copies["row_pick"].wait()
    left_r[:, 0:192] = mm_t(row_pick[...], rolled_own).astype(BF)
    left_r[:, 192:256] = mm_t(row_pick[...], rolled_east).astype(BF)
    left_o[...] = mm_t(row_pick[...], attended[...]).astype(BF)
    copies["to_quad"].wait()
    copies["win_quad"].wait()
    copies["w_out"].wait()
    features_quad = mm(to_quad[...], tokens16)
    exchange(1, east_id).wait()
    widen_reach(1)

    extended = jnp.concatenate([attended[0:192], ex_recv[1]], 0)
    attended_quad = mm(win_quad[...], extended).astype(BF)
    hidden = (features_quad + mm(attended_quad, w_out[...])).astype(BF).astype(F32)
    quads = [hidden[64 * e : 64 * e + 64] for e in range(4)]

    def mean(blocks):
        total = (blocks[0] + blocks[1]) + (blocks[2] + blocks[3])
        return jnp.sum(total, -1, keepdims=True) * (1.0 / (4 * C))

    centre = mean(quads)
    quads = [quad - centre for quad in quads]
    quad_std = lax.rsqrt(mean([quad * quad for quad in quads]) + 1e-05)
    quads = [quad * quad_std for quad in quads]
    grads = [quad_grad_in[:, C * e : C * e + C] for e in range(4)]
    first = mean(grads)
    second = mean([grad * quad for grad, quad in zip(grads, quads)])
    for e in range(4):
        value = quad_std * (grads[e] - first - quads[e] * second)
        hidden_grad[64 * e : 64 * e + 64] = value.astype(BF)
    copies["win_quad_t"].wait()
    ex_send[2] = mm(win_quad_t[192:256], hidden_grad[...]).astype(BF)
    exchange(2, west_id).start()
    own_grad = mm(win_quad_t[0:192], hidden_grad[...]).astype(BF)
    branch_grad[0:192] = own_grad
    outer[0:192] = mm_t(own_grad, w_out[...]).astype(BF)
    merged = mm(jnp.concatenate([quad.astype(BF) for quad in quads], 1), w_merge[...])
    for i in range(7):
        merged_ref[i] = merged[8 * i : 8 * i + 7].astype(BF)
    copies["to_quad_t"].wait()
    hidden_own = mm(to_quad_t[...], hidden_grad[...])

    def values_back(*windows):
        units = units_of(windows)
        wide = [
            t_mm(probs[GROUPS * w + g].astype(BF), of_window(outer, w, 0, g)) for w, g in units
        ]
        for (w, g), value in zip(units, wide):
            back = heads_of(value).astype(BF)
            put_window(proj_grad, *WINDOWS[w], group_lanes(2, g), back)

    def scores_back(*windows):
        units = units_of(windows)
        wide = [
            mm_t(of_window(outer, w, 0, g), spread(of_window(qkv, w, 2, g))) for w, g in units
        ]
        grads = split_halves(wide)
        prob = split_halves([probs[GROUPS * w + g] for w, g in units])
        sums = half_sums([p * grad for p, grad in zip(prob, grads)])
        parts = [p * (grad - total) * SCALE for p, grad, total in zip(prob, grads, sums)]
        soft = join_halves(parts)
        wide = [t_mm(part, of_window(qkv, w, 0, g)) for (w, g), part in zip(units, soft)]
        for (w, g), part in zip(units, soft):
            back = mm(part, spread(of_window(qkv, w, 1, g))).astype(BF)
            put_window(proj_grad, *WINDOWS[w], group_lanes(0, g), back)
        for (w, g), value in zip(units, wide):
            back = heads_of(value).astype(BF)
            put_window(proj_grad, *WINDOWS[w], group_lanes(1, g), back)

    def core_copy(i):
        return pltpu.make_async_remote_copy(
            src_ref=g_send.at[i, 1 - core], dst_ref=g_recv.at[i], send_sem=c_ssem.at[i],
            recv_sem=c_rsem.at[i], device_id={"frame_2": 1 - core},
        )

    def start_core(i, product):
        product = product.reshape(2, 192, C)
        g_own[i] = product
        if scatter:
            g_send[i] = product.astype(BF)
            core_copy(i).start()

    def x_copies(i, sent, landing):
        return [
            pltpu.make_async_remote_copy(
                src_ref=sent.at[(xi + step) % 4], dst_ref=landing.at[step - 1],
                send_sem=x_ssem.at[i, step - 1], recv_sem=x_rsem.at[i, step - 1],
                device_id=x_id(step),
            )
            for step in (2, 1, 3)
        ]

    def y_copy(i, m, sent, landing):
        return pltpu.make_async_remote_copy(
            src_ref=sent.at[m], dst_ref=landing.at[y], send_sem=y_ssem.at[i, m],
            recv_sem=y_rsem.at[i, y],
            device_id={"frame_1": 2 * core + m // 2, "frame_2": m % 2},
        )

    def y_landed(i, source, sent, landing):
        return pltpu.make_async_remote_copy(
            src_ref=sent.at[0], dst_ref=landing.at[source], send_sem=y_ssem.at[i, 0],
            recv_sem=y_rsem.at[i, source], device_id={"frame_2": 1 - core},
        )

    def stays(m):
        return jnp.logical_and(2 * core + m // 2 == y, core == m % 2)

    def start_y(i, sent, landing):
        for m in range(4):

            @pl.when(stays(m))
            def _():
                landing[y] = sent[m]

            @pl.when(jnp.logical_not(stays(m)))
            def _():
                y_copy(i, m, sent, landing).start()

    def end_y(i, sent, landing):
        for source in range(4):
            mine = jnp.logical_and(y == source, y // 2 == core)

            @pl.when(jnp.logical_not(mine))
            def _():
                y_landed(i, source, sent, landing).wait_recv()

        for m in range(4):

            @pl.when(jnp.logical_not(stays(m)))
            def _():
                y_copy(i, m, sent, landing).wait_send()

        total = landing[0].astype(F32)
        for source in range(1, 4):
            total = total + landing[source].astype(F32)
        return total

    wide_lane = lax.broadcasted_iota(jnp.int32, (1, C), 1)

    def segments(i, block):
        one, two, three = (block[16 * k : 16 * k + 16] for k in range(3))

        def left(value, count):
            return pltpu.roll(value, C - count, 1)

        if i == 0:
            second = jnp.where(wide_lane < 96, left(one, 288), pltpu.roll(two, 96, 1))
            third = jnp.where(wide_lane < 192, left(two, 192), pltpu.roll(three, 192, 1))
            return one, second, third, left(three, 96)
        if i == 1:
            return one, left(one, 96), two, three
        if i == 2:
            return one, two, three, left(three, 288)
        return one, two, left(two, 192), three

    def start_first(i):
        if not scatter:
            return
        core_copy(i).wait()
        total = (g_own[i, core] + g_recv[i].astype(F32)).reshape(4, 48, C)
        j = i // 2
        if i % 2 == 0:
            x_own[j] = total
            x_send[j] = total.astype(BF)
            for copy in x_copies(i, x_send.at[j], x_recv.at[j]):
                copy.start()
        else:
            for block in range(4):
                for m, value in enumerate(segments(i, total[block])):
                    y_send[j, m, block] = value.astype(BF)
            start_y(i, y_send.at[j], y_recv.at[j])

    def start_second(i):
        j = i // 2
        if i % 2 == 0:
            for copy in x_copies(i, x_send.at[j], x_recv.at[j]):
                copy.wait()
            total = x_own[j, xi]
            for step in (1, 2, 3):
                total = total + x_recv[j, step - 1].astype(F32)
            for m, value in enumerate(segments(i, total)):
                y_send2[j, m] = value.astype(BF)
            start_y(4 + j, y_send2.at[j], y_recv2.at[j])
        else:
            total = end_y(i, y_send.at[j], y_recv.at[j])
            x_own2[j] = total
            x_send2[j] = total.astype(BF)
            for copy in x_copies(4 + j, x_send2.at[j], x_recv2.at[j]):
                copy.start()

    def z_copy(j, step):
        return pltpu.make_async_remote_copy(
            src_ref=z_send.at[j, (z + step) % 16], dst_ref=z_recv.at[j, step - 1],
            send_sem=z_ssem.at[j, step - 1], recv_sem=z_rsem.at[j, step - 1],
            device_id=z_id(step),
        )

    z_steps = sorted(range(1, 16), key=lambda step: -min(step, 16 - step))

    def start_z(j):
        first = end_y(4 + j, y_send2.at[j], y_recv2.at[j])
        for copy in x_copies(4 + j, x_send2.at[j], x_recv2.at[j]):
            copy.wait()
        second = x_own2[j, xi]
        for step in (1, 2, 3):
            second = second + x_recv2[j, step - 1].astype(F32)
        for t in range(3):
            lanes = slice(128 * t, 128 * t + 128)
            z_line[j, pl.ds(t, 16, stride=8), :] = first[:, lanes]
            z_line[j, pl.ds(t + 3, 16, stride=8), :] = second[:, lanes]
        for t in (6, 7):
            z_line[j, pl.ds(t, 16, stride=8), :] = jnp.zeros((16, 128), F32)
        z_send[j] = z_line[j].reshape(16, 8, 128).astype(BF)
        for step in z_steps:
            z_copy(j, step).start()

    def end_z(j):
        total = z_send[j, z].astype(F32)
        for step in z_steps[::-1]:
            z_copy(j, step).wait()
            total = total + z_recv[j, step - 1].astype(F32)
        share_ref[8 * j : 8 * j + 8] = total

    scores_back(2, 3)
    exchange(2, west_id).wait()
    widen_reach(2)
    branch_grad[192:256] = ex_recv[2]
    outer[192:256] = mm_t(ex_recv[2], w_out[...]).astype(BF)
    start_core(0, mm(left_o[...], branch_grad[...]))
    values_back(0, 1, 2, 3)
    start_core(1, mm(left_r[...], proj_grad[:, 2 * C : 3 * C]))
    start_first(0)
    scores_back(0, 1)
    start_first(1)
    start_core(2, mm(left_r[...], proj_grad[:, 0:C]))
    start_core(3, mm(left_r[...], proj_grad[:, C : 2 * C]))
    east_grad = mm_t(proj_grad[192:256], w_attend[...])
    east_grad = normalize_back(normed_east[...], std_east[...], east_grad)
    ex_send[3] = east_grad.astype(BF)
    exchange(3, east_id).start()
    start_first(2)
    start_first(3)
    copies["to_window_t"].wait()
    own_proj = mm(to_window_t[:, 0:192], proj_grad[0:192]).astype(BF)
    own_grad = mm_t(own_proj, w_attend[...])
    own_grad = normalize_back(normed_scr[...], std_scr[...], own_grad)
    feature_scr[...] = hidden_own + own_grad

    def end_features():
        exchange(3, east_id).wait()
        grad = feature_scr[...] + mm(to_window_t[:, 192:256], ex_recv[3])
        grad = grad.reshape(14, 16, C)
        for row in range(14):
            grad_ref[row] = grad[row, 0:14].astype(BF)

    if scatter:
        for group in range(4):
            start_second(group)
        start_z(0)
        start_z(1)
        end_features()
        end_z(0)
        end_z(1)
    else:
        end_features()
        share_ref[...] = jnp.zeros_like(share_ref)
        local_ref[...] = g_own[...]


def finish(merged_in, grad_in, share, merged_ref, grad_ref, attend_ref, output_ref):
    merged_ref[0] = merged_in[...]
    grad_ref[0] = grad_in[...]
    lane = lax.broadcasted_iota(jnp.int32, (1, 128), 1)

    def put(ref, pieces):
        lines = [jnp.zeros((1, 128), F32) for _ in range(-(-ref.shape[0] // 128))]
        start = 0
        for first, width in pieces:
            skip, turn = divmod(start, 128)
            values = [share[first + i : first + i + 1, :] for i in range(3)]
            if turn:
                values = [pltpu.roll(value, turn, 1) for value in values]
            for j in range(skip, (start + width - 1) // 128 + 1):
                value = values[min(j - skip, 2)]
                if turn and j > skip:
                    value = jnp.where(lane < turn, values[j - skip - 1], value)
                at = lane + 128 * j
                inside = jnp.logical_and(at >= start, at < start + width)
                lines[j] = jnp.where(inside, value, lines[j])
            start += width
        for j, value in enumerate(lines):
            count = min(128, ref.shape[0] - 128 * j)
            ref[128 * j : 128 * j + count] = value.reshape(128)[:count]

    put(output_ref, ((0, 288),))
    v, q, k = 3, 8, 11
    segment = 2 * (lax.axis_index("frame_1") % 2) + lax.axis_index("frame_2")
    for m, pieces in enumerate((
        ((q, 384), (k, 384), (v, 96)),
        ((v, 288), (q, 384), (k, 192)),
        ((k, 192), (v, 384), (q, 288)),
        ((q, 96), (k, 384), (v, 384)),
    )):
        pl.when(segment == m)(functools.partial(put, attend_ref, pieces))


def local_call(scatter, features, position_bias, attend_weight, output_weight, merge_weight, cotangent):
    given = (features[0], cotangent[0], position_bias.T, attend_weight, output_weight, merge_weight)
    given = given + tuple(jnp.asarray(table) for table in tables())
    dma = pltpu.SemaphoreType.DMA
    scratch = [pltpu.VMEM(a.shape, a.dtype) for a in given]
    scratch += [
        pltpu.VMEM((14, 16, C), F32),
        pltpu.VMEM((8, 8, OUT), F32),
        pltpu.VMEM((16, 256), F32),
        pltpu.VMEM((1024, 128), F32),
        pltpu.VMEM((1024, 128), F32),
        pltpu.VMEM((224, C), F32),
        pltpu.VMEM((224, 1), F32),
        pltpu.VMEM((64, C), F32),
        pltpu.VMEM((64, 1), F32),
        pltpu.VMEM((256, 3 * C), BF),
        pltpu.VMEM((12, 64, 256), F32),
        pltpu.VMEM((256, C), BF),
        pltpu.VMEM((256, C), BF),
        pltpu.VMEM((256, C), BF),
        pltpu.VMEM((256, 3 * C), BF),
        pltpu.VMEM((256, C), BF),
        pltpu.VMEM((C, 256), BF),
        pltpu.VMEM((C, 256), BF),
        pltpu.VMEM((224, C), F32),
        pltpu.VMEM((4, 64, C), BF),
        pltpu.VMEM((4, 64, C), BF),
        pltpu.VMEM((4, 2, 192, C), F32),
        pltpu.VMEM((4, 2, 192, C), BF),
        pltpu.VMEM((4, 192, C), BF),
        pltpu.VMEM((2, 4, 48, C), F32),
        pltpu.VMEM((2, 4, 48, C), BF),
        pltpu.VMEM((2, 3, 48, C), BF),
        pltpu.VMEM((2, 4, 4, 16, C), BF),
        pltpu.VMEM((2, 4, 4, 16, C), BF),
        pltpu.VMEM((2, 4, 16, C), F32),
        pltpu.VMEM((2, 4, 16, C), BF),
        pltpu.VMEM((2, 3, 16, C), BF),
        pltpu.VMEM((2, 4, 16, C), BF),
        pltpu.VMEM((2, 4, 16, C), BF),
        pltpu.VMEM((2, 128, 128), F32),
        pltpu.VMEM((2, 16, 8, 128), BF),
        pltpu.VMEM((2, 15, 8, 128), BF),
        dma((N_IN,)), dma((4,)), dma((4,)), dma((4,)), dma((4,)), dma((6, 3)), dma((6, 3)),
        dma((6, 4)), dma((6, 4)), dma((2, 15)), dma((2, 15)), pltpu.SemaphoreType.REGULAR((3,)),
    ]
    vmem = pl.BlockSpec(memory_space=pltpu.VMEM)
    return pl.pallas_call(
        functools.partial(kernel, scatter),
        out_shape=(
            pltpu.VMEM((7, 7, OUT), BF),
            pltpu.VMEM((14, 14, C), BF),
            pltpu.VMEM((16, 128), F32),
        )
        + (() if scatter else (jax.ShapeDtypeStruct((4, 2, 192, C), F32),)),
        in_specs=[pl.BlockSpec(memory_space=pl.ANY)] * N_IN,
        out_specs=(vmem,) * (3 if scatter else 4),
        scratch_shapes=scratch,
        compiler_params=pltpu.CompilerParams(collective_id=0, has_side_effects=True),
    )(*given)


def per_device(*arrays):
    merged, feature_grad, share = local_call(True, *arrays)
    vmem = pl.BlockSpec(memory_space=pltpu.VMEM)
    return pl.pallas_call(
        finish,
        out_shape=(
            jax.ShapeDtypeStruct((1, *merged.shape), BF),
            jax.ShapeDtypeStruct((1, *feature_grad.shape), BF),
            jax.ShapeDtypeStruct((864,), F32),
            jax.ShapeDtypeStruct((288,), F32),
        ),
        in_specs=(vmem,) * 3,
        out_specs=(vmem,) * 4,
        compiler_params=pltpu.CompilerParams(vmem_limit_bytes=8 << 20),
    )(merged, feature_grad, share)


def solution(mesh):
    split = Mesh(mesh.devices.reshape(16, 2, 2, 4, 2), AZIM_FRAME)
    placed = (P(FRAME, None, AZIM, None), P(), P(), P(), P(), P(FRAME, None, AZIM, None))
    return jax.shard_map(
        per_device,
        mesh=split,
        in_specs=placed,
        out_specs=(
            P(FRAME, None, AZIM, None),
            P(FRAME, None, AZIM, None),
            P(AZIM_FRAME),
            P(AZIM_FRAME),
        ),
        check_vma=False,
    )
```

```python
import functools

import jax
import jax.numpy as jnp
import ml_dtypes
import numpy as np
from jax import lax
from jax.experimental import pallas as pl
from jax.experimental.pallas import tpu as pltpu
from jax.sharding import Mesh
from jax.sharding import PartitionSpec as P

AZIM = ("azim_0", "azim_1")
AZIM_FRAME = ("azim_0", "azim_1", "frame_0", "frame_1", "frame_2")
FRAME = ("frame_0", "frame_1", "frame_2")

BF = jnp.bfloat16
F32 = jnp.float32
C = 384
OUT = 768
GROUPS = 3
SCALE = 32 ** (-0.5)
WINDOWS = ((0, 1), (1, 1), (0, 0), (1, 0))


def position_row(row, col):
    return 4 * row + col if col < 4 else 32 + 3 * row + col - 4


def east_row(row, col):
    rolled = (row - 3) % 14
    return 32 * (rolled // 7) + 3 * (rolled % 7) + col


@functools.cache
def tables():
    to_window = np.zeros((256, 224), np.float32)
    for a in range(2):
        for b in range(2):
            for row in range(7):
                for col in range(7):
                    frame_row, frame_col = (7 * a + row + 3) % 14, 7 * b + col + 3
                    if frame_col >= 14:
                        continue
                    at = position_row(row, col)
                    line = 64 * a + at if b == 0 else 128 + 32 * a + at
                    to_window[line, 16 * frame_row + frame_col] = 1
    for row in range(14):
        for col in range(3):
            to_window[192 + east_row(row, col), 16 * row + col] = 1
    to_quad = np.zeros((256, 224), np.float32)
    for block in range(4):
        for i in range(7):
            for j in range(7):
                token = 16 * (2 * i + block % 2) + 2 * j + block // 2
                to_quad[64 * block + 8 * i + j, token] = 1
    window_to_quad = to_quad @ to_window.T
    rows = np.zeros((C, C), np.float32)
    for c in range(2):
        for xi in range(4):
            for k in range(3):
                for z in range(16):
                    rows[192 * c + 48 * xi + 16 * k + z, 24 * z + 6 * xi + 3 * c + k] = 1
    index = np.full((64, 64), 255.0, np.float32)
    mask = np.zeros((2, 64, 64), np.float32)
    valid = np.zeros(64, bool)
    for row in range(7):
        for col in range(7):
            p = position_row(row, col)
            valid[p] = True
            for row_q in range(7):
                for col_q in range(7):
                    q = position_row(row_q, col_q)
                    index[p, q] = 13 * (row - row_q + 6) + col - col_q + 6
                    if (row < 4) != (row_q < 4):
                        mask[1, p, q] = -100.0
    mask[:, :, ~valid] = -1e30
    mask = np.concatenate([mask, mask], -1)
    bf = ml_dtypes.bfloat16
    return (
        to_window.astype(bf),
        np.ascontiguousarray(to_window.T).astype(bf),
        to_quad.astype(bf),
        np.ascontiguousarray(to_quad.T).astype(bf),
        window_to_quad.astype(bf),
        np.ascontiguousarray(window_to_quad.T).astype(bf),
        rows.astype(bf),
        index.reshape(32, 128),
        mask,
    )


def mm(left, right):
    return lax.dot_general(left, right, (((1,), (0,)), ((), ())), preferred_element_type=F32)


def mm_t(left, right):
    return lax.dot_general(left, right, (((1,), (1,)), ((), ())), preferred_element_type=F32)


def t_mm(left, right):
    return lax.dot_general(left, right, (((0,), (0,)), ((), ())), preferred_element_type=F32)


def normalize(values):
    centred = values - jnp.mean(values, -1, keepdims=True)
    inverse_std = lax.rsqrt(jnp.mean(centred * centred, -1, keepdims=True) + 1e-05)
    return centred * inverse_std, inverse_std


def normalize_back(normed, inverse_std, grads):
    first = jnp.mean(grads, -1, keepdims=True)
    second = jnp.mean(grads * normed, -1, keepdims=True)
    return inverse_std * (grads - first - normed * second)


def window_of(values, a, b):
    if b == 0:
        return values[64 * a : 64 * a + 64]
    near, far = 128 + 32 * a, 192 + 32 * a
    return jnp.concatenate([values[near : near + 32], values[far : far + 32]], 0)


def put_window(ref, a, b, lanes, values):
    if b == 0:
        ref[64 * a : 64 * a + 64, lanes] = values
    else:
        near, far = 128 + 32 * a, 192 + 32 * a
        ref[near : near + 32, lanes] = values[:32]
        ref[far : far + 32, lanes] = values[32:]


def get_window(ref, a, b, lanes):
    if b == 0:
        return ref[64 * a : 64 * a + 64, lanes]
    near, far = 128 + 32 * a, 192 + 32 * a
    return jnp.concatenate([ref[near : near + 32, lanes], ref[far : far + 32, lanes]], 0)


def halves(op, empty, low, values):
    first = op(jnp.where(low, values, empty), -1, keepdims=True)
    second = op(jnp.where(low, empty, values), -1, keepdims=True)
    return jnp.where(low, first, second)


NAMES = (
    "feat", "cot", "pos", "w_attend", "w_out", "w_merge", "to_window", "to_window_t", "to_quad",
    "to_quad_t", "win_quad", "win_quad_t", "row_pick", "index", "mask",
)
ORDER = (
    "feat", "to_window", "w_attend", "pos", "index", "mask", "cot", "w_merge", "row_pick",
    "to_quad", "win_quad", "w_out", "win_quad_t", "to_quad_t", "to_window_t",
)
N_IN = len(NAMES)


def kernel(scatter, *refs):
    given, refs = refs[:N_IN], refs[N_IN:]
    merged_ref, grad_ref, share_ref = refs[:3]
    if scatter:
        refs = refs[3:]
    else:
        local_ref, refs = refs[3], refs[4:]
    held, refs = refs[:N_IN], refs[N_IN:]
    (
        x_scr, cot_scr, table_scr, bias_a, bias_b, normed_scr, std_scr,
        normed_east, std_east, qkv, probs, attended, branch_grad, outer, proj_grad,
        hidden_grad, left_o, left_r, feature_scr, first_scr,
        ex_send, ex_recv,
        g_own, g_send, g_recv, x_own, x_send, x_recv, y_send, y_recv,
        x_own2, x_send2, x_recv2, y_send2, y_recv2, z_line, z_send, z_recv,
        in_sem, ex_ssem, ex_rsem, c_ssem, c_rsem, x_ssem, x_rsem, y_ssem, y_rsem,
        z_ssem, z_rsem, near_sem,
    ) = refs
    (
        feat, cot, pos, w_attend, w_out, w_merge, to_window, to_window_t, to_quad, to_quad_t,
        win_quad, win_quad_t, row_pick, index, mask,
    ) = held
    copies = {
        name: pltpu.make_async_copy(given[i], held[i], in_sem.at[i])
        for i, name in enumerate(NAMES)
    }
    for name in ORDER[:2]:
        copies[name].start()

    z, x_lo = lax.axis_index("azim_0"), lax.axis_index("azim_1")
    x_hi, y, core = (lax.axis_index(name) for name in FRAME)
    n_z = lax.axis_size("azim_0")
    n_azim = n_z * 2
    azim = 2 * z + x_lo
    east, west = (azim + 1) % n_azim, (azim + n_azim - 1) % n_azim
    east_id = {"azim_0": east // 2, "azim_1": east % 2}
    west_id = {"azim_0": west // 2, "azim_1": west % 2}
    xi = 2 * x_lo + x_hi

    def x_id(step):
        other = (xi + step) % 4
        return {"azim_1": other // 2, "frame_0": other % 2}

    def z_id(step):
        return {"azim_0": (z + n_z + step) % n_z}

    barrier = pltpu.get_barrier_semaphore()
    near = [east_id, west_id]
    if scatter:
        near += [{"frame_2": 1 - core}]
        near += [x_id(step) for step in (1, 2, 3)]
        near += [{"frame_1": (y + step) % 4} for step in (1, 2, 3)]
        near += [{"frame_1": (y + step) % 4, "frame_2": 1 - core} for step in (1, 2, 3)]
        near += [z_id(1), z_id(-1)]
    for device in near:
        pl.semaphore_signal(barrier, inc=1, device_id=device)

    def exchange(i, device):
        return pltpu.make_async_remote_copy(
            src_ref=ex_send.at[i], dst_ref=ex_recv.at[i], send_sem=ex_ssem.at[i],
            recv_sem=ex_rsem.at[i], device_id=device,
        )

    for name in ORDER[2:7]:
        copies[name].start()
    copies["feat"].wait()
    for name in ORDER[7:]:
        copies[name].start()
    x_scr[...] = jnp.zeros_like(x_scr)
    for row in range(14):
        x_scr[row, 0:14, :] = feat[row].astype(F32)
    tokens = x_scr[...].reshape(224, C)
    tokens16 = tokens.astype(BF)
    copies["to_window"].wait()
    shared = mm(to_window[128:256], tokens16).astype(BF)
    ex_send[0] = shared[64:128]
    ex_send[1] = shared[0:64]
    pl.semaphore_wait(barrier, len(near))
    exchange(0, west_id).start()
    exchange(1, east_id).start()
    if scatter:
        for step in (1, -1):
            pl.semaphore_signal(near_sem.at[0], inc=1, device_id=z_id(step))

    def widen_reach(i):
        if not scatter:
            return
        pl.semaphore_wait(near_sem.at[i], 2)
        if i < 2:
            for step in (2 ** (i + 1), -(2 ** (i + 1))):
                pl.semaphore_signal(near_sem.at[i + 1], inc=1, device_id=z_id(step))

    normed, inverse_std = normalize(tokens)
    normed_scr[...] = normed
    std_scr[...] = inverse_std
    rolled = mm(to_window[...], normed.astype(BF)).astype(BF)
    rolled_own = rolled[0:192]
    copies["w_attend"].wait()
    projected = mm(rolled, w_attend[...]).astype(BF)
    qkv[0:192] = projected[0:192]
    qkv[320:384] = projected[192:256]

    copies["pos"].wait()
    copies["index"].wait()
    copies["mask"].wait()
    table_scr[...] = jnp.zeros_like(table_scr)
    table_scr[0:12, 0:169] = pos[...]
    table = table_scr[...]
    high = table.astype(BF).astype(F32)
    both = jnp.concatenate([high, table - high], 0).astype(BF)
    lane = lax.broadcasted_iota(jnp.int32, (1, 128), 1)
    entry = lax.broadcasted_iota(jnp.int32, (256, 128), 0).astype(F32)
    for t in range(0, 32, 4):
        picks = [
            jnp.where(entry == index[u : u + 1, :], 1.0, 0.0).astype(BF) for u in range(t, t + 4)
        ]
        wide = mm(both, jnp.concatenate(picks, 1))
        for u in range(4):
            part = wide[:, 128 * u : 128 * u + 128]
            part = part[0:16] + part[16:32]
            turned = pltpu.roll(part, 64, 1)
            p = 2 * (t + u)
            bias_a[pl.ds(p, 16, stride=64), :] = part
            bias_a[pl.ds(p + 1, 16, stride=64), :] = turned
            bias_b[pl.ds(p, 16, stride=64), :] = turned
            bias_b[pl.ds(p + 1, 16, stride=64), :] = part
    low = lane < 64

    def pair_bias(pair):
        first = bias_a[128 * pair : 128 * pair + 64, :]
        second = bias_b[128 * pair + 64 : 128 * pair + 128, :]
        return jnp.where(low, first, second)

    copies["cot"].wait()
    cot_scr[...] = jnp.zeros_like(cot_scr)
    for row in range(7):
        cot_scr[row, 0:7, :] = cot[row].astype(F32)
    copies["w_merge"].wait()
    quad_grad_in = mm_t(cot_scr[...].reshape(64, OUT).astype(BF), w_merge[...])

    head_lanes = [(lane // 32 == h).astype(F32).astype(BF) for h in range(4)]

    def spread(block):
        return jnp.concatenate([block * head_lanes[h] for h in range(4)], 0)

    def heads_of(wide):
        total = wide[0:64] * head_lanes[0].astype(F32)
        for h in range(1, 4):
            total = total + wide[64 * h : 64 * h + 64] * head_lanes[h].astype(F32)
        return total

    def group_lanes(kind, group):
        start = C * kind + 128 * group
        return slice(start, start + 128)

    def units_of(windows):
        return [(w, group) for w in windows for group in range(GROUPS)]

    def of_window(ref, w, kind, group):
        return get_window(ref, *WINDOWS[w], group_lanes(kind, group))

    ones = (lax.broadcasted_iota(jnp.int32, (128, 128), 0) < 64) == low
    ones = ones.astype(F32).astype(BF)

    def half_sums(values):
        rows = values[0].shape[0]
        joined = jnp.concatenate(values, 0)
        high = joined.astype(BF)
        rest = (joined - high.astype(F32)).astype(BF)
        total = mm(high, ones) + mm(rest, ones)
        return [total[rows * i : rows * i + rows] for i in range(len(values))]

    def split_halves(wide):
        return [part[:, 128 * i : 128 * i + 128] for part in wide for i in range(2)]

    def join_halves(parts):
        return [
            jnp.concatenate([parts[i].astype(BF), parts[i + 1].astype(BF)], 1)
            for i in range(0, len(parts), 2)
        ]

    def softmax(units, scores, rows):
        parts = split_halves(scores)
        for i, (a, g) in enumerate(units):
            for j in range(2):
                bias = pair_bias(2 * g + j)[rows] + mask[a, rows]
                parts[2 * i + j] = parts[2 * i + j] * SCALE + bias
        tops = [halves(jnp.max, -3e38, low, part) for part in parts]
        parts = [jnp.exp(part - top) for part, top in zip(parts, tops)]
        sums = half_sums(parts)
        return [part * (1.0 / total) for part, total in zip(parts, sums)]

    def attend(*windows):
        units = units_of(windows)
        scores = [
            mm_t(of_window(qkv, w, 0, g), spread(of_window(qkv, w, 1, g))) for w, g in units
        ]
        parts = softmax([(WINDOWS[w][0], g) for w, g in units], scores, slice(0, 64))
        for i, (w, g) in enumerate(units):
            for j in range(2):
                probs[GROUPS * w + g, :, 128 * j : 128 * j + 128] = parts[2 * i + j]
        for (w, g), prob in zip(units, join_halves(parts)):
            result = mm(prob, spread(of_window(qkv, w, 2, g))).astype(BF)
            put_window(attended, *WINDOWS[w], group_lanes(0, g), result)

    def attend_first():
        units = [(a, g) for a in range(2) for g in range(GROUPS)]

        def part(a, kind, g):
            lanes = group_lanes(kind, g)
            near, far = 256 + 32 * a, 320 + 32 * a
            return jnp.concatenate([qkv[near : near + 32, lanes], qkv[far : far + 32, lanes]], 0)

        scores = [
            mm_t(qkv[320 + 32 * a : 352 + 32 * a, group_lanes(0, g)], spread(part(a, 1, g)))
            for a, g in units
        ]
        parts = softmax(units, scores, slice(32, 64))
        for (a, g), prob in zip(units, join_halves(parts)):
            result = mm(prob, spread(part(a, 2, g))).astype(BF)
            first_scr[32 * a : 32 * a + 32, group_lanes(0, g)] = result

    attend(2, 3)

    exchange(0, west_id).wait()
    exchange(1, east_id).wait()
    widen_reach(0)
    normed, inverse_std = normalize(ex_recv[0:2].astype(F32).reshape(128, C))
    normed_east[...] = normed[0:64]
    std_east[...] = inverse_std[0:64]
    rolled = normed.astype(BF)
    rolled_east = rolled[0:64]
    qkv[192:320] = mm(rolled, w_attend[...]).astype(BF)
    attend_first()
    attend(0, 1)
    copies["to_quad"].wait()
    copies["win_quad"].wait()
    copies["w_out"].wait()
    features_quad = mm(to_quad[...], tokens16)
    widen_reach(1)

    extended = jnp.concatenate([attended[0:192], first_scr[...]], 0)
    attended_quad = mm(win_quad[...], extended).astype(BF)
    hidden = (features_quad + mm(attended_quad, w_out[...])).astype(BF).astype(F32)
    quads = [hidden[64 * e : 64 * e + 64] for e in range(4)]

    def mean(blocks):
        total = (blocks[0] + blocks[1]) + (blocks[2] + blocks[3])
        return jnp.sum(total, -1, keepdims=True) * (1.0 / (4 * C))

    centre = mean(quads)
    quads = [quad - centre for quad in quads]
    quad_std = lax.rsqrt(mean([quad * quad for quad in quads]) + 1e-05)
    quads = [quad * quad_std for quad in quads]
    grads = [quad_grad_in[:, C * e : C * e + C] for e in range(4)]
    first = mean(grads)
    second = mean([grad * quad for grad, quad in zip(grads, quads)])
    for e in range(4):
        value = quad_std * (grads[e] - first - quads[e] * second)
        hidden_grad[64 * e : 64 * e + 64] = value.astype(BF)
    copies["win_quad_t"].wait()
    ex_send[2] = mm(win_quad_t[192:256], hidden_grad[...]).astype(BF)
    exchange(2, west_id).start()
    copies["row_pick"].wait()
    left_r[:, 0:192] = mm_t(row_pick[...], rolled_own).astype(BF)
    left_r[:, 192:256] = mm_t(row_pick[...], rolled_east).astype(BF)
    left_o[...] = mm_t(row_pick[...], attended[...]).astype(BF)
    own_grad = mm(win_quad_t[0:192], hidden_grad[...]).astype(BF)
    branch_grad[0:192] = own_grad
    outer[0:192] = mm_t(own_grad, w_out[...]).astype(BF)
    merged = mm(jnp.concatenate([quad.astype(BF) for quad in quads], 1), w_merge[...])
    for i in range(7):
        merged_ref[i] = merged[8 * i : 8 * i + 7].astype(BF)
    copies["to_quad_t"].wait()
    hidden_own = mm(to_quad_t[...], hidden_grad[...])

    def values_back(*windows):
        units = units_of(windows)
        wide = [
            t_mm(probs[GROUPS * w + g].astype(BF), of_window(outer, w, 0, g)) for w, g in units
        ]
        for (w, g), value in zip(units, wide):
            back = heads_of(value).astype(BF)
            put_window(proj_grad, *WINDOWS[w], group_lanes(2, g), back)

    def scores_back(*windows):
        units = units_of(windows)
        wide = [
            mm_t(of_window(outer, w, 0, g), spread(of_window(qkv, w, 2, g))) for w, g in units
        ]
        grads = split_halves(wide)
        prob = split_halves([probs[GROUPS * w + g] for w, g in units])
        sums = half_sums([p * grad for p, grad in zip(prob, grads)])
        parts = [p * (grad - total) * SCALE for p, grad, total in zip(prob, grads, sums)]
        soft = join_halves(parts)
        wide = [t_mm(part, of_window(qkv, w, 0, g)) for (w, g), part in zip(units, soft)]
        for (w, g), part in zip(units, soft):
            back = mm(part, spread(of_window(qkv, w, 1, g))).astype(BF)
            put_window(proj_grad, *WINDOWS[w], group_lanes(0, g), back)
        for (w, g), value in zip(units, wide):
            back = heads_of(value).astype(BF)
            put_window(proj_grad, *WINDOWS[w], group_lanes(1, g), back)

    def core_copy(i):
        return pltpu.make_async_remote_copy(
            src_ref=g_send.at[i, 1 - core], dst_ref=g_recv.at[i], send_sem=c_ssem.at[i],
            recv_sem=c_rsem.at[i], device_id={"frame_2": 1 - core},
        )

    def start_core(i, product):
        product = product.reshape(2, 192, C)
        g_own[i] = product
        if scatter:
            g_send[i] = product.astype(BF)
            core_copy(i).start()

    def x_copies(i, sent, landing):
        return [
            pltpu.make_async_remote_copy(
                src_ref=sent.at[(xi + step) % 4], dst_ref=landing.at[step - 1],
                send_sem=x_ssem.at[i, step - 1], recv_sem=x_rsem.at[i, step - 1],
                device_id=x_id(step),
            )
            for step in (2, 1, 3)
        ]

    def y_copy(i, m, sent, landing):
        return pltpu.make_async_remote_copy(
            src_ref=sent.at[m], dst_ref=landing.at[y], send_sem=y_ssem.at[i, m],
            recv_sem=y_rsem.at[i, y],
            device_id={"frame_1": 2 * core + m // 2, "frame_2": m % 2},
        )

    def y_landed(i, source, sent, landing):
        return pltpu.make_async_remote_copy(
            src_ref=sent.at[0], dst_ref=landing.at[source], send_sem=y_ssem.at[i, 0],
            recv_sem=y_rsem.at[i, source], device_id={"frame_2": 1 - core},
        )

    def stays(m):
        return jnp.logical_and(2 * core + m // 2 == y, core == m % 2)

    def start_y(i, sent, landing):
        for m in range(4):

            @pl.when(stays(m))
            def _():
                landing[y] = sent[m]

            @pl.when(jnp.logical_not(stays(m)))
            def _():
                y_copy(i, m, sent, landing).start()

    def end_y(i, sent, landing):
        for source in range(4):
            mine = jnp.logical_and(y == source, y // 2 == core)

            @pl.when(jnp.logical_not(mine))
            def _():
                y_landed(i, source, sent, landing).wait_recv()

        for m in range(4):

            @pl.when(jnp.logical_not(stays(m)))
            def _():
                y_copy(i, m, sent, landing).wait_send()

        total = landing[0].astype(F32)
        for source in range(1, 4):
            total = total + landing[source].astype(F32)
        return total

    wide_lane = lax.broadcasted_iota(jnp.int32, (1, C), 1)

    def segments(i, block):
        one, two, three = (block[16 * k : 16 * k + 16] for k in range(3))

        def left(value, count):
            return pltpu.roll(value, C - count, 1)

        if i == 0:
            second = jnp.where(wide_lane < 96, left(one, 288), pltpu.roll(two, 96, 1))
            third = jnp.where(wide_lane < 192, left(two, 192), pltpu.roll(three, 192, 1))
            return one, second, third, left(three, 96)
        if i == 1:
            return one, left(one, 96), two, three
        if i == 2:
            return one, two, three, left(three, 288)
        return one, two, left(two, 192), three

    def start_first(i):
        if not scatter:
            return
        core_copy(i).wait()
        total = (g_own[i, core] + g_recv[i].astype(F32)).reshape(4, 48, C)
        j = i // 2
        if i % 2 == 0:
            x_own[j] = total
            x_send[j] = total.astype(BF)
            for copy in x_copies(i, x_send.at[j], x_recv.at[j]):
                copy.start()
        else:
            for block in range(4):
                for m, value in enumerate(segments(i, total[block])):
                    y_send[j, m, block] = value.astype(BF)
            start_y(i, y_send.at[j], y_recv.at[j])

    def start_second(i):
        j = i // 2
        if i % 2 == 0:
            for copy in x_copies(i, x_send.at[j], x_recv.at[j]):
                copy.wait()
            total = x_own[j, xi]
            for step in (1, 2, 3):
                total = total + x_recv[j, step - 1].astype(F32)
            for m, value in enumerate(segments(i, total)):
                y_send2[j, m] = value.astype(BF)
            start_y(4 + j, y_send2.at[j], y_recv2.at[j])
        else:
            total = end_y(i, y_send.at[j], y_recv.at[j])
            x_own2[j] = total
            x_send2[j] = total.astype(BF)
            for copy in x_copies(4 + j, x_send2.at[j], x_recv2.at[j]):
                copy.start()

    def z_copy(j, step):
        return pltpu.make_async_remote_copy(
            src_ref=z_send.at[j, (z + step) % 16], dst_ref=z_recv.at[j, step - 1],
            send_sem=z_ssem.at[j, step - 1], recv_sem=z_rsem.at[j, step - 1],
            device_id=z_id(step),
        )

    z_steps = sorted(range(1, 16), key=lambda step: -min(step, 16 - step))

    def start_z(j):
        first = end_y(4 + j, y_send2.at[j], y_recv2.at[j])
        for copy in x_copies(4 + j, x_send2.at[j], x_recv2.at[j]):
            copy.wait()
        second = x_own2[j, xi]
        for step in (1, 2, 3):
            second = second + x_recv2[j, step - 1].astype(F32)
        for t in range(3):
            lanes = slice(128 * t, 128 * t + 128)
            z_line[j, pl.ds(t, 16, stride=8), :] = first[:, lanes]
            z_line[j, pl.ds(t + 3, 16, stride=8), :] = second[:, lanes]
        for t in (6, 7):
            z_line[j, pl.ds(t, 16, stride=8), :] = jnp.zeros((16, 128), F32)
        z_send[j] = z_line[j].reshape(16, 8, 128).astype(BF)
        for step in z_steps:
            z_copy(j, step).start()

    def end_z(j):
        total = z_send[j, z].astype(F32)
        for step in z_steps[::-1]:
            z_copy(j, step).wait()
            total = total + z_recv[j, step - 1].astype(F32)
        share_ref[8 * j : 8 * j + 8] = total

    scores_back(2, 3)
    exchange(2, west_id).wait()
    widen_reach(2)
    branch_grad[192:256] = ex_recv[2]
    outer[192:256] = mm_t(ex_recv[2], w_out[...]).astype(BF)
    start_core(0, mm(left_o[...], branch_grad[...]))
    values_back(0, 1, 2, 3)
    start_core(1, mm(left_r[...], proj_grad[:, 2 * C : 3 * C]))
    start_first(0)
    scores_back(0, 1)
    start_first(1)
    start_core(2, mm(left_r[...], proj_grad[:, 0:C]))
    start_core(3, mm(left_r[...], proj_grad[:, C : 2 * C]))
    east_grad = mm_t(proj_grad[192:256], w_attend[...])
    east_grad = normalize_back(normed_east[...], std_east[...], east_grad)
    ex_send[3] = east_grad.astype(BF)
    exchange(3, east_id).start()
    start_first(2)
    start_first(3)
    copies["to_window_t"].wait()
    own_proj = mm(to_window_t[:, 0:192], proj_grad[0:192]).astype(BF)
    own_grad = mm_t(own_proj, w_attend[...])
    own_grad = normalize_back(normed_scr[...], std_scr[...], own_grad)
    feature_scr[...] = hidden_own + own_grad

    def end_features():
        exchange(3, east_id).wait()
        grad = feature_scr[...] + mm(to_window_t[:, 192:256], ex_recv[3])
        grad = grad.reshape(14, 16, C)
        for row in range(14):
            grad_ref[row] = grad[row, 0:14].astype(BF)

    if scatter:
        for group in range(4):
            start_second(group)
        start_z(0)
        start_z(1)
        end_features()
        end_z(0)
        end_z(1)
    else:
        end_features()
        share_ref[...] = jnp.zeros_like(share_ref)
        local_ref[...] = g_own[...]


def finish(merged_in, grad_in, share, merged_ref, grad_ref, attend_ref, output_ref):
    merged_ref[0] = merged_in[...]
    grad_ref[0] = grad_in[...]
    lane = lax.broadcasted_iota(jnp.int32, (1, 128), 1)

    def put(ref, pieces):
        lines = [jnp.zeros((1, 128), F32) for _ in range(-(-ref.shape[0] // 128))]
        start = 0
        for first, width in pieces:
            skip, turn = divmod(start, 128)
            values = [share[first + i : first + i + 1, :] for i in range(3)]
            if turn:
                values = [pltpu.roll(value, turn, 1) for value in values]
            for j in range(skip, (start + width - 1) // 128 + 1):
                value = values[min(j - skip, 2)]
                if turn and j > skip:
                    value = jnp.where(lane < turn, values[j - skip - 1], value)
                at = lane + 128 * j
                inside = jnp.logical_and(at >= start, at < start + width)
                lines[j] = jnp.where(inside, value, lines[j])
            start += width
        for j, value in enumerate(lines):
            count = min(128, ref.shape[0] - 128 * j)
            ref[128 * j : 128 * j + count] = value.reshape(128)[:count]

    put(output_ref, ((0, 288),))
    v, q, k = 3, 8, 11
    segment = 2 * (lax.axis_index("frame_1") % 2) + lax.axis_index("frame_2")
    for m, pieces in enumerate((
        ((q, 384), (k, 384), (v, 96)),
        ((v, 288), (q, 384), (k, 192)),
        ((k, 192), (v, 384), (q, 288)),
        ((q, 96), (k, 384), (v, 384)),
    )):
        pl.when(segment == m)(functools.partial(put, attend_ref, pieces))


def local_call(scatter, features, position_bias, attend_weight, output_weight, merge_weight, cotangent):
    given = (features[0], cotangent[0], position_bias.T, attend_weight, output_weight, merge_weight)
    given = given + tuple(jnp.asarray(table) for table in tables())
    dma = pltpu.SemaphoreType.DMA
    scratch = [pltpu.VMEM(a.shape, a.dtype) for a in given]
    scratch += [
        pltpu.VMEM((14, 16, C), F32),
        pltpu.VMEM((8, 8, OUT), F32),
        pltpu.VMEM((16, 256), F32),
        pltpu.VMEM((1024, 128), F32),
        pltpu.VMEM((1024, 128), F32),
        pltpu.VMEM((224, C), F32),
        pltpu.VMEM((224, 1), F32),
        pltpu.VMEM((64, C), F32),
        pltpu.VMEM((64, 1), F32),
        pltpu.VMEM((384, 3 * C), BF),
        pltpu.VMEM((12, 64, 256), F32),
        pltpu.VMEM((256, C), BF),
        pltpu.VMEM((256, C), BF),
        pltpu.VMEM((256, C), BF),
        pltpu.VMEM((256, 3 * C), BF),
        pltpu.VMEM((256, C), BF),
        pltpu.VMEM((C, 256), BF),
        pltpu.VMEM((C, 256), BF),
        pltpu.VMEM((224, C), F32),
        pltpu.VMEM((64, C), BF),
        pltpu.VMEM((4, 64, C), BF),
        pltpu.VMEM((4, 64, C), BF),
        pltpu.VMEM((4, 2, 192, C), F32),
        pltpu.VMEM((4, 2, 192, C), BF),
        pltpu.VMEM((4, 192, C), BF),
        pltpu.VMEM((2, 4, 48, C), F32),
        pltpu.VMEM((2, 4, 48, C), BF),
        pltpu.VMEM((2, 3, 48, C), BF),
        pltpu.VMEM((2, 4, 4, 16, C), BF),
        pltpu.VMEM((2, 4, 4, 16, C), BF),
        pltpu.VMEM((2, 4, 16, C), F32),
        pltpu.VMEM((2, 4, 16, C), BF),
        pltpu.VMEM((2, 3, 16, C), BF),
        pltpu.VMEM((2, 4, 16, C), BF),
        pltpu.VMEM((2, 4, 16, C), BF),
        pltpu.VMEM((2, 128, 128), F32),
        pltpu.VMEM((2, 16, 8, 128), BF),
        pltpu.VMEM((2, 15, 8, 128), BF),
        dma((N_IN,)), dma((4,)), dma((4,)), dma((4,)), dma((4,)), dma((6, 3)), dma((6, 3)),
        dma((6, 4)), dma((6, 4)), dma((2, 15)), dma((2, 15)), pltpu.SemaphoreType.REGULAR((3,)),
    ]
    vmem = pl.BlockSpec(memory_space=pltpu.VMEM)
    return pl.pallas_call(
        functools.partial(kernel, scatter),
        out_shape=(
            pltpu.VMEM((7, 7, OUT), BF),
            pltpu.VMEM((14, 14, C), BF),
            pltpu.VMEM((16, 128), F32),
        )
        + (() if scatter else (jax.ShapeDtypeStruct((4, 2, 192, C), F32),)),
        in_specs=[pl.BlockSpec(memory_space=pl.ANY)] * N_IN,
        out_specs=(vmem,) * (3 if scatter else 4),
        scratch_shapes=scratch,
        compiler_params=pltpu.CompilerParams(collective_id=0, has_side_effects=True),
    )(*given)


def per_device(*arrays):
    merged, feature_grad, share = local_call(True, *arrays)
    vmem = pl.BlockSpec(memory_space=pltpu.VMEM)
    return pl.pallas_call(
        finish,
        out_shape=(
            jax.ShapeDtypeStruct((1, *merged.shape), BF),
            jax.ShapeDtypeStruct((1, *feature_grad.shape), BF),
            jax.ShapeDtypeStruct((864,), F32),
            jax.ShapeDtypeStruct((288,), F32),
        ),
        in_specs=(vmem,) * 3,
        out_specs=(vmem,) * 4,
        compiler_params=pltpu.CompilerParams(vmem_limit_bytes=8 << 20),
    )(merged, feature_grad, share)


def solution(mesh):
    split = Mesh(mesh.devices.reshape(16, 2, 2, 4, 2), AZIM_FRAME)
    placed = (P(FRAME, None, AZIM, None), P(), P(), P(), P(), P(FRAME, None, AZIM, None))
    return jax.shard_map(
        per_device,
        mesh=split,
        in_specs=placed,
        out_specs=(
            P(FRAME, None, AZIM, None),
            P(FRAME, None, AZIM, None),
            P(AZIM_FRAME),
            P(AZIM_FRAME),
        ),
        check_vma=False,
    )
```

```python
import functools

import jax
import jax.numpy as jnp
import ml_dtypes
import numpy as np
from jax import lax
from jax.experimental import pallas as pl
from jax.experimental.pallas import tpu as pltpu
from jax.sharding import Mesh
from jax.sharding import PartitionSpec as P

AZIM = ("azim_0", "azim_1")
AZIM_FRAME = ("azim_0", "azim_1", "frame_0", "frame_1", "frame_2")
FRAME = ("frame_0", "frame_1", "frame_2")

BF = jnp.bfloat16
F32 = jnp.float32
C = 384
OUT = 768
GROUPS = 3
SCALE = 32 ** (-0.5)
WINDOWS = ((0, 1), (1, 1), (0, 0), (1, 0))


def position_row(row, col):
    return 4 * row + col if col < 4 else 32 + 3 * row + col - 4


def east_row(row, col):
    rolled = (row - 3) % 14
    return 32 * (rolled // 7) + 3 * (rolled % 7) + col


@functools.cache
def tables():
    to_window = np.zeros((256, 224), np.float32)
    for a in range(2):
        for b in range(2):
            for row in range(7):
                for col in range(7):
                    frame_row, frame_col = (7 * a + row + 3) % 14, 7 * b + col + 3
                    if frame_col >= 14:
                        continue
                    at = position_row(row, col)
                    line = 64 * a + at if b == 0 else 128 + 32 * a + at
                    to_window[line, 16 * frame_row + frame_col] = 1
    for row in range(14):
        for col in range(3):
            to_window[192 + east_row(row, col), 16 * row + col] = 1
    to_quad = np.zeros((256, 224), np.float32)
    for block in range(4):
        for i in range(7):
            for j in range(7):
                token = 16 * (2 * i + block % 2) + 2 * j + block // 2
                to_quad[64 * block + 8 * i + j, token] = 1
    window_to_quad = to_quad @ to_window.T
    rows = np.zeros((C, C), np.float32)
    for c in range(2):
        for xi in range(4):
            for k in range(3):
                for z in range(16):
                    rows[192 * c + 48 * xi + 16 * k + z, 24 * z + 6 * xi + 3 * c + k] = 1
    index = np.full((64, 64), 255.0, np.float32)
    mask = np.zeros((2, 64, 64), np.float32)
    valid = np.zeros(64, bool)
    for row in range(7):
        for col in range(7):
            p = position_row(row, col)
            valid[p] = True
            for row_q in range(7):
                for col_q in range(7):
                    q = position_row(row_q, col_q)
                    index[p, q] = 13 * (row - row_q + 6) + col - col_q + 6
                    if (row < 4) != (row_q < 4):
                        mask[1, p, q] = -100.0
    mask[:, :, ~valid] = -1e30
    mask = np.concatenate([mask, mask], -1)
    bf = ml_dtypes.bfloat16
    return (
        to_window.astype(bf),
        np.ascontiguousarray(to_window.T).astype(bf),
        to_quad.astype(bf),
        np.ascontiguousarray(to_quad.T).astype(bf),
        window_to_quad.astype(bf),
        np.ascontiguousarray(window_to_quad.T).astype(bf),
        rows.astype(bf),
        index.reshape(32, 128),
        mask,
    )


def mm(left, right):
    return lax.dot_general(left, right, (((1,), (0,)), ((), ())), preferred_element_type=F32)


def mm_t(left, right):
    return lax.dot_general(left, right, (((1,), (1,)), ((), ())), preferred_element_type=F32)


def t_mm(left, right):
    return lax.dot_general(left, right, (((0,), (0,)), ((), ())), preferred_element_type=F32)


def normalize(values):
    centred = values - jnp.mean(values, -1, keepdims=True)
    inverse_std = lax.rsqrt(jnp.mean(centred * centred, -1, keepdims=True) + 1e-05)
    return centred * inverse_std, inverse_std


def normalize_back(normed, inverse_std, grads):
    first = jnp.mean(grads, -1, keepdims=True)
    second = jnp.mean(grads * normed, -1, keepdims=True)
    return inverse_std * (grads - first - normed * second)


def window_of(values, a, b):
    if b == 0:
        return values[64 * a : 64 * a + 64]
    near, far = 128 + 32 * a, 192 + 32 * a
    return jnp.concatenate([values[near : near + 32], values[far : far + 32]], 0)


def put_window(ref, a, b, lanes, values):
    if b == 0:
        ref[64 * a : 64 * a + 64, lanes] = values
    else:
        near, far = 128 + 32 * a, 192 + 32 * a
        ref[near : near + 32, lanes] = values[:32]
        ref[far : far + 32, lanes] = values[32:]


def get_window(ref, a, b, lanes):
    if b == 0:
        return ref[64 * a : 64 * a + 64, lanes]
    near, far = 128 + 32 * a, 192 + 32 * a
    return jnp.concatenate([ref[near : near + 32, lanes], ref[far : far + 32, lanes]], 0)


def halves(op, empty, low, values):
    first = op(jnp.where(low, values, empty), -1, keepdims=True)
    second = op(jnp.where(low, empty, values), -1, keepdims=True)
    return jnp.where(low, first, second)


NAMES = (
    "feat", "cot", "pos", "w_attend", "w_out", "w_merge", "to_window", "to_window_t", "to_quad",
    "to_quad_t", "win_quad", "win_quad_t", "row_pick", "index", "mask",
)
ORDER = (
    "feat", "to_window", "w_attend", "pos", "index", "mask", "cot", "w_merge", "row_pick",
    "to_quad", "win_quad", "w_out", "win_quad_t", "to_quad_t", "to_window_t",
)
N_IN = len(NAMES)


def kernel(scatter, *refs):
    given, refs = refs[:N_IN], refs[N_IN:]
    merged_ref, grad_ref, share_ref = refs[:3]
    if scatter:
        refs = refs[3:]
    else:
        local_ref, refs = refs[3], refs[4:]
    held, refs = refs[:N_IN], refs[N_IN:]
    (
        x_scr, cot_scr, table_scr, bias_a, bias_b, normed_scr, std_scr,
        normed_east, std_east, qkv, probs, attended, branch_grad, outer, proj_grad,
        hidden_grad, left_o, left_r, feature_scr, first_scr,
        ex_send, ex_recv,
        g_own, g_send, g_recv, x_own, x_send, x_recv, y_send, y_recv,
        x_own2, x_send2, x_recv2, y_send2, y_recv2, z_line, z_send, z_recv,
        in_sem, ex_ssem, ex_rsem, c_ssem, c_rsem, x_ssem, x_rsem, y_ssem, y_rsem,
        z_ssem, z_rsem, near_sem,
    ) = refs
    (
        feat, cot, pos, w_attend, w_out, w_merge, to_window, to_window_t, to_quad, to_quad_t,
        win_quad, win_quad_t, row_pick, index, mask,
    ) = held
    copies = {
        name: pltpu.make_async_copy(given[i], held[i], in_sem.at[i])
        for i, name in enumerate(NAMES)
    }
    for name in ORDER[:2]:
        copies[name].start()

    z, x_lo = lax.axis_index("azim_0"), lax.axis_index("azim_1")
    x_hi, y, core = (lax.axis_index(name) for name in FRAME)
    n_z = lax.axis_size("azim_0")
    n_azim = n_z * 2
    azim = 2 * z + x_lo
    east, west = (azim + 1) % n_azim, (azim + n_azim - 1) % n_azim
    east_id = {"azim_0": east // 2, "azim_1": east % 2}
    west_id = {"azim_0": west // 2, "azim_1": west % 2}
    xi = 2 * x_lo + x_hi

    def x_id(step):
        other = (xi + step) % 4
        return {"azim_1": other // 2, "frame_0": other % 2}

    def z_id(step):
        return {"azim_0": (z + n_z + step) % n_z}

    barrier = pltpu.get_barrier_semaphore()
    near = [east_id, west_id]
    if scatter:
        near += [{"frame_2": 1 - core}]
        near += [x_id(step) for step in (1, 2, 3)]
        near += [{"frame_1": (y + step) % 4} for step in (1, 2, 3)]
        near += [{"frame_1": (y + step) % 4, "frame_2": 1 - core} for step in (1, 2, 3)]
        near += [z_id(1), z_id(-1)]
    for device in near:
        pl.semaphore_signal(barrier, inc=1, device_id=device)

    def exchange(i, device):
        return pltpu.make_async_remote_copy(
            src_ref=ex_send.at[i], dst_ref=ex_recv.at[i], send_sem=ex_ssem.at[i],
            recv_sem=ex_rsem.at[i], device_id=device,
        )

    for name in ORDER[2:7]:
        copies[name].start()
    copies["feat"].wait()
    for name in ORDER[7:]:
        copies[name].start()
    x_scr[...] = jnp.zeros_like(x_scr)
    for row in range(14):
        x_scr[row, 0:14, :] = feat[row].astype(F32)
    tokens = x_scr[...].reshape(224, C)
    tokens16 = tokens.astype(BF)
    copies["to_window"].wait()
    shared = mm(to_window[128:256], tokens16).astype(BF)
    ex_send[0] = shared[64:128]
    ex_send[1] = shared[0:64]
    pl.semaphore_wait(barrier, len(near))
    exchange(0, west_id).start()
    exchange(1, east_id).start()
    if scatter:
        for step in (1, -1):
            pl.semaphore_signal(near_sem.at[0], inc=1, device_id=z_id(step))

    def widen_reach(i):
        if not scatter:
            return
        pl.semaphore_wait(near_sem.at[i], 2)
        if i < 2:
            for step in (2 ** (i + 1), -(2 ** (i + 1))):
                pl.semaphore_signal(near_sem.at[i + 1], inc=1, device_id=z_id(step))

    normed, inverse_std = normalize(tokens)
    normed_scr[...] = normed
    std_scr[...] = inverse_std
    rolled = mm(to_window[...], normed.astype(BF)).astype(BF)
    rolled_own = rolled[0:192]
    copies["w_attend"].wait()
    projected = mm(rolled, w_attend[...]).astype(BF)
    qkv[0:192] = projected[0:192]
    qkv[320:384] = projected[192:256]

    copies["pos"].wait()
    copies["index"].wait()
    copies["mask"].wait()
    table_scr[...] = jnp.zeros_like(table_scr)
    table_scr[0:12, 0:169] = pos[...]
    table = table_scr[...]
    high = table.astype(BF).astype(F32)
    both = jnp.concatenate([high, table - high], 0).astype(BF)
    lane = lax.broadcasted_iota(jnp.int32, (1, 128), 1)
    entry = lax.broadcasted_iota(jnp.int32, (256, 128), 0).astype(F32)
    for t in range(0, 32, 4):
        picks = [
            jnp.where(entry == index[u : u + 1, :], 1.0, 0.0).astype(BF) for u in range(t, t + 4)
        ]
        wide = mm(both, jnp.concatenate(picks, 1))
        for u in range(4):
            part = wide[:, 128 * u : 128 * u + 128]
            part = part[0:16] + part[16:32]
            turned = pltpu.roll(part, 64, 1)
            p = 2 * (t + u)
            bias_a[pl.ds(p, 16, stride=64), :] = part
            bias_a[pl.ds(p + 1, 16, stride=64), :] = turned
            bias_b[pl.ds(p, 16, stride=64), :] = turned
            bias_b[pl.ds(p + 1, 16, stride=64), :] = part
    low = lane < 64

    def pair_bias(pair):
        first = bias_a[128 * pair : 128 * pair + 64, :]
        second = bias_b[128 * pair + 64 : 128 * pair + 128, :]
        return jnp.where(low, first, second)

    copies["cot"].wait()
    cot_scr[...] = jnp.zeros_like(cot_scr)
    for row in range(7):
        cot_scr[row, 0:7, :] = cot[row].astype(F32)
    copies["w_merge"].wait()
    quad_grad_in = mm_t(cot_scr[...].reshape(64, OUT).astype(BF), w_merge[...])

    head_lanes = [(lane // 32 == h).astype(F32).astype(BF) for h in range(4)]

    def spread(block):
        return jnp.concatenate([block * head_lanes[h] for h in range(4)], 0)

    def heads_of(wide):
        total = wide[0:64] * head_lanes[0].astype(F32)
        for h in range(1, 4):
            total = total + wide[64 * h : 64 * h + 64] * head_lanes[h].astype(F32)
        return total

    def group_lanes(kind, group):
        start = C * kind + 128 * group
        return slice(start, start + 128)

    def units_of(windows):
        return [(w, group) for w in windows for group in range(GROUPS)]

    def of_window(ref, w, kind, group):
        return get_window(ref, *WINDOWS[w], group_lanes(kind, group))

    ones = (lax.broadcasted_iota(jnp.int32, (128, 128), 0) < 64) == low
    ones = ones.astype(F32).astype(BF)

    def half_sums(values):
        joined = jnp.concatenate(values, 0)
        high = joined.astype(BF)
        rest = (joined - high.astype(F32)).astype(BF)
        total = mm(high, ones) + mm(rest, ones)
        ends = [sum(value.shape[0] for value in values[: i + 1]) for i in range(len(values))]
        return [total[end - value.shape[0] : end] for value, end in zip(values, ends)]

    def split_halves(wide):
        return [part[:, 128 * i : 128 * i + 128] for part in wide for i in range(2)]

    def join_halves(parts):
        return [
            jnp.concatenate([parts[i].astype(BF), parts[i + 1].astype(BF)], 1)
            for i in range(0, len(parts), 2)
        ]

    def softmax(units, scores):
        parts = split_halves(scores)
        for i, (a, g, rows) in enumerate(units):
            for j in range(2):
                bias = pair_bias(2 * g + j)[rows] + mask[a, rows]
                parts[2 * i + j] = parts[2 * i + j] * SCALE + bias
        tops = [halves(jnp.max, -3e38, low, part) for part in parts]
        parts = [jnp.exp(part - top) for part, top in zip(parts, tops)]
        sums = half_sums(parts)
        return [part * (1.0 / total) for part, total in zip(parts, sums)]

    def of_first(a, kind, g):
        lanes = group_lanes(kind, g)
        near, far = 256 + 32 * a, 320 + 32 * a
        return jnp.concatenate([qkv[near : near + 32, lanes], qkv[far : far + 32, lanes]], 0)

    def attend(*windows, first=()):
        units = units_of(windows)
        extra = [(a, g) for a in first for g in range(GROUPS)]
        scores = [
            mm_t(of_window(qkv, w, 0, g), spread(of_window(qkv, w, 1, g))) for w, g in units
        ] + [
            mm_t(qkv[320 + 32 * a : 352 + 32 * a, group_lanes(0, g)], spread(of_first(a, 1, g)))
            for a, g in extra
        ]
        parts = softmax(
            [(WINDOWS[w][0], g, slice(0, 64)) for w, g in units]
            + [(a, g, slice(32, 64)) for a, g in extra],
            scores,
        )
        for i, (w, g) in enumerate(units):
            for j in range(2):
                probs[GROUPS * w + g, :, 128 * j : 128 * j + 128] = parts[2 * i + j]
        joined = join_halves(parts)
        for (w, g), prob in zip(units, joined):
            result = mm(prob, spread(of_window(qkv, w, 2, g))).astype(BF)
            put_window(attended, *WINDOWS[w], group_lanes(0, g), result)
        for (a, g), prob in zip(extra, joined[len(units) :]):
            result = mm(prob, spread(of_first(a, 2, g))).astype(BF)
            first_scr[32 * a : 32 * a + 32, group_lanes(0, g)] = result

    attend(2, 3)
    copies["to_quad"].wait()
    features_quad = mm(to_quad[...], tokens16)

    exchange(0, west_id).wait()
    exchange(1, east_id).wait()
    widen_reach(0)
    normed, inverse_std = normalize(ex_recv[0:2].astype(F32).reshape(128, C))
    normed_east[...] = normed[0:64]
    std_east[...] = inverse_std[0:64]
    rolled = normed.astype(BF)
    rolled_east = rolled[0:64]
    qkv[192:320] = mm(rolled, w_attend[...]).astype(BF)
    attend(0, 1, first=(0, 1))
    copies["win_quad"].wait()
    copies["w_out"].wait()
    widen_reach(1)

    extended = jnp.concatenate([attended[0:192], first_scr[...]], 0)
    attended_quad = mm(win_quad[...], extended).astype(BF)
    hidden = (features_quad + mm(attended_quad, w_out[...])).astype(BF).astype(F32)
    quads = [hidden[64 * e : 64 * e + 64] for e in range(4)]

    def mean(blocks):
        total = (blocks[0] + blocks[1]) + (blocks[2] + blocks[3])
        return jnp.sum(total, -1, keepdims=True) * (1.0 / (4 * C))

    centre = mean(quads)
    quads = [quad - centre for quad in quads]
    quad_std = lax.rsqrt(mean([quad * quad for quad in quads]) + 1e-05)
    quads = [quad * quad_std for quad in quads]
    grads = [quad_grad_in[:, C * e : C * e + C] for e in range(4)]
    first = mean(grads)
    second = mean([grad * quad for grad, quad in zip(grads, quads)])
    for e in range(4):
        value = quad_std * (grads[e] - first - quads[e] * second)
        hidden_grad[64 * e : 64 * e + 64] = value.astype(BF)
    copies["win_quad_t"].wait()
    ex_send[2] = mm(win_quad_t[192:256], hidden_grad[...]).astype(BF)
    exchange(2, west_id).start()
    copies["row_pick"].wait()
    left_r[:, 0:192] = mm_t(row_pick[...], rolled_own).astype(BF)
    left_r[:, 192:256] = mm_t(row_pick[...], rolled_east).astype(BF)
    left_o[...] = mm_t(row_pick[...], attended[...]).astype(BF)
    own_grad = mm(win_quad_t[0:192], hidden_grad[...]).astype(BF)
    branch_grad[0:192] = own_grad
    outer[0:192] = mm_t(own_grad, w_out[...]).astype(BF)
    merged = mm(jnp.concatenate([quad.astype(BF) for quad in quads], 1), w_merge[...])
    for i in range(7):
        merged_ref[i] = merged[8 * i : 8 * i + 7].astype(BF)
    copies["to_quad_t"].wait()
    hidden_own = mm(to_quad_t[...], hidden_grad[...])

    def values_back(*windows):
        units = units_of(windows)
        wide = [
            t_mm(probs[GROUPS * w + g].astype(BF), of_window(outer, w, 0, g)) for w, g in units
        ]
        for (w, g), value in zip(units, wide):
            back = heads_of(value).astype(BF)
            put_window(proj_grad, *WINDOWS[w], group_lanes(2, g), back)

    def scores_back(*windows):
        units = units_of(windows)
        wide = [
            mm_t(of_window(outer, w, 0, g), spread(of_window(qkv, w, 2, g))) for w, g in units
        ]
        grads = split_halves(wide)
        prob = split_halves([probs[GROUPS * w + g] for w, g in units])
        sums = half_sums([p * grad for p, grad in zip(prob, grads)])
        parts = [p * (grad - total) * SCALE for p, grad, total in zip(prob, grads, sums)]
        soft = join_halves(parts)
        wide = [t_mm(part, of_window(qkv, w, 0, g)) for (w, g), part in zip(units, soft)]
        for (w, g), part in zip(units, soft):
            back = mm(part, spread(of_window(qkv, w, 1, g))).astype(BF)
            put_window(proj_grad, *WINDOWS[w], group_lanes(0, g), back)
        for (w, g), value in zip(units, wide):
            back = heads_of(value).astype(BF)
            put_window(proj_grad, *WINDOWS[w], group_lanes(1, g), back)

    def core_copy(i):
        return pltpu.make_async_remote_copy(
            src_ref=g_send.at[i, 1 - core], dst_ref=g_recv.at[i], send_sem=c_ssem.at[i],
            recv_sem=c_rsem.at[i], device_id={"frame_2": 1 - core},
        )

    def start_core(i, product):
        product = product.reshape(2, 192, C)
        g_own[i] = product
        if scatter:
            g_send[i] = product.astype(BF)
            core_copy(i).start()

    def x_copies(i, sent, landing):
        return [
            pltpu.make_async_remote_copy(
                src_ref=sent.at[(xi + step) % 4], dst_ref=landing.at[step - 1],
                send_sem=x_ssem.at[i, step - 1], recv_sem=x_rsem.at[i, step - 1],
                device_id=x_id(step),
            )
            for step in (2, 1, 3)
        ]

    def y_copy(i, m, sent, landing):
        return pltpu.make_async_remote_copy(
            src_ref=sent.at[m], dst_ref=landing.at[y], send_sem=y_ssem.at[i, m],
            recv_sem=y_rsem.at[i, y],
            device_id={"frame_1": 2 * core + m // 2, "frame_2": m % 2},
        )

    def y_landed(i, source, sent, landing):
        return pltpu.make_async_remote_copy(
            src_ref=sent.at[0], dst_ref=landing.at[source], send_sem=y_ssem.at[i, 0],
            recv_sem=y_rsem.at[i, source], device_id={"frame_2": 1 - core},
        )

    def stays(m):
        return jnp.logical_and(2 * core + m // 2 == y, core == m % 2)

    def start_y(i, sent, landing):
        for m in range(4):

            @pl.when(stays(m))
            def _():
                landing[y] = sent[m]

            @pl.when(jnp.logical_not(stays(m)))
            def _():
                y_copy(i, m, sent, landing).start()

    def end_y(i, sent, landing):
        for source in range(4):
            mine = jnp.logical_and(y == source, y // 2 == core)

            @pl.when(jnp.logical_not(mine))
            def _():
                y_landed(i, source, sent, landing).wait_recv()

        for m in range(4):

            @pl.when(jnp.logical_not(stays(m)))
            def _():
                y_copy(i, m, sent, landing).wait_send()

        total = landing[0].astype(F32)
        for source in range(1, 4):
            total = total + landing[source].astype(F32)
        return total

    wide_lane = lax.broadcasted_iota(jnp.int32, (1, C), 1)

    def segments(i, block):
        one, two, three = (block[16 * k : 16 * k + 16] for k in range(3))

        def left(value, count):
            return pltpu.roll(value, C - count, 1)

        if i == 0:
            second = jnp.where(wide_lane < 96, left(one, 288), pltpu.roll(two, 96, 1))
            third = jnp.where(wide_lane < 192, left(two, 192), pltpu.roll(three, 192, 1))
            return one, second, third, left(three, 96)
        if i == 1:
            return one, left(one, 96), two, three
        if i == 2:
            return one, two, three, left(three, 288)
        return one, two, left(two, 192), three

    def start_first(i):
        if not scatter:
            return
        core_copy(i).wait()
        total = (g_own[i, core] + g_recv[i].astype(F32)).reshape(4, 48, C)
        j = i // 2
        if i % 2 == 0:
            x_own[j] = total
            x_send[j] = total.astype(BF)
            for copy in x_copies(i, x_send.at[j], x_recv.at[j]):
                copy.start()
        else:
            for block in range(4):
                for m, value in enumerate(segments(i, total[block])):
                    y_send[j, m, block] = value.astype(BF)
            start_y(i, y_send.at[j], y_recv.at[j])

    def start_second(i):
        j = i // 2
        if i % 2 == 0:
            for copy in x_copies(i, x_send.at[j], x_recv.at[j]):
                copy.wait()
            total = x_own[j, xi]
            for step in (1, 2, 3):
                total = total + x_recv[j, step - 1].astype(F32)
            for m, value in enumerate(segments(i, total)):
                y_send2[j, m] = value.astype(BF)
            start_y(4 + j, y_send2.at[j], y_recv2.at[j])
        else:
            total = end_y(i, y_send.at[j], y_recv.at[j])
            x_own2[j] = total
            x_send2[j] = total.astype(BF)
            for copy in x_copies(4 + j, x_send2.at[j], x_recv2.at[j]):
                copy.start()

    def z_copy(j, step):
        return pltpu.make_async_remote_copy(
            src_ref=z_send.at[j, (z + step) % 16], dst_ref=z_recv.at[j, step - 1],
            send_sem=z_ssem.at[j, step - 1], recv_sem=z_rsem.at[j, step - 1],
            device_id=z_id(step),
        )

    z_steps = sorted(range(1, 16), key=lambda step: -min(step, 16 - step))

    def start_z(j):
        first = end_y(4 + j, y_send2.at[j], y_recv2.at[j])
        for copy in x_copies(4 + j, x_send2.at[j], x_recv2.at[j]):
            copy.wait()
        second = x_own2[j, xi]
        for step in (1, 2, 3):
            second = second + x_recv2[j, step - 1].astype(F32)
        for t in range(3):
            lanes = slice(128 * t, 128 * t + 128)
            z_line[j, pl.ds(t, 16, stride=8), :] = first[:, lanes]
            z_line[j, pl.ds(t + 3, 16, stride=8), :] = second[:, lanes]
        for t in (6, 7):
            z_line[j, pl.ds(t, 16, stride=8), :] = jnp.zeros((16, 128), F32)
        z_send[j] = z_line[j].reshape(16, 8, 128).astype(BF)
        for step in z_steps:
            z_copy(j, step).start()

    def end_z(j):
        total = z_send[j, z].astype(F32)
        for step in z_steps[::-1]:
            z_copy(j, step).wait()
            total = total + z_recv[j, step - 1].astype(F32)
        share_ref[8 * j : 8 * j + 8] = total

    scores_back(2, 3)
    exchange(2, west_id).wait()
    widen_reach(2)
    branch_grad[192:256] = ex_recv[2]
    outer[192:256] = mm_t(ex_recv[2], w_out[...]).astype(BF)
    start_core(0, mm(left_o[...], branch_grad[...]))
    values_back(0, 1, 2, 3)
    start_core(1, mm(left_r[...], proj_grad[:, 2 * C : 3 * C]))
    start_first(0)
    scores_back(0, 1)
    start_first(1)
    start_core(2, mm(left_r[...], proj_grad[:, 0:C]))
    start_core(3, mm(left_r[...], proj_grad[:, C : 2 * C]))
    east_grad = mm_t(proj_grad[192:256], w_attend[...])
    east_grad = normalize_back(normed_east[...], std_east[...], east_grad)
    ex_send[3] = east_grad.astype(BF)
    exchange(3, east_id).start()
    start_first(2)
    start_first(3)
    copies["to_window_t"].wait()
    own_proj = mm(to_window_t[:, 0:192], proj_grad[0:192]).astype(BF)
    own_grad = mm_t(own_proj, w_attend[...])
    own_grad = normalize_back(normed_scr[...], std_scr[...], own_grad)
    feature_scr[...] = hidden_own + own_grad

    def end_features():
        exchange(3, east_id).wait()
        grad = feature_scr[...] + mm(to_window_t[:, 192:256], ex_recv[3])
        grad = grad.reshape(14, 16, C)
        for row in range(14):
            grad_ref[row] = grad[row, 0:14].astype(BF)

    if scatter:
        for group in range(4):
            start_second(group)
        start_z(0)
        start_z(1)
        end_features()
        end_z(0)
        end_z(1)
    else:
        end_features()
        share_ref[...] = jnp.zeros_like(share_ref)
        local_ref[...] = g_own[...]


def finish(merged_in, grad_in, share, merged_ref, grad_ref, attend_ref, output_ref):
    merged_ref[0] = merged_in[...]
    grad_ref[0] = grad_in[...]
    lane = lax.broadcasted_iota(jnp.int32, (1, 128), 1)

    def put(ref, pieces):
        lines = [jnp.zeros((1, 128), F32) for _ in range(-(-ref.shape[0] // 128))]
        start = 0
        for first, width in pieces:
            skip, turn = divmod(start, 128)
            values = [share[first + i : first + i + 1, :] for i in range(3)]
            if turn:
                values = [pltpu.roll(value, turn, 1) for value in values]
            for j in range(skip, (start + width - 1) // 128 + 1):
                value = values[min(j - skip, 2)]
                if turn and j > skip:
                    value = jnp.where(lane < turn, values[j - skip - 1], value)
                at = lane + 128 * j
                inside = jnp.logical_and(at >= start, at < start + width)
                lines[j] = jnp.where(inside, value, lines[j])
            start += width
        for j, value in enumerate(lines):
            count = min(128, ref.shape[0] - 128 * j)
            ref[128 * j : 128 * j + count] = value.reshape(128)[:count]

    put(output_ref, ((0, 288),))
    v, q, k = 3, 8, 11
    segment = 2 * (lax.axis_index("frame_1") % 2) + lax.axis_index("frame_2")
    for m, pieces in enumerate((
        ((q, 384), (k, 384), (v, 96)),
        ((v, 288), (q, 384), (k, 192)),
        ((k, 192), (v, 384), (q, 288)),
        ((q, 96), (k, 384), (v, 384)),
    )):
        pl.when(segment == m)(functools.partial(put, attend_ref, pieces))


def local_call(scatter, features, position_bias, attend_weight, output_weight, merge_weight, cotangent):
    given = (features[0], cotangent[0], position_bias.T, attend_weight, output_weight, merge_weight)
    given = given + tuple(jnp.asarray(table) for table in tables())
    dma = pltpu.SemaphoreType.DMA
    scratch = [pltpu.VMEM(a.shape, a.dtype) for a in given]
    scratch += [
        pltpu.VMEM((14, 16, C), F32),
        pltpu.VMEM((8, 8, OUT), F32),
        pltpu.VMEM((16, 256), F32),
        pltpu.VMEM((1024, 128), F32),
        pltpu.VMEM((1024, 128), F32),
        pltpu.VMEM((224, C), F32),
        pltpu.VMEM((224, 1), F32),
        pltpu.VMEM((64, C), F32),
        pltpu.VMEM((64, 1), F32),
        pltpu.VMEM((384, 3 * C), BF),
        pltpu.VMEM((12, 64, 256), F32),
        pltpu.VMEM((256, C), BF),
        pltpu.VMEM((256, C), BF),
        pltpu.VMEM((256, C), BF),
        pltpu.VMEM((256, 3 * C), BF),
        pltpu.VMEM((256, C), BF),
        pltpu.VMEM((C, 256), BF),
        pltpu.VMEM((C, 256), BF),
        pltpu.VMEM((224, C), F32),
        pltpu.VMEM((64, C), BF),
        pltpu.VMEM((4, 64, C), BF),
        pltpu.VMEM((4, 64, C), BF),
        pltpu.VMEM((4, 2, 192, C), F32),
        pltpu.VMEM((4, 2, 192, C), BF),
        pltpu.VMEM((4, 192, C), BF),
        pltpu.VMEM((2, 4, 48, C), F32),
        pltpu.VMEM((2, 4, 48, C), BF),
        pltpu.VMEM((2, 3, 48, C), BF),
        pltpu.VMEM((2, 4, 4, 16, C), BF),
        pltpu.VMEM((2, 4, 4, 16, C), BF),
        pltpu.VMEM((2, 4, 16, C), F32),
        pltpu.VMEM((2, 4, 16, C), BF),
        pltpu.VMEM((2, 3, 16, C), BF),
        pltpu.VMEM((2, 4, 16, C), BF),
        pltpu.VMEM((2, 4, 16, C), BF),
        pltpu.VMEM((2, 128, 128), F32),
        pltpu.VMEM((2, 16, 8, 128), BF),
        pltpu.VMEM((2, 15, 8, 128), BF),
        dma((N_IN,)), dma((4,)), dma((4,)), dma((4,)), dma((4,)), dma((6, 3)), dma((6, 3)),
        dma((6, 4)), dma((6, 4)), dma((2, 15)), dma((2, 15)), pltpu.SemaphoreType.REGULAR((3,)),
    ]
    vmem = pl.BlockSpec(memory_space=pltpu.VMEM)
    return pl.pallas_call(
        functools.partial(kernel, scatter),
        out_shape=(
            pltpu.VMEM((7, 7, OUT), BF),
            pltpu.VMEM((14, 14, C), BF),
            pltpu.VMEM((16, 128), F32),
        )
        + (() if scatter else (jax.ShapeDtypeStruct((4, 2, 192, C), F32),)),
        in_specs=[pl.BlockSpec(memory_space=pl.ANY)] * N_IN,
        out_specs=(vmem,) * (3 if scatter else 4),
        scratch_shapes=scratch,
        compiler_params=pltpu.CompilerParams(collective_id=0, has_side_effects=True),
    )(*given)


def per_device(*arrays):
    merged, feature_grad, share = local_call(True, *arrays)
    vmem = pl.BlockSpec(memory_space=pltpu.VMEM)
    return pl.pallas_call(
        finish,
        out_shape=(
            jax.ShapeDtypeStruct((1, *merged.shape), BF),
            jax.ShapeDtypeStruct((1, *feature_grad.shape), BF),
            jax.ShapeDtypeStruct((864,), F32),
            jax.ShapeDtypeStruct((288,), F32),
        ),
        in_specs=(vmem,) * 3,
        out_specs=(vmem,) * 4,
        compiler_params=pltpu.CompilerParams(vmem_limit_bytes=8 << 20),
    )(merged, feature_grad, share)


def solution(mesh):
    split = Mesh(mesh.devices.reshape(16, 2, 2, 4, 2), AZIM_FRAME)
    placed = (P(FRAME, None, AZIM, None), P(), P(), P(), P(), P(FRAME, None, AZIM, None))
    return jax.shard_map(
        per_device,
        mesh=split,
        in_specs=placed,
        out_specs=(
            P(FRAME, None, AZIM, None),
            P(FRAME, None, AZIM, None),
            P(AZIM_FRAME),
            P(AZIM_FRAME),
        ),
        check_vma=False,
    )
```

```python
import functools

import jax
import jax.numpy as jnp
import ml_dtypes
import numpy as np
from jax import lax
from jax.experimental import pallas as pl
from jax.experimental.pallas import tpu as pltpu
from jax.sharding import Mesh
from jax.sharding import PartitionSpec as P

AZIM = ("azim_0", "azim_1")
AZIM_FRAME = ("azim_0", "azim_1", "frame_0", "frame_1", "frame_2")
FRAME = ("frame_0", "frame_1", "frame_2")

BF = jnp.bfloat16
F32 = jnp.float32
C = 384
OUT = 768
GROUPS = 3
SCALE = 32 ** (-0.5)
WINDOWS = ((0, 1), (1, 1), (0, 0), (1, 0))


def position_row(row, col):
    return 4 * row + col if col < 4 else 32 + 3 * row + col - 4


def east_row(row, col):
    rolled = (row - 3) % 14
    return 32 * (rolled // 7) + 3 * (rolled % 7) + col


@functools.cache
def tables():
    to_window = np.zeros((256, 224), np.float32)
    for a in range(2):
        for b in range(2):
            for row in range(7):
                for col in range(7):
                    frame_row, frame_col = (7 * a + row + 3) % 14, 7 * b + col + 3
                    if frame_col >= 14:
                        continue
                    at = position_row(row, col)
                    line = 64 * a + at if b == 0 else 128 + 32 * a + at
                    to_window[line, 16 * frame_row + frame_col] = 1
    for row in range(14):
        for col in range(3):
            to_window[192 + east_row(row, col), 16 * row + col] = 1
    to_quad = np.zeros((256, 224), np.float32)
    for block in range(4):
        for i in range(7):
            for j in range(7):
                token = 16 * (2 * i + block % 2) + 2 * j + block // 2
                to_quad[64 * block + 8 * i + j, token] = 1
    window_to_quad = to_quad @ to_window.T
    rows = np.zeros((C, C), np.float32)
    for c in range(2):
        for xi in range(4):
            for k in range(3):
                for z in range(16):
                    rows[192 * c + 48 * xi + 16 * k + z, 24 * z + 6 * xi + 3 * c + k] = 1
    index = np.full((64, 64), 255.0, np.float32)
    mask = np.zeros((2, 64, 64), np.float32)
    valid = np.zeros(64, bool)
    for row in range(7):
        for col in range(7):
            p = position_row(row, col)
            valid[p] = True
            for row_q in range(7):
                for col_q in range(7):
                    q = position_row(row_q, col_q)
                    index[p, q] = 13 * (row - row_q + 6) + col - col_q + 6
                    if (row < 4) != (row_q < 4):
                        mask[1, p, q] = -100.0
    mask[:, :, ~valid] = -1e30
    mask = np.concatenate([mask, mask], -1)
    bf = ml_dtypes.bfloat16
    return (
        to_window.astype(bf),
        np.ascontiguousarray(to_window.T).astype(bf),
        to_quad.astype(bf),
        np.ascontiguousarray(to_quad.T).astype(bf),
        window_to_quad.astype(bf),
        np.ascontiguousarray(window_to_quad.T).astype(bf),
        rows.astype(bf),
        index.reshape(32, 128),
        mask,
    )


def mm(left, right):
    return lax.dot_general(left, right, (((1,), (0,)), ((), ())), preferred_element_type=F32)


def mm_t(left, right):
    return lax.dot_general(left, right, (((1,), (1,)), ((), ())), preferred_element_type=F32)


def t_mm(left, right):
    return lax.dot_general(left, right, (((0,), (0,)), ((), ())), preferred_element_type=F32)


def normalize(values):
    centred = values - jnp.mean(values, -1, keepdims=True)
    inverse_std = lax.rsqrt(jnp.mean(centred * centred, -1, keepdims=True) + 1e-05)
    return centred * inverse_std, inverse_std


def normalize_back(normed, inverse_std, grads):
    first = jnp.mean(grads, -1, keepdims=True)
    second = jnp.mean(grads * normed, -1, keepdims=True)
    return inverse_std * (grads - first - normed * second)


def window_of(values, a, b):
    if b == 0:
        return values[64 * a : 64 * a + 64]
    near, far = 128 + 32 * a, 192 + 32 * a
    return jnp.concatenate([values[near : near + 32], values[far : far + 32]], 0)


def put_window(ref, a, b, lanes, values):
    if b == 0:
        ref[64 * a : 64 * a + 64, lanes] = values
    else:
        near, far = 128 + 32 * a, 192 + 32 * a
        ref[near : near + 32, lanes] = values[:32]
        ref[far : far + 32, lanes] = values[32:]


def get_window(ref, a, b, lanes):
    if b == 0:
        return ref[64 * a : 64 * a + 64, lanes]
    near, far = 128 + 32 * a, 192 + 32 * a
    return jnp.concatenate([ref[near : near + 32, lanes], ref[far : far + 32, lanes]], 0)


def halves(op, empty, low, values):
    first = op(jnp.where(low, values, empty), -1, keepdims=True)
    second = op(jnp.where(low, empty, values), -1, keepdims=True)
    return jnp.where(low, first, second)


NAMES = (
    "feat", "cot", "pos", "w_attend", "w_out", "w_merge", "to_window", "to_window_t", "to_quad",
    "to_quad_t", "win_quad", "win_quad_t", "row_pick", "index", "mask",
)
ORDER = (
    "feat", "to_window", "w_attend", "pos", "index", "mask", "cot", "w_merge", "row_pick",
    "to_quad", "win_quad", "w_out", "win_quad_t", "to_quad_t", "to_window_t",
)
N_IN = len(NAMES)
X_SLOTS = {0: 0, 2: 1, 4: 2, 5: 3}
Y_SLOTS = {1: 0, 3: 1, 4: 2, 5: 3}


def kernel(scatter, *refs):
    given, refs = refs[:N_IN], refs[N_IN:]
    merged_ref, grad_ref, share_ref = refs[:3]
    if scatter:
        refs = refs[3:]
    else:
        local_ref, refs = refs[3], refs[4:]
    held, refs = refs[:N_IN], refs[N_IN:]
    (
        x_scr, cot_scr, table_scr, bias_a, bias_b, normed_scr, std_scr,
        normed_east, std_east, qkv, probs, attended, branch_grad, outer, proj_grad,
        hidden_grad, left_o, left_r, feature_scr, first_scr,
        ex_send, ex_recv,
        g_own, g_send, g_recv, x_own, x_send, x_recv, y_send, y_recv,
        x_own2, x_send2, x_recv2, y_send2, y_recv2, z_line, z_send, z_recv,
        in_sem, ex_ssem, ex_rsem, c_ssem, c_rsem, x_ssem, x_rsem, y_ssem, y_rsem,
        z_ssem, z_rsem, near_sem,
    ) = refs
    (
        feat, cot, pos, w_attend, w_out, w_merge, to_window, to_window_t, to_quad, to_quad_t,
        win_quad, win_quad_t, row_pick, index, mask,
    ) = held
    copies = {
        name: pltpu.make_async_copy(given[i], held[i], in_sem.at[i])
        for i, name in enumerate(NAMES)
    }
    for name in ORDER[:2]:
        copies[name].start()

    z, x_lo = lax.axis_index("azim_0"), lax.axis_index("azim_1")
    x_hi, y, core = (lax.axis_index(name) for name in FRAME)
    n_z = lax.axis_size("azim_0")
    n_azim = n_z * 2
    azim = 2 * z + x_lo
    east, west = (azim + 1) % n_azim, (azim + n_azim - 1) % n_azim
    east_id = {"azim_0": east // 2, "azim_1": east % 2}
    west_id = {"azim_0": west // 2, "azim_1": west % 2}
    xi = 2 * x_lo + x_hi

    def x_id(step):
        other = (xi + step) % 4
        return {"azim_1": other // 2, "frame_0": other % 2}

    def z_id(step):
        return {"azim_0": (z + n_z + step) % n_z}

    barrier = pltpu.get_barrier_semaphore()
    near = [east_id, west_id]
    if scatter:
        near += [{"frame_2": 1 - core}]
        near += [x_id(step) for step in (1, 2, 3)]
        near += [{"frame_1": (y + step) % 4} for step in (1, 2, 3)]
        near += [{"frame_1": (y + step) % 4, "frame_2": 1 - core} for step in (1, 2, 3)]
        near += [z_id(1), z_id(-1)]
    for device in near:
        pl.semaphore_signal(barrier, inc=1, device_id=device)

    def exchange(i, device):
        return pltpu.make_async_remote_copy(
            src_ref=ex_send.at[i], dst_ref=ex_recv.at[i], send_sem=ex_ssem.at[i],
            recv_sem=ex_rsem.at[i], device_id=device,
        )

    for name in ORDER[2:7]:
        copies[name].start()
    copies["feat"].wait()
    for name in ORDER[7:]:
        copies[name].start()
    x_scr[...] = jnp.zeros_like(x_scr)
    for row in range(14):
        x_scr[row, 0:14, :] = feat[row].astype(F32)
    tokens = x_scr[...].reshape(224, C)
    tokens16 = tokens.astype(BF)
    copies["to_window"].wait()
    shared = mm(to_window[128:256], tokens16).astype(BF)
    ex_send[0] = shared[64:128]
    ex_send[1] = shared[0:64]
    pl.semaphore_wait(barrier, len(near))
    exchange(0, west_id).start()
    exchange(1, east_id).start()
    if scatter:
        for step in (1, -1):
            pl.semaphore_signal(near_sem.at[0], inc=1, device_id=z_id(step))

    def widen_reach(i):
        if not scatter:
            return
        pl.semaphore_wait(near_sem.at[i], 2)
        if i < 2:
            for step in (2 ** (i + 1), -(2 ** (i + 1))):
                pl.semaphore_signal(near_sem.at[i + 1], inc=1, device_id=z_id(step))

    normed, inverse_std = normalize(tokens)
    normed_scr[...] = normed
    std_scr[...] = inverse_std
    rolled = mm(to_window[...], normed.astype(BF)).astype(BF)
    rolled_own = rolled[0:192]
    copies["w_attend"].wait()
    projected = mm(rolled, w_attend[...]).astype(BF)
    qkv[0:192] = projected[0:192]
    qkv[320:384] = projected[192:256]

    copies["pos"].wait()
    copies["index"].wait()
    copies["mask"].wait()
    table_scr[...] = jnp.zeros_like(table_scr)
    table_scr[0:12, 0:169] = pos[...]
    table = table_scr[...]
    high = table.astype(BF).astype(F32)
    both = jnp.concatenate([high, table - high], 0).astype(BF)
    lane = lax.broadcasted_iota(jnp.int32, (1, 128), 1)
    entry = lax.broadcasted_iota(jnp.int32, (256, 128), 0).astype(F32)
    for t in range(0, 32, 4):
        picks = [
            jnp.where(entry == index[u : u + 1, :], 1.0, 0.0).astype(BF) for u in range(t, t + 4)
        ]
        wide = mm(both, jnp.concatenate(picks, 1))
        for u in range(4):
            part = wide[:, 128 * u : 128 * u + 128]
            part = part[0:16] + part[16:32]
            turned = pltpu.roll(part, 64, 1)
            p = 2 * (t + u)
            bias_a[pl.ds(p, 16, stride=64), :] = part
            bias_a[pl.ds(p + 1, 16, stride=64), :] = turned
            bias_b[pl.ds(p, 16, stride=64), :] = turned
            bias_b[pl.ds(p + 1, 16, stride=64), :] = part
    low = lane < 64

    def pair_bias(pair):
        first = bias_a[128 * pair : 128 * pair + 64, :]
        second = bias_b[128 * pair + 64 : 128 * pair + 128, :]
        return jnp.where(low, first, second)

    copies["cot"].wait()
    cot_scr[...] = jnp.zeros_like(cot_scr)
    for row in range(7):
        cot_scr[row, 0:7, :] = cot[row].astype(F32)
    copies["w_merge"].wait()
    quad_grad_in = mm_t(cot_scr[...].reshape(64, OUT).astype(BF), w_merge[...])

    head_lanes = [(lane // 32 == h).astype(F32).astype(BF) for h in range(4)]

    def spread(block):
        return jnp.concatenate([block * head_lanes[h] for h in range(4)], 0)

    def heads_of(wide):
        total = wide[0:64] * head_lanes[0].astype(F32)
        for h in range(1, 4):
            total = total + wide[64 * h : 64 * h + 64] * head_lanes[h].astype(F32)
        return total

    def group_lanes(kind, group):
        start = C * kind + 128 * group
        return slice(start, start + 128)

    def units_of(windows):
        return [(w, group) for w in windows for group in range(GROUPS)]

    def of_window(ref, w, kind, group):
        return get_window(ref, *WINDOWS[w], group_lanes(kind, group))

    ones = (lax.broadcasted_iota(jnp.int32, (128, 128), 0) < 64) == low
    ones = ones.astype(F32).astype(BF)

    def half_sums(values):
        rows = values[0].shape[0]
        joined = jnp.concatenate(values, 0)
        high = joined.astype(BF)
        rest = (joined - high.astype(F32)).astype(BF)
        total = mm(high, ones) + mm(rest, ones)
        return [total[rows * i : rows * i + rows] for i in range(len(values))]

    def split_halves(wide):
        return [part[:, 128 * i : 128 * i + 128] for part in wide for i in range(2)]

    def join_halves(parts):
        return [
            jnp.concatenate([parts[i].astype(BF), parts[i + 1].astype(BF)], 1)
            for i in range(0, len(parts), 2)
        ]

    def softmax(units, scores, rows):
        parts = split_halves(scores)
        for i, (a, g) in enumerate(units):
            for j in range(2):
                bias = pair_bias(2 * g + j)[rows] + mask[a, rows]
                parts[2 * i + j] = parts[2 * i + j] * SCALE + bias
        tops = [halves(jnp.max, -3e38, low, part) for part in parts]
        parts = [jnp.exp(part - top) for part, top in zip(parts, tops)]
        sums = half_sums(parts)
        return [part * (1.0 / total) for part, total in zip(parts, sums)]

    def attend(*windows):
        units = units_of(windows)
        scores = [
            mm_t(of_window(qkv, w, 0, g), spread(of_window(qkv, w, 1, g))) for w, g in units
        ]
        parts = softmax([(WINDOWS[w][0], g) for w, g in units], scores, slice(0, 64))
        for i, (w, g) in enumerate(units):
            for j in range(2):
                probs[GROUPS * w + g, :, 128 * j : 128 * j + 128] = parts[2 * i + j]
        for (w, g), prob in zip(units, join_halves(parts)):
            result = mm(prob, spread(of_window(qkv, w, 2, g))).astype(BF)
            put_window(attended, *WINDOWS[w], group_lanes(0, g), result)

    def attend_first():
        units = [(a, g) for a in range(2) for g in range(GROUPS)]

        def part(a, kind, g):
            lanes = group_lanes(kind, g)
            near, far = 256 + 32 * a, 320 + 32 * a
            return jnp.concatenate([qkv[near : near + 32, lanes], qkv[far : far + 32, lanes]], 0)

        scores = [
            mm_t(qkv[320 + 32 * a : 352 + 32 * a, group_lanes(0, g)], spread(part(a, 1, g)))
            for a, g in units
        ]
        parts = softmax(units, scores, slice(32, 64))
        for (a, g), prob in zip(units, join_halves(parts)):
            result = mm(prob, spread(part(a, 2, g))).astype(BF)
            first_scr[32 * a : 32 * a + 32, group_lanes(0, g)] = result

    attend(2, 3)

    exchange(0, west_id).wait()
    exchange(1, east_id).wait()
    widen_reach(0)
    normed, inverse_std = normalize(ex_recv[0:2].astype(F32).reshape(128, C))
    normed_east[...] = normed[0:64]
    std_east[...] = inverse_std[0:64]
    rolled = normed.astype(BF)
    rolled_east = rolled[0:64]
    qkv[192:320] = mm(rolled, w_attend[...]).astype(BF)
    attend_first()
    attend(0, 1)
    copies["to_quad"].wait()
    copies["win_quad"].wait()
    copies["w_out"].wait()
    features_quad = mm(to_quad[...], tokens16)
    widen_reach(1)

    extended = jnp.concatenate([attended[0:192], first_scr[...]], 0)
    attended_quad = mm(win_quad[...], extended).astype(BF)
    hidden = (features_quad + mm(attended_quad, w_out[...])).astype(BF).astype(F32)
    quads = [hidden[64 * e : 64 * e + 64] for e in range(4)]

    def mean(blocks):
        total = (blocks[0] + blocks[1]) + (blocks[2] + blocks[3])
        return jnp.sum(total, -1, keepdims=True) * (1.0 / (4 * C))

    centre = mean(quads)
    quads = [quad - centre for quad in quads]
    quad_std = lax.rsqrt(mean([quad * quad for quad in quads]) + 1e-05)
    quads = [quad * quad_std for quad in quads]
    grads = [quad_grad_in[:, C * e : C * e + C] for e in range(4)]
    first = mean(grads)
    second = mean([grad * quad for grad, quad in zip(grads, quads)])
    for e in range(4):
        value = quad_std * (grads[e] - first - quads[e] * second)
        hidden_grad[64 * e : 64 * e + 64] = value.astype(BF)
    copies["win_quad_t"].wait()
    ex_send[2] = mm(win_quad_t[192:256], hidden_grad[...]).astype(BF)
    exchange(2, west_id).start()
    copies["row_pick"].wait()
    left_r[:, 0:192] = mm_t(row_pick[...], rolled_own).astype(BF)
    left_r[:, 192:256] = mm_t(row_pick[...], rolled_east).astype(BF)
    left_o[...] = mm_t(row_pick[...], attended[...]).astype(BF)
    own_grad = mm(win_quad_t[0:192], hidden_grad[...]).astype(BF)
    branch_grad[0:192] = own_grad
    outer[0:192] = mm_t(own_grad, w_out[...]).astype(BF)
    merged = mm(jnp.concatenate([quad.astype(BF) for quad in quads], 1), w_merge[...])
    for i in range(7):
        merged_ref[i] = merged[8 * i : 8 * i + 7].astype(BF)
    copies["to_quad_t"].wait()
    hidden_own = mm(to_quad_t[...], hidden_grad[...])

    def values_back(*windows):
        units = units_of(windows)
        wide = [
            t_mm(probs[GROUPS * w + g].astype(BF), of_window(outer, w, 0, g)) for w, g in units
        ]
        for (w, g), value in zip(units, wide):
            back = heads_of(value).astype(BF)
            put_window(proj_grad, *WINDOWS[w], group_lanes(2, g), back)

    def scores_back(*windows):
        units = units_of(windows)
        wide = [
            mm_t(of_window(outer, w, 0, g), spread(of_window(qkv, w, 2, g))) for w, g in units
        ]
        grads = split_halves(wide)
        prob = split_halves([probs[GROUPS * w + g] for w, g in units])
        sums = half_sums([p * grad for p, grad in zip(prob, grads)])
        parts = [p * (grad - total) * SCALE for p, grad, total in zip(prob, grads, sums)]
        soft = join_halves(parts)
        wide = [t_mm(part, of_window(qkv, w, 0, g)) for (w, g), part in zip(units, soft)]
        for (w, g), part in zip(units, soft):
            back = mm(part, spread(of_window(qkv, w, 1, g))).astype(BF)
            put_window(proj_grad, *WINDOWS[w], group_lanes(0, g), back)
        for (w, g), value in zip(units, wide):
            back = heads_of(value).astype(BF)
            put_window(proj_grad, *WINDOWS[w], group_lanes(1, g), back)

    def core_copy(i):
        return pltpu.make_async_remote_copy(
            src_ref=g_send.at[i, 1 - core], dst_ref=g_recv.at[i], send_sem=c_ssem.at[i],
            recv_sem=c_rsem.at[i], device_id={"frame_2": 1 - core},
        )

    def start_core(i, product):
        product = product.reshape(2, 192, C)
        g_own[i] = product
        if scatter:
            g_send[i] = product.astype(BF)
            core_copy(i).start()

    def x_copies(i, sent, landing):
        return [
            pltpu.make_async_remote_copy(
                src_ref=sent.at[(xi + step) % 4], dst_ref=landing.at[step - 1],
                send_sem=x_ssem.at[X_SLOTS[i]], recv_sem=x_rsem.at[X_SLOTS[i]],
                device_id=x_id(step),
            )
            for step in (2, 1, 3)
        ]

    def end_all(landing, sent_sem, landed_sem):
        pltpu.make_async_remote_copy(
            src_ref=landing, dst_ref=landing, send_sem=sent_sem, recv_sem=landed_sem,
            device_id={"frame_2": 1 - core},
        ).wait()

    def end_x(i, landing):
        end_all(landing, x_ssem.at[X_SLOTS[i]], x_rsem.at[X_SLOTS[i]])

    def y_copy(i, m, sent, landing):
        return pltpu.make_async_remote_copy(
            src_ref=sent.at[m], dst_ref=landing.at[y], send_sem=y_ssem.at[Y_SLOTS[i], m],
            recv_sem=y_rsem.at[Y_SLOTS[i], y],
            device_id={"frame_1": 2 * core + m // 2, "frame_2": m % 2},
        )

    def y_landed(i, source, sent, landing):
        return pltpu.make_async_remote_copy(
            src_ref=sent.at[0], dst_ref=landing.at[source], send_sem=y_ssem.at[Y_SLOTS[i], 0],
            recv_sem=y_rsem.at[Y_SLOTS[i], source], device_id={"frame_2": 1 - core},
        )

    def stays(m):
        return jnp.logical_and(2 * core + m // 2 == y, core == m % 2)

    def start_y(i, sent, landing):
        for m in range(4):

            @pl.when(stays(m))
            def _():
                landing[y] = sent[m]

            @pl.when(jnp.logical_not(stays(m)))
            def _():
                y_copy(i, m, sent, landing).start()

    def end_y(i, sent, landing):
        for source in range(4):
            mine = jnp.logical_and(y == source, y // 2 == core)

            @pl.when(jnp.logical_not(mine))
            def _():
                y_landed(i, source, sent, landing).wait_recv()

        for m in range(4):

            @pl.when(jnp.logical_not(stays(m)))
            def _():
                y_copy(i, m, sent, landing).wait_send()

        total = landing[0].astype(F32)
        for source in range(1, 4):
            total = total + landing[source].astype(F32)
        return total

    wide_lane = lax.broadcasted_iota(jnp.int32, (1, C), 1)

    def segments(i, block):
        one, two, three = (block[16 * k : 16 * k + 16] for k in range(3))

        def left(value, count):
            return pltpu.roll(value, C - count, 1)

        if i == 0:
            second = jnp.where(wide_lane < 96, left(one, 288), pltpu.roll(two, 96, 1))
            third = jnp.where(wide_lane < 192, left(two, 192), pltpu.roll(three, 192, 1))
            return one, second, third, left(three, 96)
        if i == 1:
            return one, left(one, 96), two, three
        if i == 2:
            return one, two, three, left(three, 288)
        return one, two, left(two, 192), three

    def start_first(i):
        if not scatter:
            return
        core_copy(i).wait()
        total = (g_own[i, core] + g_recv[i].astype(F32)).reshape(4, 48, C)
        j = i // 2
        if i % 2 == 0:
            x_own[j] = total
            x_send[j] = total.astype(BF)
            for copy in x_copies(i, x_send.at[j], x_recv.at[j]):
                copy.start()
        else:
            for block in range(4):
                for m, value in enumerate(segments(i, total[block])):
                    y_send[j, m, block] = value.astype(BF)
            start_y(i, y_send.at[j], y_recv.at[j])

    def start_second(i):
        j = i // 2
        if i % 2 == 0:
            end_x(i, x_recv.at[j])
            total = x_own[j, xi]
            for step in (1, 2, 3):
                total = total + x_recv[j, step - 1].astype(F32)
            for m, value in enumerate(segments(i, total)):
                y_send2[j, m] = value.astype(BF)
            start_y(4 + j, y_send2.at[j], y_recv2.at[j])
        else:
            total = end_y(i, y_send.at[j], y_recv.at[j])
            x_own2[j] = total
            x_send2[j] = total.astype(BF)
            for copy in x_copies(4 + j, x_send2.at[j], x_recv2.at[j]):
                copy.start()

    def z_copy(j, step):
        return pltpu.make_async_remote_copy(
            src_ref=z_send.at[j, (z + step) % 16], dst_ref=z_recv.at[j, step - 1],
            send_sem=z_ssem.at[j], recv_sem=z_rsem.at[j], device_id=z_id(step),
        )

    z_steps = sorted(range(1, 16), key=lambda step: -min(step, 16 - step))

    def start_z(j):
        first = end_y(4 + j, y_send2.at[j], y_recv2.at[j])
        end_x(4 + j, x_recv2.at[j])
        second = x_own2[j, xi]
        for step in (1, 2, 3):
            second = second + x_recv2[j, step - 1].astype(F32)
        for t in range(3):
            lanes = slice(128 * t, 128 * t + 128)
            z_line[j, pl.ds(t, 16, stride=8), :] = first[:, lanes]
            z_line[j, pl.ds(t + 3, 16, stride=8), :] = second[:, lanes]
        for t in (6, 7):
            z_line[j, pl.ds(t, 16, stride=8), :] = jnp.zeros((16, 128), F32)
        z_send[j] = z_line[j].reshape(16, 8, 128).astype(BF)
        for step in z_steps:
            z_copy(j, step).start()

    def end_z(j):
        total = z_send[j, z].astype(F32)
        end_all(z_recv.at[j], z_ssem.at[j], z_rsem.at[j])
        for step in z_steps:
            total = total + z_recv[j, step - 1].astype(F32)
        share_ref[8 * j : 8 * j + 8] = total

    scores_back(2, 3)
    exchange(2, west_id).wait()
    widen_reach(2)
    branch_grad[192:256] = ex_recv[2]
    outer[192:256] = mm_t(ex_recv[2], w_out[...]).astype(BF)
    start_core(0, mm(left_o[...], branch_grad[...]))
    values_back(0, 1, 2, 3)
    start_core(1, mm(left_r[...], proj_grad[:, 2 * C : 3 * C]))
    start_first(0)
    scores_back(0, 1)
    start_first(1)
    start_core(2, mm(left_r[...], proj_grad[:, 0:C]))
    start_core(3, mm(left_r[...], proj_grad[:, C : 2 * C]))
    east_grad = mm_t(proj_grad[192:256], w_attend[...])
    east_grad = normalize_back(normed_east[...], std_east[...], east_grad)
    ex_send[3] = east_grad.astype(BF)
    exchange(3, east_id).start()
    start_first(2)
    start_first(3)
    copies["to_window_t"].wait()
    own_proj = mm(to_window_t[:, 0:192], proj_grad[0:192]).astype(BF)
    own_grad = mm_t(own_proj, w_attend[...])
    own_grad = normalize_back(normed_scr[...], std_scr[...], own_grad)
    feature_scr[...] = hidden_own + own_grad

    def end_features():
        exchange(3, east_id).wait()
        grad = feature_scr[...] + mm(to_window_t[:, 192:256], ex_recv[3])
        grad = grad.reshape(14, 16, C)
        for row in range(14):
            grad_ref[row] = grad[row, 0:14].astype(BF)

    if scatter:
        for group in range(4):
            start_second(group)
        start_z(0)
        start_z(1)
        end_features()
        end_z(0)
        end_z(1)
    else:
        end_features()
        share_ref[...] = jnp.zeros_like(share_ref)
        local_ref[...] = g_own[...]


def finish(merged_in, grad_in, share, merged_ref, grad_ref, attend_ref, output_ref):
    merged_ref[0] = merged_in[...]
    grad_ref[0] = grad_in[...]
    lane = lax.broadcasted_iota(jnp.int32, (1, 128), 1)

    def put(ref, pieces):
        lines = [jnp.zeros((1, 128), F32) for _ in range(-(-ref.shape[0] // 128))]
        start = 0
        for first, width in pieces:
            skip, turn = divmod(start, 128)
            values = [share[first + i : first + i + 1, :] for i in range(3)]
            if turn:
                values = [pltpu.roll(value, turn, 1) for value in values]
            for j in range(skip, (start + width - 1) // 128 + 1):
                value = values[min(j - skip, 2)]
                if turn and j > skip:
                    value = jnp.where(lane < turn, values[j - skip - 1], value)
                at = lane + 128 * j
                inside = jnp.logical_and(at >= start, at < start + width)
                lines[j] = jnp.where(inside, value, lines[j])
            start += width
        for j, value in enumerate(lines):
            count = min(128, ref.shape[0] - 128 * j)
            ref[128 * j : 128 * j + count] = value.reshape(128)[:count]

    put(output_ref, ((0, 288),))
    v, q, k = 3, 8, 11
    segment = 2 * (lax.axis_index("frame_1") % 2) + lax.axis_index("frame_2")
    for m, pieces in enumerate((
        ((q, 384), (k, 384), (v, 96)),
        ((v, 288), (q, 384), (k, 192)),
        ((k, 192), (v, 384), (q, 288)),
        ((q, 96), (k, 384), (v, 384)),
    )):
        pl.when(segment == m)(functools.partial(put, attend_ref, pieces))


def local_call(scatter, features, position_bias, attend_weight, output_weight, merge_weight, cotangent):
    given = (features[0], cotangent[0], position_bias.T, attend_weight, output_weight, merge_weight)
    given = given + tuple(jnp.asarray(table) for table in tables())
    dma = pltpu.SemaphoreType.DMA
    scratch = [pltpu.VMEM(a.shape, a.dtype) for a in given]
    scratch += [
        pltpu.VMEM((14, 16, C), F32),
        pltpu.VMEM((8, 8, OUT), F32),
        pltpu.VMEM((16, 256), F32),
        pltpu.VMEM((1024, 128), F32),
        pltpu.VMEM((1024, 128), F32),
        pltpu.VMEM((224, C), F32),
        pltpu.VMEM((224, 1), F32),
        pltpu.VMEM((64, C), F32),
        pltpu.VMEM((64, 1), F32),
        pltpu.VMEM((384, 3 * C), BF),
        pltpu.VMEM((12, 64, 256), F32),
        pltpu.VMEM((256, C), BF),
        pltpu.VMEM((256, C), BF),
        pltpu.VMEM((256, C), BF),
        pltpu.VMEM((256, 3 * C), BF),
        pltpu.VMEM((256, C), BF),
        pltpu.VMEM((C, 256), BF),
        pltpu.VMEM((C, 256), BF),
        pltpu.VMEM((224, C), F32),
        pltpu.VMEM((64, C), BF),
        pltpu.VMEM((4, 64, C), BF),
        pltpu.VMEM((4, 64, C), BF),
        pltpu.VMEM((4, 2, 192, C), F32),
        pltpu.VMEM((4, 2, 192, C), BF),
        pltpu.VMEM((4, 192, C), BF),
        pltpu.VMEM((2, 4, 48, C), F32),
        pltpu.VMEM((2, 4, 48, C), BF),
        pltpu.VMEM((2, 3, 48, C), BF),
        pltpu.VMEM((2, 4, 4, 16, C), BF),
        pltpu.VMEM((2, 4, 4, 16, C), BF),
        pltpu.VMEM((2, 4, 16, C), F32),
        pltpu.VMEM((2, 4, 16, C), BF),
        pltpu.VMEM((2, 3, 16, C), BF),
        pltpu.VMEM((2, 4, 16, C), BF),
        pltpu.VMEM((2, 4, 16, C), BF),
        pltpu.VMEM((2, 128, 128), F32),
        pltpu.VMEM((2, 16, 8, 128), BF),
        pltpu.VMEM((2, 15, 8, 128), BF),
        dma((N_IN,)), dma((4,)), dma((4,)), dma((4,)), dma((4,)), dma((4,)), dma((4,)),
        dma((4, 4)), dma((4, 4)), dma((2,)), dma((2,)), pltpu.SemaphoreType.REGULAR((3,)),
    ]
    vmem = pl.BlockSpec(memory_space=pltpu.VMEM)
    return pl.pallas_call(
        functools.partial(kernel, scatter),
        out_shape=(
            pltpu.VMEM((7, 7, OUT), BF),
            pltpu.VMEM((14, 14, C), BF),
            pltpu.VMEM((16, 128), F32),
        )
        + (() if scatter else (jax.ShapeDtypeStruct((4, 2, 192, C), F32),)),
        in_specs=[pl.BlockSpec(memory_space=pl.ANY)] * N_IN,
        out_specs=(vmem,) * (3 if scatter else 4),
        scratch_shapes=scratch,
        compiler_params=pltpu.CompilerParams(collective_id=0, has_side_effects=True),
    )(*given)


def per_device(*arrays):
    merged, feature_grad, share = local_call(True, *arrays)
    vmem = pl.BlockSpec(memory_space=pltpu.VMEM)
    return pl.pallas_call(
        finish,
        out_shape=(
            jax.ShapeDtypeStruct((1, *merged.shape), BF),
            jax.ShapeDtypeStruct((1, *feature_grad.shape), BF),
            jax.ShapeDtypeStruct((864,), F32),
            jax.ShapeDtypeStruct((288,), F32),
        ),
        in_specs=(vmem,) * 3,
        out_specs=(vmem,) * 4,
        compiler_params=pltpu.CompilerParams(vmem_limit_bytes=8 << 20),
    )(merged, feature_grad, share)


def solution(mesh):
    split = Mesh(mesh.devices.reshape(16, 2, 2, 4, 2), AZIM_FRAME)
    placed = (P(FRAME, None, AZIM, None), P(), P(), P(), P(), P(FRAME, None, AZIM, None))
    return jax.shard_map(
        per_device,
        mesh=split,
        in_specs=placed,
        out_specs=(
            P(FRAME, None, AZIM, None),
            P(FRAME, None, AZIM, None),
            P(AZIM_FRAME),
            P(AZIM_FRAME),
        ),
        check_vma=False,
    )
```

```python
import functools

import jax
import jax.numpy as jnp
import ml_dtypes
import numpy as np
from jax import lax
from jax.experimental import pallas as pl
from jax.experimental.pallas import tpu as pltpu
from jax.sharding import Mesh
from jax.sharding import PartitionSpec as P

AZIM = ("azim_0", "azim_1")
AZIM_FRAME = ("azim_0", "azim_1", "frame_0", "frame_1", "frame_2")
FRAME = ("frame_0", "frame_1", "frame_2")

BF = jnp.bfloat16
F32 = jnp.float32
C = 384
OUT = 768
GROUPS = 3
SCALE = 32 ** (-0.5)
WINDOWS = ((0, 1), (1, 1), (0, 0), (1, 0))


def position_row(row, col):
    return 4 * row + col if col < 4 else 32 + 3 * row + col - 4


def east_row(row, col):
    rolled = (row - 3) % 14
    return 32 * (rolled // 7) + 3 * (rolled % 7) + col


@functools.cache
def tables():
    to_window = np.zeros((256, 224), np.float32)
    for a in range(2):
        for b in range(2):
            for row in range(7):
                for col in range(7):
                    frame_row, frame_col = (7 * a + row + 3) % 14, 7 * b + col + 3
                    if frame_col >= 14:
                        continue
                    at = position_row(row, col)
                    line = 64 * a + at if b == 0 else 128 + 32 * a + at
                    to_window[line, 16 * frame_row + frame_col] = 1
    for row in range(14):
        for col in range(3):
            to_window[192 + east_row(row, col), 16 * row + col] = 1
    to_quad = np.zeros((256, 224), np.float32)
    for block in range(4):
        for i in range(7):
            for j in range(7):
                token = 16 * (2 * i + block % 2) + 2 * j + block // 2
                to_quad[64 * block + 8 * i + j, token] = 1
    window_to_quad = to_quad @ to_window.T
    rows = np.zeros((C, C), np.float32)
    for c in range(2):
        for xi in range(4):
            for k in range(3):
                for z in range(16):
                    rows[192 * c + 48 * xi + 16 * k + z, 24 * z + 6 * xi + 3 * c + k] = 1
    index = np.full((64, 64), 255.0, np.float32)
    mask = np.zeros((2, 64, 64), np.float32)
    valid = np.zeros(64, bool)
    for row in range(7):
        for col in range(7):
            p = position_row(row, col)
            valid[p] = True
            for row_q in range(7):
                for col_q in range(7):
                    q = position_row(row_q, col_q)
                    index[p, q] = 13 * (row - row_q + 6) + col - col_q + 6
                    if (row < 4) != (row_q < 4):
                        mask[1, p, q] = -100.0
    mask[:, :, ~valid] = -1e30
    mask = np.concatenate([mask, mask], -1)
    bf = ml_dtypes.bfloat16
    return (
        to_window.astype(bf),
        np.ascontiguousarray(to_window.T).astype(bf),
        to_quad.astype(bf),
        np.ascontiguousarray(to_quad.T).astype(bf),
        window_to_quad.astype(bf),
        np.ascontiguousarray(window_to_quad.T).astype(bf),
        rows.astype(bf),
        index.reshape(32, 128),
        mask,
    )


def mm(left, right):
    return lax.dot_general(left, right, (((1,), (0,)), ((), ())), preferred_element_type=F32)


def mm_t(left, right):
    return lax.dot_general(left, right, (((1,), (1,)), ((), ())), preferred_element_type=F32)


def t_mm(left, right):
    return lax.dot_general(left, right, (((0,), (0,)), ((), ())), preferred_element_type=F32)


def normalize(values):
    centred = values - jnp.mean(values, -1, keepdims=True)
    inverse_std = lax.rsqrt(jnp.mean(centred * centred, -1, keepdims=True) + 1e-05)
    return centred * inverse_std, inverse_std


def normalize_back(normed, inverse_std, grads):
    first = jnp.mean(grads, -1, keepdims=True)
    second = jnp.mean(grads * normed, -1, keepdims=True)
    return inverse_std * (grads - first - normed * second)


def window_of(values, a, b):
    if b == 0:
        return values[64 * a : 64 * a + 64]
    near, far = 128 + 32 * a, 192 + 32 * a
    return jnp.concatenate([values[near : near + 32], values[far : far + 32]], 0)


def put_window(ref, a, b, lanes, values):
    if b == 0:
        ref[64 * a : 64 * a + 64, lanes] = values
    else:
        near, far = 128 + 32 * a, 192 + 32 * a
        ref[near : near + 32, lanes] = values[:32]
        ref[far : far + 32, lanes] = values[32:]


def get_window(ref, a, b, lanes):
    if b == 0:
        return ref[64 * a : 64 * a + 64, lanes]
    near, far = 128 + 32 * a, 192 + 32 * a
    return jnp.concatenate([ref[near : near + 32, lanes], ref[far : far + 32, lanes]], 0)


def halves(op, empty, low, values):
    first = op(jnp.where(low, values, empty), -1, keepdims=True)
    second = op(jnp.where(low, empty, values), -1, keepdims=True)
    return jnp.where(low, first, second)


NAMES = (
    "feat", "cot", "pos", "w_attend", "w_out", "w_merge", "to_window", "to_window_t", "to_quad",
    "to_quad_t", "win_quad", "win_quad_t", "row_pick", "index", "mask",
)
ORDER = (
    "feat", "to_window", "w_attend", "pos", "index", "mask", "cot", "w_merge", "row_pick",
    "to_quad", "win_quad", "w_out", "win_quad_t", "to_quad_t", "to_window_t",
)
N_IN = len(NAMES)
X_SLOTS = {0: 0, 2: 1, 4: 2, 5: 3}
Y_SLOTS = {1: 0, 3: 1, 4: 2, 5: 3}


def kernel(scatter, *refs):
    given, refs = refs[:N_IN], refs[N_IN:]
    merged_ref, grad_ref, share_ref = refs[:3]
    if scatter:
        refs = refs[3:]
    else:
        local_ref, refs = refs[3], refs[4:]
    held, refs = refs[:N_IN], refs[N_IN:]
    (
        x_scr, cot_scr, table_scr, bias_a, bias_b, normed_scr, std_scr,
        normed_east, std_east, qkv, probs, attended, branch_grad, outer, proj_grad,
        hidden_grad, left_o, left_r, feature_scr, first_scr,
        ex_send, ex_recv,
        g_own, g_send, g_recv, x_own, x_send, x_recv, y_send, y_recv,
        x_own2, x_send2, x_recv2, y_send2, y_recv2, z_line, z_send, z_recv,
        in_sem, ex_ssem, ex_rsem, c_ssem, c_rsem, x_ssem, x_rsem, y_ssem, y_rsem,
        z_ssem, z_rsem, near_sem,
    ) = refs
    (
        feat, cot, pos, w_attend, w_out, w_merge, to_window, to_window_t, to_quad, to_quad_t,
        win_quad, win_quad_t, row_pick, index, mask,
    ) = held
    copies = {
        name: pltpu.make_async_copy(given[i], held[i], in_sem.at[i])
        for i, name in enumerate(NAMES)
    }
    for name in ORDER[:2]:
        copies[name].start()

    z, x_lo = lax.axis_index("azim_0"), lax.axis_index("azim_1")
    x_hi, y, core = (lax.axis_index(name) for name in FRAME)
    n_z = lax.axis_size("azim_0")
    n_azim = n_z * 2
    azim = 2 * z + x_lo
    east, west = (azim + 1) % n_azim, (azim + n_azim - 1) % n_azim
    east_id = {"azim_0": east // 2, "azim_1": east % 2}
    west_id = {"azim_0": west // 2, "azim_1": west % 2}
    xi = 2 * x_lo + x_hi

    def x_id(step):
        other = (xi + step) % 4
        return {"azim_1": other // 2, "frame_0": other % 2}

    def z_id(step):
        return {"azim_0": (z + n_z + step) % n_z}

    barrier = pltpu.get_barrier_semaphore()
    near = [east_id, west_id]
    if scatter:
        near += [{"frame_2": 1 - core}]
        near += [x_id(step) for step in (1, 2, 3)]
        near += [{"frame_1": (y + step) % 4} for step in (1, 2, 3)]
        near += [{"frame_1": (y + step) % 4, "frame_2": 1 - core} for step in (1, 2, 3)]
        near += [z_id(1), z_id(-1)]
    for device in near:
        pl.semaphore_signal(barrier, inc=1, device_id=device)

    def exchange(i, device):
        return pltpu.make_async_remote_copy(
            src_ref=ex_send.at[i], dst_ref=ex_recv.at[i], send_sem=ex_ssem.at[i],
            recv_sem=ex_rsem.at[i], device_id=device,
        )

    for name in ORDER[2:7]:
        copies[name].start()
    copies["feat"].wait()
    for name in ORDER[7:]:
        copies[name].start()
    x_scr[...] = jnp.zeros_like(x_scr)
    for row in range(14):
        x_scr[row, 0:14, :] = feat[row].astype(F32)
    tokens = x_scr[...].reshape(224, C)
    tokens16 = tokens.astype(BF)
    copies["to_window"].wait()
    shared = mm(to_window[128:256], tokens16).astype(BF)
    ex_send[0] = shared[64:128]
    ex_send[1] = shared[0:64]
    pl.semaphore_wait(barrier, len(near))
    exchange(0, west_id).start()
    exchange(1, east_id).start()
    if scatter:
        for step in (1, -1):
            pl.semaphore_signal(near_sem.at[0], inc=1, device_id=z_id(step))

    def widen_reach(i):
        if not scatter:
            return
        pl.semaphore_wait(near_sem.at[i], 2)
        if i < 2:
            for step in (2 ** (i + 1), -(2 ** (i + 1))):
                pl.semaphore_signal(near_sem.at[i + 1], inc=1, device_id=z_id(step))

    normed, inverse_std = normalize(tokens)
    normed_scr[...] = normed
    std_scr[...] = inverse_std
    rolled = mm(to_window[...], normed.astype(BF)).astype(BF)
    rolled_own = rolled[0:192]
    copies["w_attend"].wait()
    projected = mm(rolled, w_attend[...]).astype(BF)
    qkv[0:192] = projected[0:192]
    qkv[320:384] = projected[192:256]

    copies["pos"].wait()
    copies["index"].wait()
    copies["mask"].wait()
    table_scr[...] = jnp.zeros_like(table_scr)
    table_scr[0:12, 0:169] = pos[...]
    table = table_scr[...]
    high = table.astype(BF).astype(F32)
    both = jnp.concatenate([high, table - high], 0).astype(BF)
    lane = lax.broadcasted_iota(jnp.int32, (1, 128), 1)
    entry = lax.broadcasted_iota(jnp.int32, (256, 128), 0).astype(F32)
    for t in range(0, 32, 4):
        picks = [
            jnp.where(entry == index[u : u + 1, :], 1.0, 0.0).astype(BF) for u in range(t, t + 4)
        ]
        wide = mm(both, jnp.concatenate(picks, 1))
        for u in range(4):
            part = wide[:, 128 * u : 128 * u + 128]
            part = part[0:16] + part[16:32]
            turned = pltpu.roll(part, 64, 1)
            p = 2 * (t + u)
            bias_a[pl.ds(p, 16, stride=64), :] = part
            bias_a[pl.ds(p + 1, 16, stride=64), :] = turned
            bias_b[pl.ds(p, 16, stride=64), :] = turned
            bias_b[pl.ds(p + 1, 16, stride=64), :] = part
    low = lane < 64

    def pair_bias(pair):
        first = bias_a[128 * pair : 128 * pair + 64, :]
        second = bias_b[128 * pair + 64 : 128 * pair + 128, :]
        return jnp.where(low, first, second)

    copies["cot"].wait()
    cot_scr[...] = jnp.zeros_like(cot_scr)
    for row in range(7):
        cot_scr[row, 0:7, :] = cot[row].astype(F32)
    copies["w_merge"].wait()
    quad_grad_in = mm_t(cot_scr[...].reshape(64, OUT).astype(BF), w_merge[...])

    head_lanes = [(lane // 32 == h).astype(F32).astype(BF) for h in range(4)]

    def spread(block):
        return jnp.concatenate([block * head_lanes[h] for h in range(4)], 0)

    def heads_of(wide):
        total = wide[0:64] * head_lanes[0].astype(F32)
        for h in range(1, 4):
            total = total + wide[64 * h : 64 * h + 64] * head_lanes[h].astype(F32)
        return total

    def group_lanes(kind, group):
        start = C * kind + 128 * group
        return slice(start, start + 128)

    def units_of(windows):
        return [(w, group) for w in windows for group in range(GROUPS)]

    def of_window(ref, w, kind, group):
        return get_window(ref, *WINDOWS[w], group_lanes(kind, group))

    ones = (lax.broadcasted_iota(jnp.int32, (128, 128), 0) < 64) == low
    ones = ones.astype(F32).astype(BF)

    def half_sums(values):
        rows = values[0].shape[0]
        joined = jnp.concatenate(values, 0)
        high = joined.astype(BF)
        rest = (joined - high.astype(F32)).astype(BF)
        total = mm(high, ones) + mm(rest, ones)
        return [total[rows * i : rows * i + rows] for i in range(len(values))]

    def split_halves(wide):
        return [part[:, 128 * i : 128 * i + 128] for part in wide for i in range(2)]

    def join_halves(parts):
        return [
            jnp.concatenate([parts[i].astype(BF), parts[i + 1].astype(BF)], 1)
            for i in range(0, len(parts), 2)
        ]

    def softmax(units, scores, rows):
        parts = split_halves(scores)
        for i, (a, g) in enumerate(units):
            for j in range(2):
                bias = pair_bias(2 * g + j)[rows] + mask[a, rows]
                parts[2 * i + j] = parts[2 * i + j] * SCALE + bias
        tops = [halves(jnp.max, -3e38, low, part) for part in parts]
        parts = [jnp.exp(part - top) for part, top in zip(parts, tops)]
        sums = half_sums(parts)
        return [part * (1.0 / total) for part, total in zip(parts, sums)]

    def attend(*windows):
        units = units_of(windows)
        scores = [
            mm_t(of_window(qkv, w, 0, g), spread(of_window(qkv, w, 1, g))) for w, g in units
        ]
        parts = softmax([(WINDOWS[w][0], g) for w, g in units], scores, slice(0, 64))
        for i, (w, g) in enumerate(units):
            for j in range(2):
                probs[GROUPS * w + g, :, 128 * j : 128 * j + 128] = parts[2 * i + j]
        for (w, g), prob in zip(units, join_halves(parts)):
            result = mm(prob, spread(of_window(qkv, w, 2, g))).astype(BF)
            put_window(attended, *WINDOWS[w], group_lanes(0, g), result)

    def attend_first():
        units = [(a, g) for a in range(2) for g in range(GROUPS)]

        def part(a, kind, g):
            lanes = group_lanes(kind, g)
            near, far = 256 + 32 * a, 320 + 32 * a
            return jnp.concatenate([qkv[near : near + 32, lanes], qkv[far : far + 32, lanes]], 0)

        scores = [
            mm_t(qkv[320 + 32 * a : 352 + 32 * a, group_lanes(0, g)], spread(part(a, 1, g)))
            for a, g in units
        ]
        parts = softmax(units, scores, slice(32, 64))
        for (a, g), prob in zip(units, join_halves(parts)):
            result = mm(prob, spread(part(a, 2, g))).astype(BF)
            first_scr[32 * a : 32 * a + 32, group_lanes(0, g)] = result

    attend(2, 3)

    exchange(0, west_id).wait()
    exchange(1, east_id).wait()
    widen_reach(0)
    normed, inverse_std = normalize(ex_recv[0:2].astype(F32).reshape(128, C))
    normed_east[...] = normed[0:64]
    std_east[...] = inverse_std[0:64]
    rolled = normed.astype(BF)
    rolled_east = rolled[0:64]
    qkv[192:320] = mm(rolled, w_attend[...]).astype(BF)
    attend_first()
    attend(0, 1)
    copies["to_quad"].wait()
    copies["win_quad"].wait()
    copies["w_out"].wait()
    features_quad = mm(to_quad[...], tokens16)
    widen_reach(1)

    extended = jnp.concatenate([attended[0:192], first_scr[...]], 0)
    attended_quad = mm(win_quad[...], extended).astype(BF)
    hidden = (features_quad + mm(attended_quad, w_out[...])).astype(BF).astype(F32)
    quads = [hidden[64 * e : 64 * e + 64] for e in range(4)]

    def mean(blocks):
        total = (blocks[0] + blocks[1]) + (blocks[2] + blocks[3])
        return jnp.sum(total, -1, keepdims=True) * (1.0 / (4 * C))

    centre = mean(quads)
    quads = [quad - centre for quad in quads]
    quad_std = lax.rsqrt(mean([quad * quad for quad in quads]) + 1e-05)
    quads = [quad * quad_std for quad in quads]
    grads = [quad_grad_in[:, C * e : C * e + C] for e in range(4)]
    first = mean(grads)
    second = mean([grad * quad for grad, quad in zip(grads, quads)])
    for e in range(4):
        value = quad_std * (grads[e] - first - quads[e] * second)
        hidden_grad[64 * e : 64 * e + 64] = value.astype(BF)
    copies["win_quad_t"].wait()
    ex_send[2] = mm(win_quad_t[192:256], hidden_grad[...]).astype(BF)
    exchange(2, west_id).start()
    copies["row_pick"].wait()
    left_r[:, 0:192] = mm_t(row_pick[...], rolled_own).astype(BF)
    left_r[:, 192:256] = mm_t(row_pick[...], rolled_east).astype(BF)
    left_o[...] = mm_t(row_pick[...], attended[...]).astype(BF)
    own_grad = mm(win_quad_t[0:192], hidden_grad[...]).astype(BF)
    branch_grad[0:192] = own_grad
    outer[0:192] = mm_t(own_grad, w_out[...]).astype(BF)
    merged = mm(jnp.concatenate([quad.astype(BF) for quad in quads], 1), w_merge[...])
    for i in range(7):
        merged_ref[i] = merged[8 * i : 8 * i + 7].astype(BF)
    copies["to_quad_t"].wait()
    hidden_own = mm(to_quad_t[...], hidden_grad[...])

    def values_back(*windows):
        units = units_of(windows)
        wide = [
            t_mm(probs[GROUPS * w + g].astype(BF), of_window(outer, w, 0, g)) for w, g in units
        ]
        for (w, g), value in zip(units, wide):
            back = heads_of(value).astype(BF)
            put_window(proj_grad, *WINDOWS[w], group_lanes(2, g), back)

    def scores_back(*windows):
        units = units_of(windows)
        wide = [
            mm_t(of_window(outer, w, 0, g), spread(of_window(qkv, w, 2, g))) for w, g in units
        ]
        grads = split_halves(wide)
        prob = split_halves([probs[GROUPS * w + g] for w, g in units])
        sums = half_sums([p * grad for p, grad in zip(prob, grads)])
        parts = [p * (grad - total) * SCALE for p, grad, total in zip(prob, grads, sums)]
        soft = join_halves(parts)
        wide = [t_mm(part, of_window(qkv, w, 0, g)) for (w, g), part in zip(units, soft)]
        for (w, g), part in zip(units, soft):
            back = mm(part, spread(of_window(qkv, w, 1, g))).astype(BF)
            put_window(proj_grad, *WINDOWS[w], group_lanes(0, g), back)
        for (w, g), value in zip(units, wide):
            back = heads_of(value).astype(BF)
            put_window(proj_grad, *WINDOWS[w], group_lanes(1, g), back)

    def core_copy(i):
        return pltpu.make_async_remote_copy(
            src_ref=g_send.at[i, 1 - core], dst_ref=g_recv.at[i], send_sem=c_ssem.at[i],
            recv_sem=c_rsem.at[i], device_id={"frame_2": 1 - core},
        )

    def start_core(i, product):
        product = product.reshape(2, 192, C)
        g_own[i] = product
        if scatter:
            g_send[i] = product.astype(BF)
            core_copy(i).start()

    def x_copies(i, sent, landing):
        return [
            pltpu.make_async_remote_copy(
                src_ref=sent.at[(xi + step) % 4], dst_ref=landing.at[step - 1],
                send_sem=x_ssem.at[X_SLOTS[i]], recv_sem=x_rsem.at[X_SLOTS[i]],
                device_id=x_id(step),
            )
            for step in (2, 1, 3)
        ]

    def end_all(landing, sent_sem, landed_sem):
        pltpu.make_async_remote_copy(
            src_ref=landing, dst_ref=landing, send_sem=sent_sem, recv_sem=landed_sem,
            device_id={"frame_2": 1 - core},
        ).wait()

    def end_x(i, landing):
        end_all(landing, x_ssem.at[X_SLOTS[i]], x_rsem.at[X_SLOTS[i]])

    def y_copy(i, m, sent, landing):
        return pltpu.make_async_remote_copy(
            src_ref=sent.at[m], dst_ref=landing.at[y], send_sem=y_ssem.at[Y_SLOTS[i], m],
            recv_sem=y_rsem.at[Y_SLOTS[i], y],
            device_id={"frame_1": 2 * core + m // 2, "frame_2": m % 2},
        )

    def y_landed(i, source, sent, landing):
        return pltpu.make_async_remote_copy(
            src_ref=sent.at[0], dst_ref=landing.at[source], send_sem=y_ssem.at[Y_SLOTS[i], 0],
            recv_sem=y_rsem.at[Y_SLOTS[i], source], device_id={"frame_2": 1 - core},
        )

    def stays(m):
        return jnp.logical_and(2 * core + m // 2 == y, core == m % 2)

    def start_y(i, sent, landing):
        for m in range(4):

            @pl.when(stays(m))
            def _():
                landing[y] = sent[m]

            @pl.when(jnp.logical_not(stays(m)))
            def _():
                y_copy(i, m, sent, landing).start()

    def end_y(i, sent, landing):
        for source in range(4):
            mine = jnp.logical_and(y == source, y // 2 == core)

            @pl.when(jnp.logical_not(mine))
            def _():
                y_landed(i, source, sent, landing).wait_recv()

        for m in range(4):

            @pl.when(jnp.logical_not(stays(m)))
            def _():
                y_copy(i, m, sent, landing).wait_send()

        total = landing[0].astype(F32)
        for source in range(1, 4):
            total = total + landing[source].astype(F32)
        return total

    wide_lane = lax.broadcasted_iota(jnp.int32, (1, C), 1)

    def segments(i, block):
        one, two, three = (block[16 * k : 16 * k + 16] for k in range(3))

        def left(value, count):
            return pltpu.roll(value, C - count, 1)

        if i == 0:
            second = jnp.where(wide_lane < 96, left(one, 288), pltpu.roll(two, 96, 1))
            third = jnp.where(wide_lane < 192, left(two, 192), pltpu.roll(three, 192, 1))
            return one, second, third, left(three, 96)
        if i == 1:
            return one, left(one, 96), two, three
        if i == 2:
            return one, two, three, left(three, 288)
        return one, two, left(two, 192), three

    def start_first(i):
        if not scatter:
            return
        core_copy(i).wait()
        total = (g_own[i, core] + g_recv[i].astype(F32)).reshape(4, 48, C)
        j = i // 2
        if i % 2 == 0:
            x_own[j] = total
            x_send[j] = total.astype(BF)
            for copy in x_copies(i, x_send.at[j], x_recv.at[j]):
                copy.start()
        else:
            for block in range(4):
                for m, value in enumerate(segments(i, total[block])):
                    y_send[j, m, block] = value.astype(BF)
            start_y(i, y_send.at[j], y_recv.at[j])

    def start_second(i):
        j = i // 2
        if i % 2 == 0:
            end_x(i, x_recv.at[j])
            total = x_own[j, xi]
            for step in (1, 2, 3):
                total = total + x_recv[j, step - 1].astype(F32)
            for m, value in enumerate(segments(i, total)):
                y_send2[j, m] = value.astype(BF)
            start_y(4 + j, y_send2.at[j], y_recv2.at[j])
        else:
            total = end_y(i, y_send.at[j], y_recv.at[j])
            x_own2[j] = total
            x_send2[j] = total.astype(BF)
            for copy in x_copies(4 + j, x_send2.at[j], x_recv2.at[j]):
                copy.start()

    def z_copy(j, step):
        return pltpu.make_async_remote_copy(
            src_ref=z_send.at[j, (z + step) % 16], dst_ref=z_recv.at[j, step - 1],
            send_sem=z_ssem.at[j], recv_sem=z_rsem.at[j], device_id=z_id(step),
        )

    z_steps = sorted(range(1, 16), key=lambda step: -min(step, 16 - step))

    def start_z(j):
        first = end_y(4 + j, y_send2.at[j], y_recv2.at[j])
        end_x(4 + j, x_recv2.at[j])
        second = x_own2[j, xi]
        for step in (1, 2, 3):
            second = second + x_recv2[j, step - 1].astype(F32)
        for t in range(3):
            lanes = slice(128 * t, 128 * t + 128)
            z_line[j, pl.ds(t, 16, stride=8), :] = first[:, lanes]
            z_line[j, pl.ds(t + 3, 16, stride=8), :] = second[:, lanes]
        for t in (6, 7):
            z_line[j, pl.ds(t, 16, stride=8), :] = jnp.zeros((16, 128), F32)
        z_send[j] = z_line[j].reshape(16, 8, 128).astype(BF)
        for step in z_steps:
            z_copy(j, step).start()

    def end_z(j):
        total = z_send[j, z].astype(F32)
        end_all(z_recv.at[j], z_ssem.at[j], z_rsem.at[j])
        for step in z_steps:
            total = total + z_recv[j, step - 1].astype(F32)
        share_ref[8 * j : 8 * j + 8] = total

    scores_back(2, 3)
    exchange(2, west_id).wait()
    widen_reach(2)
    branch_grad[192:256] = ex_recv[2]
    outer[192:256] = mm_t(ex_recv[2], w_out[...]).astype(BF)
    start_core(0, mm(left_o[...], branch_grad[...]))
    values_back(0, 1, 2, 3)
    start_core(1, mm(left_r[...], proj_grad[:, 2 * C : 3 * C]))
    start_first(0)
    scores_back(0, 1)
    start_first(1)
    start_core(3, mm(left_r[...], proj_grad[:, C : 2 * C]))
    start_core(2, mm(left_r[...], proj_grad[:, 0:C]))
    east_grad = mm_t(proj_grad[192:256], w_attend[...])
    east_grad = normalize_back(normed_east[...], std_east[...], east_grad)
    ex_send[3] = east_grad.astype(BF)
    exchange(3, east_id).start()
    start_first(3)
    start_first(2)
    copies["to_window_t"].wait()
    own_proj = mm(to_window_t[:, 0:192], proj_grad[0:192]).astype(BF)
    own_grad = mm_t(own_proj, w_attend[...])
    own_grad = normalize_back(normed_scr[...], std_scr[...], own_grad)
    feature_scr[...] = hidden_own + own_grad

    def end_features():
        exchange(3, east_id).wait()
        grad = feature_scr[...] + mm(to_window_t[:, 192:256], ex_recv[3])
        grad = grad.reshape(14, 16, C)
        for row in range(14):
            grad_ref[row] = grad[row, 0:14].astype(BF)

    if scatter:
        for group in range(4):
            start_second(group)
        start_z(0)
        start_z(1)
        end_features()
        end_z(0)
        end_z(1)
    else:
        end_features()
        share_ref[...] = jnp.zeros_like(share_ref)
        local_ref[...] = g_own[...]


def finish(merged_in, grad_in, share, merged_ref, grad_ref, attend_ref, output_ref):
    merged_ref[0] = merged_in[...]
    grad_ref[0] = grad_in[...]
    lane = lax.broadcasted_iota(jnp.int32, (1, 128), 1)

    def put(ref, pieces):
        lines = [jnp.zeros((1, 128), F32) for _ in range(-(-ref.shape[0] // 128))]
        start = 0
        for first, width in pieces:
            skip, turn = divmod(start, 128)
            values = [share[first + i : first + i + 1, :] for i in range(3)]
            if turn:
                values = [pltpu.roll(value, turn, 1) for value in values]
            for j in range(skip, (start + width - 1) // 128 + 1):
                value = values[min(j - skip, 2)]
                if turn and j > skip:
                    value = jnp.where(lane < turn, values[j - skip - 1], value)
                at = lane + 128 * j
                inside = jnp.logical_and(at >= start, at < start + width)
                lines[j] = jnp.where(inside, value, lines[j])
            start += width
        for j, value in enumerate(lines):
            count = min(128, ref.shape[0] - 128 * j)
            ref[128 * j : 128 * j + count] = value.reshape(128)[:count]

    put(output_ref, ((0, 288),))
    v, q, k = 3, 8, 11
    segment = 2 * (lax.axis_index("frame_1") % 2) + lax.axis_index("frame_2")
    for m, pieces in enumerate((
        ((q, 384), (k, 384), (v, 96)),
        ((v, 288), (q, 384), (k, 192)),
        ((k, 192), (v, 384), (q, 288)),
        ((q, 96), (k, 384), (v, 384)),
    )):
        pl.when(segment == m)(functools.partial(put, attend_ref, pieces))


def local_call(scatter, features, position_bias, attend_weight, output_weight, merge_weight, cotangent):
    given = (features[0], cotangent[0], position_bias.T, attend_weight, output_weight, merge_weight)
    given = given + tuple(jnp.asarray(table) for table in tables())
    dma = pltpu.SemaphoreType.DMA
    scratch = [pltpu.VMEM(a.shape, a.dtype) for a in given]
    scratch += [
        pltpu.VMEM((14, 16, C), F32),
        pltpu.VMEM((8, 8, OUT), F32),
        pltpu.VMEM((16, 256), F32),
        pltpu.VMEM((1024, 128), F32),
        pltpu.VMEM((1024, 128), F32),
        pltpu.VMEM((224, C), F32),
        pltpu.VMEM((224, 1), F32),
        pltpu.VMEM((64, C), F32),
        pltpu.VMEM((64, 1), F32),
        pltpu.VMEM((384, 3 * C), BF),
        pltpu.VMEM((12, 64, 256), F32),
        pltpu.VMEM((256, C), BF),
        pltpu.VMEM((256, C), BF),
        pltpu.VMEM((256, C), BF),
        pltpu.VMEM((256, 3 * C), BF),
        pltpu.VMEM((256, C), BF),
        pltpu.VMEM((C, 256), BF),
        pltpu.VMEM((C, 256), BF),
        pltpu.VMEM((224, C), F32),
        pltpu.VMEM((64, C), BF),
        pltpu.VMEM((4, 64, C), BF),
        pltpu.VMEM((4, 64, C), BF),
        pltpu.VMEM((4, 2, 192, C), F32),
        pltpu.VMEM((4, 2, 192, C), BF),
        pltpu.VMEM((4, 192, C), BF),
        pltpu.VMEM((2, 4, 48, C), F32),
        pltpu.VMEM((2, 4, 48, C), BF),
        pltpu.VMEM((2, 3, 48, C), BF),
        pltpu.VMEM((2, 4, 4, 16, C), BF),
        pltpu.VMEM((2, 4, 4, 16, C), BF),
        pltpu.VMEM((2, 4, 16, C), F32),
        pltpu.VMEM((2, 4, 16, C), BF),
        pltpu.VMEM((2, 3, 16, C), BF),
        pltpu.VMEM((2, 4, 16, C), BF),
        pltpu.VMEM((2, 4, 16, C), BF),
        pltpu.VMEM((2, 128, 128), F32),
        pltpu.VMEM((2, 16, 8, 128), BF),
        pltpu.VMEM((2, 15, 8, 128), BF),
        dma((N_IN,)), dma((4,)), dma((4,)), dma((4,)), dma((4,)), dma((4,)), dma((4,)),
        dma((4, 4)), dma((4, 4)), dma((2,)), dma((2,)), pltpu.SemaphoreType.REGULAR((3,)),
    ]
    vmem = pl.BlockSpec(memory_space=pltpu.VMEM)
    return pl.pallas_call(
        functools.partial(kernel, scatter),
        out_shape=(
            pltpu.VMEM((7, 7, OUT), BF),
            pltpu.VMEM((14, 14, C), BF),
            pltpu.VMEM((16, 128), F32),
        )
        + (() if scatter else (jax.ShapeDtypeStruct((4, 2, 192, C), F32),)),
        in_specs=[pl.BlockSpec(memory_space=pl.ANY)] * N_IN,
        out_specs=(vmem,) * (3 if scatter else 4),
        scratch_shapes=scratch,
        compiler_params=pltpu.CompilerParams(collective_id=0, has_side_effects=True),
    )(*given)


def per_device(*arrays):
    merged, feature_grad, share = local_call(True, *arrays)
    vmem = pl.BlockSpec(memory_space=pltpu.VMEM)
    return pl.pallas_call(
        finish,
        out_shape=(
            jax.ShapeDtypeStruct((1, *merged.shape), BF),
            jax.ShapeDtypeStruct((1, *feature_grad.shape), BF),
            jax.ShapeDtypeStruct((864,), F32),
            jax.ShapeDtypeStruct((288,), F32),
        ),
        in_specs=(vmem,) * 3,
        out_specs=(vmem,) * 4,
        compiler_params=pltpu.CompilerParams(vmem_limit_bytes=8 << 20),
    )(merged, feature_grad, share)


def solution(mesh):
    split = Mesh(mesh.devices.reshape(16, 2, 2, 4, 2), AZIM_FRAME)
    placed = (P(FRAME, None, AZIM, None), P(), P(), P(), P(), P(FRAME, None, AZIM, None))
    return jax.shard_map(
        per_device,
        mesh=split,
        in_specs=placed,
        out_specs=(
            P(FRAME, None, AZIM, None),
            P(FRAME, None, AZIM, None),
            P(AZIM_FRAME),
            P(AZIM_FRAME),
        ),
        check_vma=False,
    )
```
